32 devices in a mesh: energy: 8 (over z, x), slab: 4 (over y, core).
Axes of the slice: x: 2, y: 2, z: 4, core: 2. Of those that a mesh axis runs over, the one named last changes fastest.
Arguments:
- green_blocks: bfloat16 [8, 4, 512, 512], P('energy', 'slab'), may hold values from -6 to 6
- coulomb: bfloat16 [4, 512, 512], P('slab'), may hold values from -0.25 to 0.25
- couple_cols: int32 [4, 128, 8], P('slab'), may hold values from 0 to 127
- couple_vals: bfloat16 [4, 128, 8], P('slab'), may hold values from -0.8984375 to 0.8984375
Outputs:
- new_green: bfloat16 [8, 4, 512, 512], P('energy', 'slab')
The draws below stay inside these ranges and needn't reach their ends.
Inputs may be any that keep to these rules, and one draw needn't show every extreme that they name: couple_cols[s, i, k] names one of the first 128 orbitals of slab s + 1.
All inputs are finite; a program needn't handle non-finite values.
Results may differ from the reference program's by a relative error of at most 0.015.
Values may be sent and summed in bfloat16 or wider, within the bound.
A program may use at most 64 MiB of HBM per device.

```python
import math
import jax
import jax.numpy as jnp
from jax import lax

M = 512
COUPLINGS = 8
IFACE = 128
NE = 8
SLABS = 4


def with_ends(values, own_key, least, high):
    spot = [jax.random.randint(jax.random.fold_in(own_key, axis), (), 0, length) for axis, length in enumerate(values.shape)]
    main_axis = values.shape.index(max(values.shape))
    neighbour = spot[:main_axis] + [(spot[main_axis] + 1) % values.shape[main_axis]] + spot[main_axis + 1:]
    return values.at[tuple(spot)].set(least).at[tuple(neighbour)].set(high)


def block_scale(own_key, dims, split, low, largest):
    factor_of = 1.0
    for position, shards_of in split:
        steps = jax.random.uniform(jax.random.fold_in(jax.random.fold_in(own_key, 6), position), (shards_of,), jnp.float32, low / len(split), largest / len(split))
        factor_of = factor_of * jnp.repeat(jnp.exp(steps), dims[position] // shards_of).reshape((-1,) + (1,) * (len(dims) - 1 - position))
    return factor_of


def bell_draw(rng, shape, deviation, bound, cuts=(), kind=jnp.bfloat16):
    array = jax.random.normal(rng, shape, jnp.float32) * deviation
    if len(cuts) > 0:
        array = block_scale(rng, shape, cuts, -0.22, 0.18) * array
    return jnp.clip(array, min=-bound, max=bound).astype(kind)


def setup_inputs(seed: int = 0) -> dict:
    streams_of = jax.random.split(jax.random.key(seed), 5)
    green_blocks = bell_draw(streams_of[0], (NE, SLABS, M, M), 1.0, 6.0, ((0, 8), (1, 4)))
    coulomb = bell_draw(streams_of[1], (SLABS, M, M), M ** -0.5, 0.25, ((0, 4),))
    couple_cols = with_ends(jax.random.randint(streams_of[2], (SLABS, IFACE, COUPLINGS), 0, IFACE), jax.random.fold_in(streams_of[2], 1), 0, IFACE - 1).astype(jnp.int32)
    couple_vals = bell_draw(streams_of[3], (SLABS, IFACE, COUPLINGS), 0.15, 0.8984375, ((0, 4),))
    return dict(green_blocks=green_blocks, coulomb=coulomb, couple_cols=couple_cols, couple_vals=couple_vals)


row_block = 32

def coupling_matrix(column_ids, coupling_values):
    width = column_ids.shape[0]
    hits = column_ids[:, :, None] == jnp.arange(width, dtype=jnp.int32)[None, None, :]
    summed = lax.optimization_barrier(jnp.sum(jnp.where(hits, coupling_values.astype(jnp.float32)[:, :, None], jnp.float32(0.0)), axis=1))
    return summed.astype(jnp.bfloat16)

def screen(polar_one, coulomb_block):
    inner = jnp.dot(coulomb_block, polar_one, preferred_element_type=jnp.float32).astype(jnp.bfloat16)
    second = jnp.dot(inner, coulomb_block, preferred_element_type=jnp.float32)
    third = jnp.dot(inner, second.astype(jnp.bfloat16), preferred_element_type=jnp.float32)
    return (coulomb_block.astype(jnp.float32) + second + third).astype(jnp.bfloat16)

def batched(left, right):
    return jnp.einsum('eij,ejk->eik', left.astype(jnp.float32), right.astype(jnp.float32))

def reference(green_blocks, coulomb, couple_cols, couple_vals):
    inv_root = 1.0 / math.sqrt(M)
    block_starts = jnp.arange(M // row_block, dtype=jnp.int32) * row_block
    outputs = []
    for slab_index in range(SLABS):
        green_slab = green_blocks[:, slab_index]
        coulomb_block = coulomb[slab_index]

        def polar_rows(start):
            rows_now = lax.dynamic_slice_in_dim(green_slab, start, row_block, 1).astype(jnp.float32)
            mirror = jnp.swapaxes(lax.dynamic_slice_in_dim(green_slab, start, row_block, 2), 1, 2).astype(jnp.float32)
            spectra = jnp.fft.fft(rows_now, axis=0) * jnp.conj(jnp.fft.fft(mirror, axis=0))
            return jnp.real(jnp.fft.ifft(spectra, axis=0)).astype(jnp.float32)
        polar = jnp.swapaxes(lax.map(polar_rows, block_starts), 0, 1).reshape(NE, M, M)
        polar = (polar * (0.5 / math.sqrt(M * NE))).astype(jnp.bfloat16)
        screened = lax.map(lambda polar_one: screen(polar_one, coulomb_block), polar)
        screened = lax.optimization_barrier(screened)

        def sigma_rows(start):
            rows_now = lax.dynamic_slice_in_dim(green_slab, start, row_block, 1).astype(jnp.float32)
            waves = lax.dynamic_slice_in_dim(screened, start, row_block, 1).astype(jnp.float32)
            spectra = jnp.fft.fft(rows_now, axis=0) * jnp.fft.fft(waves, axis=0)
            return jnp.real(jnp.fft.ifft(spectra, axis=0)).astype(jnp.float32)
        sigma = jnp.swapaxes(lax.map(sigma_rows, block_starts), 0, 1).reshape(NE, M, M)
        sigma = (sigma * (0.2 / math.sqrt(NE))).astype(jnp.bfloat16)
        total = sigma.astype(jnp.float32)
        last = M - IFACE
        if slab_index + 1 < SLABS:
            coupling = coupling_matrix(couple_cols[slab_index], couple_vals[slab_index])
            corner = green_blocks[:, slab_index + 1, :IFACE, :IFACE]
            near_next = jnp.einsum('ij,ejk->eik', coupling.astype(jnp.float32), corner.astype(jnp.float32))
            near_next = lax.optimization_barrier(near_next.astype(jnp.bfloat16))
            right_part = jnp.einsum('eij,kj->eik', near_next.astype(jnp.float32), coupling.astype(jnp.float32)) * inv_root
            total = total.at[:, last:, last:].add(right_part)
        if slab_index > 0:
            previous = coupling_matrix(couple_cols[slab_index - 1], couple_vals[slab_index - 1])
            corner = green_blocks[:, slab_index - 1, last:, last:]
            near_prev = jnp.einsum('ji,ejk->eik', previous.astype(jnp.float32), corner.astype(jnp.float32))
            near_prev = lax.optimization_barrier(near_prev.astype(jnp.bfloat16))
            left_part = jnp.einsum('eij,jk->eik', near_prev.astype(jnp.float32), previous.astype(jnp.float32)) * inv_root
            total = total.at[:, :IFACE, :IFACE].add(left_part)
        total_b = lax.optimization_barrier(total.astype(jnp.bfloat16))
        dressed = lax.optimization_barrier(batched(green_slab, total_b).astype(jnp.bfloat16))
        updated = green_slab.astype(jnp.float32) + batched(dressed, green_slab) * inv_root
        outputs.append(updated.astype(jnp.bfloat16))
    return jnp.stack(outputs, axis=1)
```

```python
import functools
import math

import jax
import jax.numpy as jnp
from jax import lax
from jax.experimental import pallas as pl
from jax.experimental.pallas import tpu as pltpu
from jax.sharding import PartitionSpec as P


def from_behind(x, axis, by):
    size = lax.axis_size(axis)
    pairs = [(i, i + by) for i in range(size) if 0 <= i + by < size]
    return lax.ppermute(x, axis, pairs)


def plain_dot(left, right):
    return jnp.dot(left, right, preferred_element_type=jnp.float32)


def split_parts(values):
    upper = values.astype(jnp.bfloat16)
    lower = (values - upper.astype(jnp.float32)).astype(jnp.bfloat16)
    return (upper, lower)


def coupling_matrix(column_ids, coupling_values):
    width = column_ids.shape[0]
    hits = column_ids[:, :, None] == jnp.arange(width, dtype=jnp.int32)[None, None, :]
    summed = jnp.sum(
        jnp.where(hits, coupling_values.astype(jnp.float32)[:, :, None], jnp.float32(0.0)), axis=1
    )
    return summed.astype(jnp.bfloat16)


def on_device(green_blocks, coulomb, couple_cols, couple_vals):
    own_green = green_blocks[:, 0]
    coulomb_block = coulomb[0]
    per_device = own_green.shape[0]
    orbitals = own_green.shape[1]
    volume = lax.axis_size("energy")
    energies = per_device * volume
    inv_root = 1.0 / math.sqrt(orbitals)
    flipped = jnp.swapaxes(own_green, 1, 2)
    received, flipped_recv = (
        lax.all_to_all(own_green, "energy", split_axis=1, concat_axis=0, tiled=True),
        lax.all_to_all(flipped, "energy", split_axis=1, concat_axis=0, tiled=True),
    )
    green_entries = received.reshape(energies, -1)
    flipped_entries = flipped_recv.reshape(energies, -1)
    entry_shape = received.shape
    halfway = energies // 2 + 1
    frequency = jnp.arange(halfway, dtype=jnp.int32)
    energy_index = jnp.arange(energies, dtype=jnp.int32)
    angles = (frequency[:, None] * energy_index[None, :] % energies).astype(jnp.float32) * (
        2.0 * math.pi / energies
    )
    cosine = jnp.cos(angles)
    sine = jnp.sin(angles)
    weights = (
        jnp.where((frequency == 0) | (2 * frequency == energies), 1.0, 2.0).astype(jnp.float32)
        / energies
    )
    forward_high, forward_low = split_parts(jnp.concatenate([cosine, -sine], axis=0))
    backward_table = jnp.concatenate(
        [cosine * weights[:, None], -sine * weights[:, None]], axis=0
    ).T
    backward_high, backward_low = split_parts(backward_table)

    def spectrum(entries):
        stacked = plain_dot(forward_high, entries) + plain_dot(forward_low, entries)
        return (stacked[:halfway], stacked[halfway:])

    def to_values(real_part, imag_part):
        data_high, data_low = split_parts(jnp.concatenate([real_part, imag_part], axis=0))
        return (
            plain_dot(backward_high, data_high)
            + plain_dot(backward_high, data_low)
            + plain_dot(backward_low, data_high)
        )

    green_real, green_imag = spectrum(green_entries)
    mirror_real, mirror_imag = spectrum(flipped_entries)
    polar_entries = to_values(
        green_real * mirror_real + green_imag * mirror_imag,
        green_imag * mirror_real - green_real * mirror_imag,
    )
    polar_entries = (polar_entries * (0.5 / math.sqrt(orbitals * energies))).astype(jnp.bfloat16)
    polar = lax.all_to_all(
        polar_entries.reshape(entry_shape), "energy", split_axis=0, concat_axis=1, tiled=True
    )
    inner = jnp.einsum(
        "ij,ejk->eik", coulomb_block, polar, preferred_element_type=jnp.float32
    ).astype(jnp.bfloat16)
    second = jnp.einsum("eij,jk->eik", inner, coulomb_block, preferred_element_type=jnp.float32)
    third = jnp.einsum(
        "eij,ejk->eik", inner, second.astype(jnp.bfloat16), preferred_element_type=jnp.float32
    )
    screened = (coulomb_block.astype(jnp.float32)[None] + second + third).astype(jnp.bfloat16)
    screened_entries = lax.all_to_all(
        screened, "energy", split_axis=1, concat_axis=0, tiled=True
    ).reshape(energies, -1)
    screen_real, screen_imag = spectrum(screened_entries)
    sigma_entries = to_values(
        green_real * screen_real - green_imag * screen_imag,
        green_real * screen_imag + green_imag * screen_real,
    )
    sigma_entries = (sigma_entries * (0.2 / math.sqrt(energies))).astype(jnp.bfloat16)
    sigma = lax.all_to_all(
        sigma_entries.reshape(entry_shape), "energy", split_axis=0, concat_axis=1, tiled=True
    )
    interface = couple_cols.shape[1]
    last = orbitals - interface
    coupling = coupling_matrix(couple_cols[0], couple_vals[0])
    prev_green, previous = from_behind((own_green, coupling), "slab", 1)
    next_green = from_behind(own_green, "slab", -1)
    prev_corner = prev_green[:, last:, last:]
    next_corner = next_green[:, :interface, :interface]
    near_next = jnp.einsum(
        "ij,ejk->eik", coupling, next_corner, preferred_element_type=jnp.float32
    ).astype(jnp.bfloat16)
    near_prev = jnp.einsum(
        "ji,ejk->eik", previous, prev_corner, preferred_element_type=jnp.float32
    ).astype(jnp.bfloat16)
    right_part = (
        jnp.einsum("eij,kj->eik", near_next, coupling, preferred_element_type=jnp.float32)
        * inv_root
    )
    left_part = (
        jnp.einsum("eij,jk->eik", near_prev, previous, preferred_element_type=jnp.float32)
        * inv_root
    )
    total = sigma.astype(jnp.float32)
    total = total.at[:, last:, last:].add(right_part)
    total = total.at[:, :interface, :interface].add(left_part)
    total_b = total.astype(jnp.bfloat16)
    dressed = jnp.einsum(
        "eij,ejk->eik", own_green, total_b, preferred_element_type=jnp.float32
    ).astype(jnp.bfloat16)
    updated = (
        own_green
        + jnp.einsum("eij,ejk->eik", dressed, own_green, preferred_element_type=jnp.float32)
        * inv_root
    )
    return updated.astype(jnp.bfloat16)[:, None]


MESH = pl.DeviceIdType.MESH


def unit_blocks(unit, grid):
    odd = grid - 1
    paired = grid * odd // 2
    slot = unit // odd
    turn = unit % odd
    diagonal = unit // paired
    first = (turn + slot) % odd
    second = (turn + odd - slot) % odd
    lone = 1 - (slot + odd - 1) // odd
    row = lone * odd + (1 - lone) * first
    col = lone * turn + (1 - lone) * second
    corner = 2 * (unit - paired)
    row0 = diagonal * corner + (1 - diagonal) * row
    col0 = diagonal * corner + (1 - diagonal) * col
    row1 = diagonal * (corner + 1) + (1 - diagonal) * col
    col1 = diagonal * (corner + 1) + (1 - diagonal) * row
    return ((row0, col0), (row1, col1))


CHUNKS = 2


def fused_kernel(
    volume, slabs, grid, scale_polar, scale_sigma, inv_root,
    green_hbm, coulomb_hbm, cols_hbm, vals_hbm, out,
    green, coulomb, cols, vals,
    stage, landed, mirror, second_half, polar_out, polar_more, matrix, inner, second, screened,
    screen_in, sigma_out, sigma,
    coupling, turned, next_corner, left_out, left_in, right_in,
    g_send, g_recv, p_send, p_recv, m_send, m_recv, w_send, w_recv, s_send, s_recv,
    slab_send, slab_recv, load_sem,
):
    loads = [
        pltpu.make_async_copy(source, target, load_sem.at[n])
        for n, (source, target) in enumerate(
            ((green_hbm, green), (coulomb_hbm, coulomb), (cols_hbm, cols), (vals_hbm, vals))
        )
    ]
    for load in loads:
        load.start()
    me = lax.axis_index("energy")
    slab = lax.axis_index("slab")
    size = green.shape[0] // grid
    last = green.shape[0] - size
    classes = volume // 2
    paired = grid * (grid - 1) // 2
    order = sorted(range(1, volume), key=lambda k: (-min(k, volume - k), k))
    has_prev = 1 - (slabs - 1 - slab + 0) // (slabs - 1)
    has_next = 1 - slab // (slabs - 1)
    diagonal = me // paired
    my_class = lax.rem(me, classes)
    first_mate = me - my_class
    own_blocks = unit_blocks(me, grid)
    chunk_rows = size // CHUNKS

    def peer_of(k):
        return lax.rem(me + k, volume)

    def from_of(k):
        return lax.rem(me + volume - k, volume)

    barrier = pltpu.get_barrier_semaphore()
    for k in range(1, volume):
        pl.semaphore_signal(barrier, inc=1, device_id=(peer_of(k), slab), device_id_type=MESH)

    @pl.when(slab > 0)
    def _():
        pl.semaphore_signal(barrier, inc=1, device_id=(me, slab - 1), device_id_type=MESH)

    @pl.when(slab < slabs - 1)
    def _():
        pl.semaphore_signal(barrier, inc=1, device_id=(me, slab + 1), device_id_type=MESH)

    def flipped(block):
        return block.astype(jnp.float32).T.astype(jnp.bfloat16)

    def region(coords, start=0, rows=None):
        rows = size if rows is None else rows
        row = pl.multiple_of(coords[0] * size + start, rows)
        col = pl.multiple_of(coords[1] * size, size)
        return pl.ds(row, rows), pl.ds(col, size)

    def block_of(ref, coords, start=0, rows=None):
        return ref.at[region(coords, start, rows)]

    def remote(src, dst, sends, recvs, device):
        return pltpu.make_async_remote_copy(
            src_ref=src, dst_ref=dst, send_sem=sends, recv_sem=recvs,
            device_id=(device, slab), device_id_type=MESH,
        )

    loads[0].wait()
    for unit in range(volume):
        coords = unit_blocks(unit, grid)[1]
        block = green[coords[0] * size:(coords[0] + 1) * size, coords[1] * size:(coords[1] + 1) * size]
        stage[unit] = block if unit >= paired else flipped(block)

    pl.semaphore_wait(barrier, volume - 1 + has_prev + has_next)

    def span(chunk):
        return pl.ds(chunk * chunk_rows, chunk_rows)

    green_copies = []
    for chunk in range(CHUNKS):
        batch = []
        for slot in range(2):
            for k in order:
                peer = peer_of(k)
                coords = unit_blocks(peer, grid)[0]
                if slot == 0:
                    source = block_of(green, coords, chunk * chunk_rows, chunk_rows)
                else:
                    source = stage.at[peer, span(chunk)]
                copy = remote(
                    source, landed.at[me, slot, span(chunk)],
                    g_send.at[k, chunk, slot], g_recv.at[k, chunk, slot], peer,
                )
                copy.start()
                batch.append(copy)
        green_copies.append(batch)
    landed[me, 0] = block_of(green, own_blocks[0])[...]
    landed[me, 1] = stage[me]

    corner_copy = pltpu.make_async_remote_copy(
        src_ref=green.at[pl.ds(0, size), pl.ds(0, size)], dst_ref=next_corner,
        send_sem=slab_send.at[0], recv_sem=slab_recv.at[0],
        device_id=(me, slab - has_prev), device_id_type=MESH,
    )
    left_copy = pltpu.make_async_remote_copy(
        src_ref=left_out, dst_ref=left_in,
        send_sem=slab_send.at[1], recv_sem=slab_recv.at[1],
        device_id=(me, slab + has_next), device_id_type=MESH,
    )

    @pl.when(slab > 0)
    def _():
        corner_copy.start()

    loads[2].wait()
    loads[3].wait()
    ids = cols[...]
    values = vals[...].astype(jnp.float32)
    columns = lax.broadcasted_iota(jnp.int32, (size, size), 0)
    summed = jnp.zeros((size, size), jnp.float32)
    for k in range(ids.shape[0]):
        summed += jnp.where(ids[k:k + 1, :] == columns, values[k:k + 1, :], jnp.float32(0.0))
    summed = summed.astype(jnp.bfloat16).astype(jnp.float32)
    turned[...] = summed.astype(jnp.bfloat16)
    coupling[...] = summed.T.astype(jnp.bfloat16)

    @pl.when(slab < slabs - 1)
    def _():
        near_prev = plain_dot(turned[...], green[last:, last:]).astype(jnp.bfloat16)
        left_out[...] = plain_dot(near_prev, coupling[...]) * inv_root
        left_copy.start()

    loads[1].wait()
    rows_at_once = 16
    steps = chunk_rows // rows_at_once

    def rows_of(step):
        return pl.ds(pl.multiple_of(step * rows_at_once, rows_at_once), rows_at_once)

    def correlation(mine, theirs, e):
        acc = mine[0] * theirs[(0 - e) % volume]
        for e2 in range(1, volume):
            acc += mine[e2] * theirs[(e2 - e) % volume]
        return (acc * scale_polar).astype(jnp.bfloat16)

    where = (
        (0, own_blocks[0]),
        (1 - diagonal, tuple(
            diagonal * d + (1 - diagonal) * o for d, o in zip(own_blocks[1], own_blocks[0])
        )),
    )

    def polar_copy(k, chunk, slot):
        peer = peer_of(k)
        index, coords = where[slot]
        return remote(
            polar_out.at[lax.rem(peer, classes), slot, span(chunk)],
            block_of(matrix.at[index], coords, chunk * chunk_rows, chunk_rows),
            p_send.at[k, chunk, slot], p_recv.at[k, chunk, slot], peer,
        )

    def send_polar(chunk):
        for slot in range(2):
            for k in order:
                polar_copy(k, chunk, slot).start()

    def more_copy(target, slot):
        return remote(
            polar_more.at[slot],
            block_of(matrix.at[1], own_blocks[slot]),
            m_send.at[target, slot], m_recv.at[lax.rem(me, paired), slot], target * classes,
        )

    def arrived(copies):
        for copy in copies:
            copy.wait_recv()

    @pl.when(diagonal == 0)
    def _():
        for chunk in range(CHUNKS):
            arrived(green_copies[chunk])

            def correlate(step, carry):
                rows = rows_of(step)
                mine = [landed[e, 0, rows, :].astype(jnp.float32) for e in range(volume)]
                theirs = [landed[e, 1, rows, :].astype(jnp.float32) for e in range(volume)]
                for e in range(volume):
                    if e % classes == 0:
                        place = (0, e // classes)
                    else:
                        place = (min(e, volume - e), e // classes)
                    polar_out[place[0], place[1], rows, :] = correlation(mine, theirs, e)
                return carry

            lax.fori_loop(chunk * steps, (chunk + 1) * steps, correlate, 0)
            send_polar(chunk)

    @pl.when(diagonal == 1)
    def _():
        def flip_both(e):
            for slot in range(2):
                mirror[e, slot] = flipped(landed[e, slot])

        flip_both(me)
        for n, k in enumerate(order):
            for batch in green_copies:
                for slot in range(2):
                    batch[slot * len(order) + n].wait_recv()
            flip_both(from_of(k))

        for slot in range(2):
            def correlate(step, carry, slot=slot):
                rows = rows_of(step)
                mine = [landed[e, slot, rows, :].astype(jnp.float32) for e in range(volume)]
                theirs = [mirror[e, slot, rows, :].astype(jnp.float32) for e in range(volume)]
                for e in range(classes):
                    polar_out[e, slot, rows, :] = correlation(mine, theirs, e)
                polar_more[slot, rows, :] = correlation(mine, theirs, classes)
                return carry

            lax.fori_loop(0, size // rows_at_once, correlate, 0)
        for chunk in range(CHUNKS):
            send_polar(chunk)
        for target in range(2):
            for slot in range(2):
                more_copy(target, slot).start()

    for slot in range(2):
        index, coords = where[slot]
        block_of(matrix.at[index], coords)[...] = polar_out[my_class, slot]

    @pl.when(diagonal == 0)
    def _():
        for e in range(volume):
            second_half[e] = flipped(landed[e, 1])

    @pl.when(diagonal == 1)
    def _():
        for e in range(volume):
            second_half[e] = landed[e, 1]

    swapped = 1 - lax.rem(my_class + classes - 1, classes) // (classes - 1)

    def complete(unit):
        coords = unit_blocks(unit, grid)
        off = 1 - unit // paired

        @pl.when(off == 1)
        def _():
            for index in range(2):
                source = swapped * (1 - index) + (1 - swapped) * index
                block_of(matrix.at[index], coords[1])[...] = flipped(
                    block_of(matrix.at[source], coords[0])[...]
                )

        @pl.when(jnp.logical_and(off == 0, my_class > 0))
        def _():
            for slot in range(2):
                block_of(matrix.at[1], coords[slot])[...] = flipped(
                    block_of(matrix.at[0], coords[slot])[...]
                )

    complete(me)
    for k in order:
        for chunk in range(CHUNKS):
            for slot in range(2):
                polar_copy(k, chunk, slot).wait_recv()
        complete(from_of(k))

    @pl.when(my_class == 0)
    def _():
        for unit in range(paired, volume):
            for slot in range(2):
                remote(
                    polar_more.at[slot], block_of(matrix.at[1], unit_blocks(unit, grid)[slot]),
                    m_send.at[0, slot], m_recv.at[unit - paired, slot], first_mate,
                ).wait_recv()

    for index in range(2):
        inner[index] = plain_dot(coulomb[...], matrix[index]).astype(jnp.bfloat16)
    for index in range(2):
        product = plain_dot(inner[index], coulomb[...])
        second[index] = product
        matrix[index] = product.astype(jnp.bfloat16)
    for index in range(2):
        third = plain_dot(inner[index], matrix[index])
        screened[index] = (coulomb[...].astype(jnp.float32) + second[index] + third).astype(jnp.bfloat16)

    wave_copies = []
    for half in range(2):
        batch = []
        for t in range(1, classes):
            mate = first_mate + lax.rem(my_class + t, classes)
            rows, width = region(unit_blocks(mate, grid)[half])
            copy = remote(
                screened.at[:, rows, width], screen_in.at[my_class, half],
                w_send.at[t, half], w_recv.at[t, half], mate,
            )
            copy.start()
            batch.append(copy)
        wave_copies.append(batch)
    for half in range(2):
        rows, width = region(own_blocks[half])
        screen_in[my_class, half] = screened[:, rows, width]

    sigma_copies = []
    for half in range(2):
        arrived(wave_copies[half])

        def convolve(step, carry, half=half):
            rows = rows_of(step)
            if half == 0:
                mine = [landed[e, 0, rows, :].astype(jnp.float32) for e in range(volume)]
            else:
                mine = [second_half[e, rows, :].astype(jnp.float32) for e in range(volume)]
            waves = [
                screen_in[min(e, volume - e) % classes, half, e // classes, rows, :].astype(jnp.float32)
                for e in range(volume)
            ]
            for e in range(volume):
                acc = mine[0] * waves[e]
                for e2 in range(1, volume):
                    acc += mine[e2] * waves[(e - e2) % volume]
                sigma_out[e, half, rows, :] = (acc * scale_sigma).astype(jnp.bfloat16)
            return carry

        lax.fori_loop(0, size // rows_at_once, convolve, 0)
        for k in order:
            peer = peer_of(k)
            copy = remote(
                sigma_out.at[peer, half], block_of(sigma, own_blocks[half]),
                s_send.at[k, half], s_recv.at[k, half], peer,
            )
            copy.start()
            sigma_copies.append(copy)
        block_of(sigma, own_blocks[half])[...] = sigma_out[me, half]

    @pl.when(slab < slabs - 1)
    def _():
        corner_copy.wait_recv()
        near_next = plain_dot(coupling[...], next_corner[...]).astype(jnp.bfloat16)
        right_in[...] = plain_dot(near_next, turned[...]) * inv_root

    arrived(sigma_copies)

    @pl.when(slab < slabs - 1)
    def _():
        sigma[last:, last:] = (sigma[last:, last:].astype(jnp.float32) + right_in[...]).astype(jnp.bfloat16)
        left_copy.wait_send()

    @pl.when(slab > 0)
    def _():
        left_copy.wait_recv()
        sigma[:size, :size] = (sigma[:size, :size].astype(jnp.float32) + left_in[...]).astype(jnp.bfloat16)
        corner_copy.wait_send()

    inner[0] = plain_dot(green[...], sigma[...]).astype(jnp.bfloat16)
    updated = green[...].astype(jnp.float32) + plain_dot(inner[0], green[...]) * inv_root
    out[...] = updated.astype(jnp.bfloat16)
    for batch in green_copies + wave_copies + [sigma_copies]:
        for copy in batch:
            copy.wait_send()
    for k in order:
        for chunk in range(CHUNKS):
            for slot in range(2):
                polar_copy(k, chunk, slot).wait_send()

    @pl.when(diagonal == 1)
    def _():
        for target in range(2):
            for slot in range(2):
                more_copy(target, slot).wait_send()


def fused_on_device(grid, green_blocks, coulomb, couple_cols, couple_vals):
    volume = lax.axis_size("energy")
    slabs = lax.axis_size("slab")
    orbitals = green_blocks.shape[-1]
    size = orbitals // grid
    half_type = jnp.bfloat16

    def pieces(*lead):
        return pltpu.VMEM((*lead, size, size), half_type)

    def wholes(*lead, kind=half_type):
        return pltpu.VMEM((*lead, orbitals, orbitals), kind)

    def pair(*lead):
        return [pltpu.SemaphoreType.DMA(lead), pltpu.SemaphoreType.DMA(lead)]

    wide = pltpu.VMEM((size, size), jnp.float32)
    classes = volume // 2
    result = pl.pallas_call(
        functools.partial(
            fused_kernel, volume, slabs, grid,
            0.5 / math.sqrt(orbitals * volume), 0.2 / math.sqrt(volume), 1.0 / math.sqrt(orbitals),
        ),
        out_shape=jax.ShapeDtypeStruct((orbitals, orbitals), half_type),
        in_specs=[pl.BlockSpec(memory_space=pltpu.HBM)] * 4,
        out_specs=pl.BlockSpec(memory_space=pltpu.VMEM),
        scratch_shapes=[
            wholes(), wholes(), pltpu.VMEM(couple_cols.shape[:0:-1], jnp.int32), pltpu.VMEM(couple_vals.shape[:0:-1], half_type),
            pieces(volume), pieces(volume, 2), pieces(volume, 2), pieces(volume), pieces(classes, 2), pieces(2),
            wholes(2), wholes(2), wholes(2, kind=jnp.float32), wholes(2),
            pieces(classes, 2, 2), pieces(volume, 2), wholes(),
            pieces(), pieces(), pieces(), wide, wide, wide,
            *pair(volume, CHUNKS, 2), *pair(volume, CHUNKS, 2), *pair(2, 2), *pair(classes, 2), *pair(volume, 2),
            *pair(2), pltpu.SemaphoreType.DMA((4,)),
        ],
        compiler_params=pltpu.CompilerParams(
            collective_id=0, has_side_effects=True, vmem_limit_bytes=67043328
        ),
    )(green_blocks[0, 0], coulomb[0], couple_cols[0].T, couple_vals[0].T)
    return result[None, None]


def fused_grid(mesh):
    volume = mesh.shape["energy"]
    grid = math.isqrt(2 * volume)
    return grid if grid * grid == 2 * volume and grid % 2 == 0 else 0


def on_any(grid, green_blocks, coulomb, couple_cols, couple_vals):
    orbitals = green_blocks.shape[-1]
    fits = (
        grid > 2
        and green_blocks.shape[:2] == (1, 1)
        and orbitals % (128 * max(grid, 1)) == 0
        and couple_cols.shape[1] * grid == orbitals
        and lax.axis_size("slab") > 1
    )
    if fits:
        return fused_on_device(grid, green_blocks, coulomb, couple_cols, couple_vals)
    return on_device(green_blocks, coulomb, couple_cols, couple_vals)


def solution(mesh):
    return jax.shard_map(
        functools.partial(on_any, fused_grid(mesh)),
        mesh=mesh,
        in_specs=(
            P("energy", "slab", None, None),
            P("slab", None, None),
            P("slab", None, None),
            P("slab", None, None),
        ),
        out_specs=P("energy", "slab", None, None),
        check_vma=False,
    )
```

```python
import functools
import math

import jax
import jax.numpy as jnp
from jax import lax
from jax.experimental import pallas as pl
from jax.experimental.pallas import tpu as pltpu
from jax.sharding import PartitionSpec as P


def from_behind(x, axis, by):
    size = lax.axis_size(axis)
    pairs = [(i, i + by) for i in range(size) if 0 <= i + by < size]
    return lax.ppermute(x, axis, pairs)


def plain_dot(left, right):
    return jnp.dot(left, right, preferred_element_type=jnp.float32)


def split_parts(values):
    upper = values.astype(jnp.bfloat16)
    lower = (values - upper.astype(jnp.float32)).astype(jnp.bfloat16)
    return (upper, lower)


def coupling_matrix(column_ids, coupling_values):
    width = column_ids.shape[0]
    hits = column_ids[:, :, None] == jnp.arange(width, dtype=jnp.int32)[None, None, :]
    summed = jnp.sum(
        jnp.where(hits, coupling_values.astype(jnp.float32)[:, :, None], jnp.float32(0.0)), axis=1
    )
    return summed.astype(jnp.bfloat16)


def on_device(green_blocks, coulomb, couple_cols, couple_vals):
    own_green = green_blocks[:, 0]
    coulomb_block = coulomb[0]
    per_device = own_green.shape[0]
    orbitals = own_green.shape[1]
    volume = lax.axis_size("energy")
    energies = per_device * volume
    inv_root = 1.0 / math.sqrt(orbitals)
    flipped = jnp.swapaxes(own_green, 1, 2)
    received, flipped_recv = (
        lax.all_to_all(own_green, "energy", split_axis=1, concat_axis=0, tiled=True),
        lax.all_to_all(flipped, "energy", split_axis=1, concat_axis=0, tiled=True),
    )
    green_entries = received.reshape(energies, -1)
    flipped_entries = flipped_recv.reshape(energies, -1)
    entry_shape = received.shape
    halfway = energies // 2 + 1
    frequency = jnp.arange(halfway, dtype=jnp.int32)
    energy_index = jnp.arange(energies, dtype=jnp.int32)
    angles = (frequency[:, None] * energy_index[None, :] % energies).astype(jnp.float32) * (
        2.0 * math.pi / energies
    )
    cosine = jnp.cos(angles)
    sine = jnp.sin(angles)
    weights = (
        jnp.where((frequency == 0) | (2 * frequency == energies), 1.0, 2.0).astype(jnp.float32)
        / energies
    )
    forward_high, forward_low = split_parts(jnp.concatenate([cosine, -sine], axis=0))
    backward_table = jnp.concatenate(
        [cosine * weights[:, None], -sine * weights[:, None]], axis=0
    ).T
    backward_high, backward_low = split_parts(backward_table)

    def spectrum(entries):
        stacked = plain_dot(forward_high, entries) + plain_dot(forward_low, entries)
        return (stacked[:halfway], stacked[halfway:])

    def to_values(real_part, imag_part):
        data_high, data_low = split_parts(jnp.concatenate([real_part, imag_part], axis=0))
        return (
            plain_dot(backward_high, data_high)
            + plain_dot(backward_high, data_low)
            + plain_dot(backward_low, data_high)
        )

    green_real, green_imag = spectrum(green_entries)
    mirror_real, mirror_imag = spectrum(flipped_entries)
    polar_entries = to_values(
        green_real * mirror_real + green_imag * mirror_imag,
        green_imag * mirror_real - green_real * mirror_imag,
    )
    polar_entries = (polar_entries * (0.5 / math.sqrt(orbitals * energies))).astype(jnp.bfloat16)
    polar = lax.all_to_all(
        polar_entries.reshape(entry_shape), "energy", split_axis=0, concat_axis=1, tiled=True
    )
    inner = jnp.einsum(
        "ij,ejk->eik", coulomb_block, polar, preferred_element_type=jnp.float32
    ).astype(jnp.bfloat16)
    second = jnp.einsum("eij,jk->eik", inner, coulomb_block, preferred_element_type=jnp.float32)
    third = jnp.einsum(
        "eij,ejk->eik", inner, second.astype(jnp.bfloat16), preferred_element_type=jnp.float32
    )
    screened = (coulomb_block.astype(jnp.float32)[None] + second + third).astype(jnp.bfloat16)
    screened_entries = lax.all_to_all(
        screened, "energy", split_axis=1, concat_axis=0, tiled=True
    ).reshape(energies, -1)
    screen_real, screen_imag = spectrum(screened_entries)
    sigma_entries = to_values(
        green_real * screen_real - green_imag * screen_imag,
        green_real * screen_imag + green_imag * screen_real,
    )
    sigma_entries = (sigma_entries * (0.2 / math.sqrt(energies))).astype(jnp.bfloat16)
    sigma = lax.all_to_all(
        sigma_entries.reshape(entry_shape), "energy", split_axis=0, concat_axis=1, tiled=True
    )
    interface = couple_cols.shape[1]
    last = orbitals - interface
    coupling = coupling_matrix(couple_cols[0], couple_vals[0])
    prev_green, previous = from_behind((own_green, coupling), "slab", 1)
    next_green = from_behind(own_green, "slab", -1)
    prev_corner = prev_green[:, last:, last:]
    next_corner = next_green[:, :interface, :interface]
    near_next = jnp.einsum(
        "ij,ejk->eik", coupling, next_corner, preferred_element_type=jnp.float32
    ).astype(jnp.bfloat16)
    near_prev = jnp.einsum(
        "ji,ejk->eik", previous, prev_corner, preferred_element_type=jnp.float32
    ).astype(jnp.bfloat16)
    right_part = (
        jnp.einsum("eij,kj->eik", near_next, coupling, preferred_element_type=jnp.float32)
        * inv_root
    )
    left_part = (
        jnp.einsum("eij,jk->eik", near_prev, previous, preferred_element_type=jnp.float32)
        * inv_root
    )
    total = sigma.astype(jnp.float32)
    total = total.at[:, last:, last:].add(right_part)
    total = total.at[:, :interface, :interface].add(left_part)
    total_b = total.astype(jnp.bfloat16)
    dressed = jnp.einsum(
        "eij,ejk->eik", own_green, total_b, preferred_element_type=jnp.float32
    ).astype(jnp.bfloat16)
    updated = (
        own_green
        + jnp.einsum("eij,ejk->eik", dressed, own_green, preferred_element_type=jnp.float32)
        * inv_root
    )
    return updated.astype(jnp.bfloat16)[:, None]


MESH = pl.DeviceIdType.MESH


def unit_blocks(unit, grid):
    odd = grid - 1
    paired = grid * odd // 2
    slot = unit // odd
    turn = unit % odd
    diagonal = unit // paired
    first = (turn + slot) % odd
    second = (turn + odd - slot) % odd
    lone = 1 - (slot + odd - 1) // odd
    row = lone * odd + (1 - lone) * first
    col = lone * turn + (1 - lone) * second
    corner = 2 * (unit - paired)
    row0 = diagonal * corner + (1 - diagonal) * row
    col0 = diagonal * corner + (1 - diagonal) * col
    row1 = diagonal * (corner + 1) + (1 - diagonal) * col
    col1 = diagonal * (corner + 1) + (1 - diagonal) * row
    return ((row0, col0), (row1, col1))


CHUNKS = 2
SUBS = 2


def fused_kernel(
    volume, slabs, grid, scale_polar, scale_sigma, inv_root,
    green_hbm, coulomb_hbm, cols_hbm, vals_hbm, out,
    green, coulomb, cols, vals,
    stage, landed, mirror, second_half, polar_out, polar_more, matrix, inner, second, screened,
    screen_in, sigma_out, sigma,
    coupling, turned, next_corner, left_out, left_in, right_in,
    g_send, g_recv, p_send, p_recv, m_send, m_recv, w_send, w_recv, s_send, s_recv,
    slab_send, slab_recv, load_sem,
):
    loads = [
        pltpu.make_async_copy(source, target, load_sem.at[n])
        for n, (source, target) in enumerate(
            ((green_hbm, green), (coulomb_hbm, coulomb), (cols_hbm, cols), (vals_hbm, vals))
        )
    ]
    for load in loads:
        load.start()
    me = lax.axis_index("energy")
    slab = lax.axis_index("slab")
    size = green.shape[0] // grid
    last = green.shape[0] - size
    classes = volume // 2
    paired = grid * (grid - 1) // 2
    order = sorted(range(1, volume), key=lambda k: (-min(k, volume - k), k))
    has_prev = 1 - (slabs - 1 - slab + 0) // (slabs - 1)
    has_next = 1 - slab // (slabs - 1)
    diagonal = me // paired
    my_class = lax.rem(me, classes)
    first_mate = me - my_class
    own_blocks = unit_blocks(me, grid)
    chunk_rows = size // CHUNKS

    def peer_of(k):
        return lax.rem(me + k, volume)

    def from_of(k):
        return lax.rem(me + volume - k, volume)

    barrier = pltpu.get_barrier_semaphore()
    for k in range(1, volume):
        pl.semaphore_signal(barrier, inc=1, device_id=(peer_of(k), slab), device_id_type=MESH)

    @pl.when(slab > 0)
    def _():
        pl.semaphore_signal(barrier, inc=1, device_id=(me, slab - 1), device_id_type=MESH)

    @pl.when(slab < slabs - 1)
    def _():
        pl.semaphore_signal(barrier, inc=1, device_id=(me, slab + 1), device_id_type=MESH)

    def flipped(block):
        return block.astype(jnp.float32).T.astype(jnp.bfloat16)

    def region(coords, start=0, rows=None):
        rows = size if rows is None else rows
        row = pl.multiple_of(coords[0] * size + start, rows)
        col = pl.multiple_of(coords[1] * size, size)
        return pl.ds(row, rows), pl.ds(col, size)

    def block_of(ref, coords, start=0, rows=None):
        return ref.at[region(coords, start, rows)]

    def remote(src, dst, sends, recvs, device):
        return pltpu.make_async_remote_copy(
            src_ref=src, dst_ref=dst, send_sem=sends, recv_sem=recvs,
            device_id=(device, slab), device_id_type=MESH,
        )

    loads[0].wait()
    for unit in range(volume):
        coords = unit_blocks(unit, grid)[1]
        block = green[coords[0] * size:(coords[0] + 1) * size, coords[1] * size:(coords[1] + 1) * size]
        stage[unit] = block if unit >= paired else flipped(block)

    pl.semaphore_wait(barrier, volume - 1 + has_prev + has_next)

    def took(shape, sem):
        pltpu.make_async_copy(shape, shape, sem).wait()

    others = pl.ds(0, volume - 1)

    def span(chunk):
        return pl.ds(chunk * chunk_rows, chunk_rows)

    for chunk in range(CHUNKS):
        for slot in range(2):
            for k in order:
                peer = peer_of(k)
                coords = unit_blocks(peer, grid)[0]
                if slot == 0:
                    source = block_of(green, coords, chunk * chunk_rows, chunk_rows)
                else:
                    source = stage.at[peer, span(chunk)]
                remote(
                    source, landed.at[me, slot, span(chunk)], g_send.at[0], g_recv.at[k, chunk], peer
                ).start()
    landed[me, 0] = block_of(green, own_blocks[0])[...]
    landed[me, 1] = stage[me]

    corner_copy = pltpu.make_async_remote_copy(
        src_ref=green.at[pl.ds(0, size), pl.ds(0, size)], dst_ref=next_corner,
        send_sem=slab_send.at[0], recv_sem=slab_recv.at[0],
        device_id=(me, slab - has_prev), device_id_type=MESH,
    )
    left_copy = pltpu.make_async_remote_copy(
        src_ref=left_out, dst_ref=left_in,
        send_sem=slab_send.at[1], recv_sem=slab_recv.at[1],
        device_id=(me, slab + has_next), device_id_type=MESH,
    )

    @pl.when(slab > 0)
    def _():
        corner_copy.start()

    loads[2].wait()
    loads[3].wait()
    ids = cols[...]
    values = vals[...].astype(jnp.float32)
    columns = lax.broadcasted_iota(jnp.int32, (size, size), 0)
    summed = jnp.zeros((size, size), jnp.float32)
    for k in range(ids.shape[0]):
        summed += jnp.where(ids[k:k + 1, :] == columns, values[k:k + 1, :], jnp.float32(0.0))
    summed = summed.astype(jnp.bfloat16).astype(jnp.float32)
    turned[...] = summed.astype(jnp.bfloat16)
    coupling[...] = summed.T.astype(jnp.bfloat16)

    @pl.when(slab < slabs - 1)
    def _():
        near_prev = plain_dot(turned[...], green[last:, last:]).astype(jnp.bfloat16)
        left_out[...] = plain_dot(near_prev, coupling[...]) * inv_root
        left_copy.start()

    loads[1].wait()
    rows_at_once = 16
    steps = chunk_rows // rows_at_once

    def rows_of(step):
        return pl.ds(pl.multiple_of(step * rows_at_once, rows_at_once), rows_at_once)

    def correlation(mine, theirs, e):
        acc = mine[0] * theirs[(0 - e) % volume]
        for e2 in range(1, volume):
            acc += mine[e2] * theirs[(e2 - e) % volume]
        return (acc * scale_polar).astype(jnp.bfloat16)

    where = (
        (0, own_blocks[0]),
        (1 - diagonal, tuple(
            diagonal * d + (1 - diagonal) * o for d, o in zip(own_blocks[1], own_blocks[0])
        )),
    )

    def polar_copy(k, chunk, slot):
        peer = peer_of(k)
        index, coords = where[slot]
        return remote(
            polar_out.at[lax.rem(peer, classes), slot, span(chunk)],
            block_of(matrix.at[index], coords, chunk * chunk_rows, chunk_rows),
            p_send.at[0], p_recv.at[k], peer,
        )

    def send_polar(chunk):
        for slot in range(2):
            for k in order:
                polar_copy(k, chunk, slot).start()

    def more_copy(target, slot):
        return remote(
            polar_more.at[slot],
            block_of(matrix.at[1], own_blocks[slot]),
            m_send.at[0], m_recv.at[0], target * classes,
        )

    def green_arrived(k, chunk):
        took(landed.at[from_of(k), :, span(chunk)], g_recv.at[k, chunk])

    @pl.when(diagonal == 0)
    def _():
        for chunk in range(CHUNKS):
            for k in order:
                green_arrived(k, chunk)

            def correlate(step, carry):
                rows = rows_of(step)
                mine = [landed[e, 0, rows, :].astype(jnp.float32) for e in range(volume)]
                theirs = [landed[e, 1, rows, :].astype(jnp.float32) for e in range(volume)]
                for e in range(volume):
                    if e % classes == 0:
                        place = (0, e // classes)
                    else:
                        place = (min(e, volume - e), e // classes)
                    polar_out[place[0], place[1], rows, :] = correlation(mine, theirs, e)
                return carry

            lax.fori_loop(chunk * steps, (chunk + 1) * steps, correlate, 0)
            send_polar(chunk)

    @pl.when(diagonal == 1)
    def _():
        def flip_both(e):
            for slot in range(2):
                mirror[e, slot] = flipped(landed[e, slot])

        flip_both(me)
        for k in order:
            for chunk in range(CHUNKS):
                green_arrived(k, chunk)
            flip_both(from_of(k))

        for slot in range(2):
            def correlate(step, carry, slot=slot):
                rows = rows_of(step)
                mine = [landed[e, slot, rows, :].astype(jnp.float32) for e in range(volume)]
                theirs = [mirror[e, slot, rows, :].astype(jnp.float32) for e in range(volume)]
                for e in range(classes):
                    polar_out[e, slot, rows, :] = correlation(mine, theirs, e)
                polar_more[slot, rows, :] = correlation(mine, theirs, classes)
                return carry

            lax.fori_loop(0, size // rows_at_once, correlate, 0)
        for chunk in range(CHUNKS):
            send_polar(chunk)
        for target in range(2):
            for slot in range(2):
                more_copy(target, slot).start()

    for slot in range(2):
        index, coords = where[slot]
        block_of(matrix.at[index], coords)[...] = polar_out[my_class, slot]

    @pl.when(diagonal == 0)
    def _():
        for e in range(volume):
            second_half[e] = flipped(landed[e, 1])

    @pl.when(diagonal == 1)
    def _():
        for e in range(volume):
            second_half[e] = landed[e, 1]

    swapped = 1 - lax.rem(my_class + classes - 1, classes) // (classes - 1)

    def complete(unit):
        coords = unit_blocks(unit, grid)
        off = 1 - unit // paired

        @pl.when(off == 1)
        def _():
            for index in range(2):
                source = swapped * (1 - index) + (1 - swapped) * index
                block_of(matrix.at[index], coords[1])[...] = flipped(
                    block_of(matrix.at[source], coords[0])[...]
                )

        @pl.when(jnp.logical_and(off == 0, my_class > 0))
        def _():
            for slot in range(2):
                block_of(matrix.at[1], coords[slot])[...] = flipped(
                    block_of(matrix.at[0], coords[slot])[...]
                )

    complete(me)
    for k in order:
        took(polar_out.at[0], p_recv.at[k])
        complete(from_of(k))

    @pl.when(my_class == 0)
    def _():
        took(polar_out.at[pl.ds(0, volume - paired)], m_recv.at[0])

    for index in range(2):
        inner[index] = plain_dot(coulomb[...], matrix[index]).astype(jnp.bfloat16)
    for index in range(2):
        product = plain_dot(inner[index], coulomb[...])
        second[index] = product
        matrix[index] = product.astype(jnp.bfloat16)
    for index in range(2):
        third = plain_dot(inner[index], matrix[index])
        screened[index] = (coulomb[...].astype(jnp.float32) + second[index] + third).astype(jnp.bfloat16)

    parts = [(half, sub) for half in range(2) for sub in range(SUBS)]
    sub_rows = size // SUBS
    for half, sub in parts:
        for t in range(1, classes):
            mate = first_mate + lax.rem(my_class + t, classes)
            rows, width = region(unit_blocks(mate, grid)[half], sub * sub_rows, sub_rows)
            remote(
                screened.at[:, rows, width],
                screen_in.at[my_class, half, :, pl.ds(sub * sub_rows, sub_rows)],
                w_send.at[0], w_recv.at[half, sub], mate,
            ).start()
    for half in range(2):
        rows, width = region(own_blocks[half])
        screen_in[my_class, half] = screened[:, rows, width]

    def sigma_copy(half, sub, target):
        return remote(
            sigma_out.at[target, half, pl.ds(sub * sub_rows, sub_rows)],
            block_of(sigma, own_blocks[half], sub * sub_rows, sub_rows),
            s_send.at[0], s_recv.at[0], target,
        )

    def for_others(act):
        for other in range(volume):
            pl.when(me != other)(functools.partial(act, other))

    for half, sub in parts:
        took(
            screen_in.at[pl.ds(0, classes - 1), half, :, pl.ds(sub * sub_rows, sub_rows)],
            w_recv.at[half, sub],
        )

        def convolve(step, carry, half=half):
            rows = rows_of(step)
            if half == 0:
                mine = [landed[e, 0, rows, :].astype(jnp.float32) for e in range(volume)]
            else:
                mine = [second_half[e, rows, :].astype(jnp.float32) for e in range(volume)]
            waves = [
                screen_in[min(e, volume - e) % classes, half, e // classes, rows, :].astype(jnp.float32)
                for e in range(volume)
            ]
            for e in range(volume):
                acc = mine[0] * waves[e]
                for e2 in range(1, volume):
                    acc += mine[e2] * waves[(e - e2) % volume]
                sigma_out[e, half, rows, :] = (acc * scale_sigma).astype(jnp.bfloat16)
            return carry

        lax.fori_loop(sub * sub_rows // rows_at_once, (sub + 1) * sub_rows // rows_at_once, convolve, 0)
        for_others(lambda target: sigma_copy(half, sub, target).start())
    for half in range(2):
        block_of(sigma, own_blocks[half])[...] = sigma_out[me, half]

    @pl.when(slab < slabs - 1)
    def _():
        corner_copy.wait_recv()
        near_next = plain_dot(coupling[...], next_corner[...]).astype(jnp.bfloat16)
        right_in[...] = plain_dot(near_next, turned[...]) * inv_root

    took(landed.at[others], s_recv.at[0])

    @pl.when(slab < slabs - 1)
    def _():
        sigma[last:, last:] = (sigma[last:, last:].astype(jnp.float32) + right_in[...]).astype(jnp.bfloat16)
        left_copy.wait_send()

    @pl.when(slab > 0)
    def _():
        left_copy.wait_recv()
        sigma[:size, :size] = (sigma[:size, :size].astype(jnp.float32) + left_in[...]).astype(jnp.bfloat16)
        corner_copy.wait_send()

    inner[0] = plain_dot(green[...], sigma[...]).astype(jnp.bfloat16)
    updated = green[...].astype(jnp.float32) + plain_dot(inner[0], green[...]) * inv_root
    out[...] = updated.astype(jnp.bfloat16)
    took(landed.at[others], g_send.at[0])
    took(landed.at[others], p_send.at[0])
    took(screen_in.at[pl.ds(0, classes - 1)], w_send.at[0])
    took(landed.at[others], s_send.at[0])

    @pl.when(diagonal == 1)
    def _():
        took(polar_out.at[pl.ds(0, 2)], m_send.at[0])


def fused_on_device(grid, green_blocks, coulomb, couple_cols, couple_vals):
    volume = lax.axis_size("energy")
    slabs = lax.axis_size("slab")
    orbitals = green_blocks.shape[-1]
    size = orbitals // grid
    half_type = jnp.bfloat16

    def pieces(*lead):
        return pltpu.VMEM((*lead, size, size), half_type)

    def wholes(*lead, kind=half_type):
        return pltpu.VMEM((*lead, orbitals, orbitals), kind)

    def pair(sends, recvs):
        return [pltpu.SemaphoreType.DMA(sends), pltpu.SemaphoreType.DMA(recvs)]

    wide = pltpu.VMEM((size, size), jnp.float32)
    classes = volume // 2
    result = pl.pallas_call(
        functools.partial(
            fused_kernel, volume, slabs, grid,
            0.5 / math.sqrt(orbitals * volume), 0.2 / math.sqrt(volume), 1.0 / math.sqrt(orbitals),
        ),
        out_shape=jax.ShapeDtypeStruct((orbitals, orbitals), half_type),
        in_specs=[pl.BlockSpec(memory_space=pltpu.HBM)] * 4,
        out_specs=pl.BlockSpec(memory_space=pltpu.VMEM),
        scratch_shapes=[
            wholes(), wholes(), pltpu.VMEM(couple_cols.shape[:0:-1], jnp.int32), pltpu.VMEM(couple_vals.shape[:0:-1], half_type),
            pieces(volume), pieces(volume, 2), pieces(volume, 2), pieces(volume), pieces(classes, 2), pieces(2),
            wholes(2), wholes(2), wholes(2, kind=jnp.float32), wholes(2),
            pieces(classes, 2, 2), pieces(volume, 2), wholes(),
            pieces(), pieces(), pieces(), wide, wide, wide,
            *pair((1,), (volume, CHUNKS)), *pair((1,), (volume,)), *pair((1,), (1,)),
            *pair((1,), (2, SUBS)), *pair((1,), (1,)), *pair((2,), (2,)), pltpu.SemaphoreType.DMA((4,)),
        ],
        compiler_params=pltpu.CompilerParams(
            collective_id=0, has_side_effects=True, vmem_limit_bytes=67043328
        ),
    )(green_blocks[0, 0], coulomb[0], couple_cols[0].T, couple_vals[0].T)
    return result[None, None]


def fused_grid(mesh):
    volume = mesh.shape["energy"]
    grid = math.isqrt(2 * volume)
    return grid if grid * grid == 2 * volume and grid % 2 == 0 else 0


def on_any(grid, green_blocks, coulomb, couple_cols, couple_vals):
    orbitals = green_blocks.shape[-1]
    fits = (
        grid > 2
        and green_blocks.shape[:2] == (1, 1)
        and orbitals % (128 * max(grid, 1)) == 0
        and couple_cols.shape[1] * grid == orbitals
        and lax.axis_size("slab") > 1
    )
    if fits:
        return fused_on_device(grid, green_blocks, coulomb, couple_cols, couple_vals)
    return on_device(green_blocks, coulomb, couple_cols, couple_vals)


def solution(mesh):
    return jax.shard_map(
        functools.partial(on_any, fused_grid(mesh)),
        mesh=mesh,
        in_specs=(
            P("energy", "slab", None, None),
            P("slab", None, None),
            P("slab", None, None),
            P("slab", None, None),
        ),
        out_specs=P("energy", "slab", None, None),
        check_vma=False,
    )
```

```python
import functools
import math

import jax
import jax.numpy as jnp
from jax import lax
from jax.experimental import pallas as pl
from jax.experimental.pallas import tpu as pltpu
from jax.sharding import PartitionSpec as P


def from_behind(x, axis, by):
    size = lax.axis_size(axis)
    pairs = [(i, i + by) for i in range(size) if 0 <= i + by < size]
    return lax.ppermute(x, axis, pairs)


def plain_dot(left, right):
    return jnp.dot(left, right, preferred_element_type=jnp.float32)


def split_parts(values):
    upper = values.astype(jnp.bfloat16)
    lower = (values - upper.astype(jnp.float32)).astype(jnp.bfloat16)
    return (upper, lower)


def coupling_matrix(column_ids, coupling_values):
    width = column_ids.shape[0]
    hits = column_ids[:, :, None] == jnp.arange(width, dtype=jnp.int32)[None, None, :]
    summed = jnp.sum(
        jnp.where(hits, coupling_values.astype(jnp.float32)[:, :, None], jnp.float32(0.0)), axis=1
    )
    return summed.astype(jnp.bfloat16)


def on_device(green_blocks, coulomb, couple_cols, couple_vals):
    own_green = green_blocks[:, 0]
    coulomb_block = coulomb[0]
    per_device = own_green.shape[0]
    orbitals = own_green.shape[1]
    volume = lax.axis_size("energy")
    energies = per_device * volume
    inv_root = 1.0 / math.sqrt(orbitals)
    flipped = jnp.swapaxes(own_green, 1, 2)
    received, flipped_recv = (
        lax.all_to_all(own_green, "energy", split_axis=1, concat_axis=0, tiled=True),
        lax.all_to_all(flipped, "energy", split_axis=1, concat_axis=0, tiled=True),
    )
    green_entries = received.reshape(energies, -1)
    flipped_entries = flipped_recv.reshape(energies, -1)
    entry_shape = received.shape
    halfway = energies // 2 + 1
    frequency = jnp.arange(halfway, dtype=jnp.int32)
    energy_index = jnp.arange(energies, dtype=jnp.int32)
    angles = (frequency[:, None] * energy_index[None, :] % energies).astype(jnp.float32) * (
        2.0 * math.pi / energies
    )
    cosine = jnp.cos(angles)
    sine = jnp.sin(angles)
    weights = (
        jnp.where((frequency == 0) | (2 * frequency == energies), 1.0, 2.0).astype(jnp.float32)
        / energies
    )
    forward_high, forward_low = split_parts(jnp.concatenate([cosine, -sine], axis=0))
    backward_table = jnp.concatenate(
        [cosine * weights[:, None], -sine * weights[:, None]], axis=0
    ).T
    backward_high, backward_low = split_parts(backward_table)

    def spectrum(entries):
        stacked = plain_dot(forward_high, entries) + plain_dot(forward_low, entries)
        return (stacked[:halfway], stacked[halfway:])

    def to_values(real_part, imag_part):
        data_high, data_low = split_parts(jnp.concatenate([real_part, imag_part], axis=0))
        return (
            plain_dot(backward_high, data_high)
            + plain_dot(backward_high, data_low)
            + plain_dot(backward_low, data_high)
        )

    green_real, green_imag = spectrum(green_entries)
    mirror_real, mirror_imag = spectrum(flipped_entries)
    polar_entries = to_values(
        green_real * mirror_real + green_imag * mirror_imag,
        green_imag * mirror_real - green_real * mirror_imag,
    )
    polar_entries = (polar_entries * (0.5 / math.sqrt(orbitals * energies))).astype(jnp.bfloat16)
    polar = lax.all_to_all(
        polar_entries.reshape(entry_shape), "energy", split_axis=0, concat_axis=1, tiled=True
    )
    inner = jnp.einsum(
        "ij,ejk->eik", coulomb_block, polar, preferred_element_type=jnp.float32
    ).astype(jnp.bfloat16)
    second = jnp.einsum("eij,jk->eik", inner, coulomb_block, preferred_element_type=jnp.float32)
    third = jnp.einsum(
        "eij,ejk->eik", inner, second.astype(jnp.bfloat16), preferred_element_type=jnp.float32
    )
    screened = (coulomb_block.astype(jnp.float32)[None] + second + third).astype(jnp.bfloat16)
    screened_entries = lax.all_to_all(
        screened, "energy", split_axis=1, concat_axis=0, tiled=True
    ).reshape(energies, -1)
    screen_real, screen_imag = spectrum(screened_entries)
    sigma_entries = to_values(
        green_real * screen_real - green_imag * screen_imag,
        green_real * screen_imag + green_imag * screen_real,
    )
    sigma_entries = (sigma_entries * (0.2 / math.sqrt(energies))).astype(jnp.bfloat16)
    sigma = lax.all_to_all(
        sigma_entries.reshape(entry_shape), "energy", split_axis=0, concat_axis=1, tiled=True
    )
    interface = couple_cols.shape[1]
    last = orbitals - interface
    coupling = coupling_matrix(couple_cols[0], couple_vals[0])
    prev_green, previous = from_behind((own_green, coupling), "slab", 1)
    next_green = from_behind(own_green, "slab", -1)
    prev_corner = prev_green[:, last:, last:]
    next_corner = next_green[:, :interface, :interface]
    near_next = jnp.einsum(
        "ij,ejk->eik", coupling, next_corner, preferred_element_type=jnp.float32
    ).astype(jnp.bfloat16)
    near_prev = jnp.einsum(
        "ji,ejk->eik", previous, prev_corner, preferred_element_type=jnp.float32
    ).astype(jnp.bfloat16)
    right_part = (
        jnp.einsum("eij,kj->eik", near_next, coupling, preferred_element_type=jnp.float32)
        * inv_root
    )
    left_part = (
        jnp.einsum("eij,jk->eik", near_prev, previous, preferred_element_type=jnp.float32)
        * inv_root
    )
    total = sigma.astype(jnp.float32)
    total = total.at[:, last:, last:].add(right_part)
    total = total.at[:, :interface, :interface].add(left_part)
    total_b = total.astype(jnp.bfloat16)
    dressed = jnp.einsum(
        "eij,ejk->eik", own_green, total_b, preferred_element_type=jnp.float32
    ).astype(jnp.bfloat16)
    updated = (
        own_green
        + jnp.einsum("eij,ejk->eik", dressed, own_green, preferred_element_type=jnp.float32)
        * inv_root
    )
    return updated.astype(jnp.bfloat16)[:, None]


MESH = pl.DeviceIdType.MESH


def unit_blocks(unit, grid):
    odd = grid - 1
    paired = grid * odd // 2
    slot = unit // odd
    turn = unit % odd
    diagonal = unit // paired
    first = (turn + slot) % odd
    second = (turn + odd - slot) % odd
    lone = 1 - (slot + odd - 1) // odd
    row = lone * odd + (1 - lone) * first
    col = lone * turn + (1 - lone) * second
    corner = 2 * (unit - paired)
    row0 = diagonal * corner + (1 - diagonal) * row
    col0 = diagonal * corner + (1 - diagonal) * col
    row1 = diagonal * (corner + 1) + (1 - diagonal) * col
    col1 = diagonal * (corner + 1) + (1 - diagonal) * row
    return ((row0, col0), (row1, col1))


CHUNKS = 2
GREEN_AHEAD = 2
POLAR_AHEAD = 2
SUBS = 2


def fused_kernel(
    volume, slabs, grid, scale_polar, scale_sigma, inv_root,
    green_hbm, coulomb_hbm, cols_hbm, vals_hbm, sigma, green,
    coulomb, cols, vals,
    stage, landed, mirror, second_half, polar_out, polar_more, matrix, inner, second, screened,
    screen_in, sigma_out,
    coupling, turned, next_corner, left_out, left_in, right_in,
    g_send, g_recv, p_send, p_recv, m_send, m_recv, w_send, w_recv, s_send, s_recv,
    slab_send, slab_recv, load_sem, turn,
):
    loads = [
        pltpu.make_async_copy(source, target, load_sem.at[n])
        for n, (source, target) in enumerate(
            ((green_hbm, green), (coulomb_hbm, coulomb), (cols_hbm, cols), (vals_hbm, vals))
        )
    ]
    for load in loads:
        load.start()
    me = lax.axis_index("energy")
    slab = lax.axis_index("slab")
    size = green.shape[0] // grid
    last = green.shape[0] - size
    classes = volume // 2
    paired = grid * (grid - 1) // 2
    order = sorted(range(1, volume), key=lambda k: (-min(k, volume - k), k))
    has_prev = 1 - (slabs - 1 - slab + 0) // (slabs - 1)
    has_next = 1 - slab // (slabs - 1)
    diagonal = me // paired
    my_class = lax.rem(me, classes)
    first_mate = me - my_class
    own_blocks = unit_blocks(me, grid)
    chunk_rows = size // CHUNKS

    def peer_of(k):
        return lax.rem(me + k, volume)

    def from_of(k):
        return lax.rem(me + volume - k, volume)

    barrier = pltpu.get_barrier_semaphore()
    for k in range(1, volume):
        pl.semaphore_signal(barrier, inc=1, device_id=(peer_of(k), slab), device_id_type=MESH)

    @pl.when(slab > 0)
    def _():
        pl.semaphore_signal(barrier, inc=1, device_id=(me, slab - 1), device_id_type=MESH)

    @pl.when(slab < slabs - 1)
    def _():
        pl.semaphore_signal(barrier, inc=1, device_id=(me, slab + 1), device_id_type=MESH)

    def flipped(block):
        return block.astype(jnp.float32).T.astype(jnp.bfloat16)

    def region(coords, start=0, rows=None):
        rows = size if rows is None else rows
        row = pl.multiple_of(coords[0] * size + start, rows)
        col = pl.multiple_of(coords[1] * size, size)
        return pl.ds(row, rows), pl.ds(col, size)

    def block_of(ref, coords, start=0, rows=None):
        return ref.at[region(coords, start, rows)]

    def remote(src, dst, sends, recvs, device):
        return pltpu.make_async_remote_copy(
            src_ref=src, dst_ref=dst, send_sem=sends, recv_sem=recvs,
            device_id=(device, slab), device_id_type=MESH,
        )

    loads[0].wait()
    for unit in range(volume):
        coords = unit_blocks(unit, grid)[1]
        block = green[coords[0] * size:(coords[0] + 1) * size, coords[1] * size:(coords[1] + 1) * size]
        stage[unit] = block if unit >= paired else flipped(block)

    pl.semaphore_wait(barrier, volume - 1 + has_prev + has_next)

    def took(shape, sem):
        pltpu.make_async_copy(shape, shape, sem).wait()

    others = pl.ds(0, volume - 1)

    def span(chunk):
        return pl.ds(chunk * chunk_rows, chunk_rows)

    for chunk in range(CHUNKS):
        for slot in range(2):
            for k in order:
                peer = peer_of(k)
                coords = unit_blocks(peer, grid)[0]
                if slot == 0:
                    source = block_of(green, coords, chunk * chunk_rows, chunk_rows)
                else:
                    source = stage.at[peer, span(chunk)]
                remote(
                    source, landed.at[me, slot, span(chunk)], g_send.at[chunk], g_recv.at[k, chunk], peer
                ).start()
    landed[me, 0] = block_of(green, own_blocks[0])[...]
    landed[me, 1] = stage[me]

    corner_copy = pltpu.make_async_remote_copy(
        src_ref=green.at[pl.ds(0, size), pl.ds(0, size)], dst_ref=next_corner,
        send_sem=slab_send.at[0], recv_sem=slab_recv.at[0],
        device_id=(me, slab - has_prev), device_id_type=MESH,
    )
    left_copy = pltpu.make_async_remote_copy(
        src_ref=left_out, dst_ref=left_in,
        send_sem=slab_send.at[1], recv_sem=slab_recv.at[1],
        device_id=(me, slab + has_next), device_id_type=MESH,
    )

    @pl.when(slab > 0)
    def _():
        corner_copy.start()

    loads[2].wait()
    loads[3].wait()
    ids = cols[...]
    values = vals[...].astype(jnp.float32)
    columns = lax.broadcasted_iota(jnp.int32, (size, size), 0)
    summed = jnp.zeros((size, size), jnp.float32)
    for k in range(ids.shape[0]):
        summed += jnp.where(ids[k:k + 1, :] == columns, values[k:k + 1, :], jnp.float32(0.0))
    summed = summed.astype(jnp.bfloat16).astype(jnp.float32)
    turned[...] = summed.astype(jnp.bfloat16)
    coupling[...] = summed.T.astype(jnp.bfloat16)

    @pl.when(slab < slabs - 1)
    def _():
        near_prev = plain_dot(turned[...], green[last:, last:]).astype(jnp.bfloat16)
        left_out[...] = plain_dot(near_prev, coupling[...]) * inv_root
        left_copy.start()

    second_core = lax.rem(slab, 2)

    @pl.when(second_core == 0)
    def _():
        for chunk in range(GREEN_AHEAD):
            took(landed.at[others, :, span(chunk)], g_send.at[chunk])
        pl.semaphore_signal(turn.at[0], inc=1, device_id=(me, slab + 1), device_id_type=MESH)

    loads[1].wait()
    rows_at_once = 16
    steps = chunk_rows // rows_at_once

    def rows_of(step):
        return pl.ds(pl.multiple_of(step * rows_at_once, rows_at_once), rows_at_once)

    def correlation(mine, theirs, e):
        acc = mine[0] * theirs[(0 - e) % volume]
        for e2 in range(1, volume):
            acc += mine[e2] * theirs[(e2 - e) % volume]
        return (acc * scale_polar).astype(jnp.bfloat16)

    where = (
        (0, own_blocks[0]),
        (1 - diagonal, tuple(
            diagonal * d + (1 - diagonal) * o for d, o in zip(own_blocks[1], own_blocks[0])
        )),
    )

    def polar_copy(k, chunk, slot):
        peer = peer_of(k)
        index, coords = where[slot]
        return remote(
            polar_out.at[lax.rem(peer, classes), slot, span(chunk)],
            block_of(matrix.at[index], coords, chunk * chunk_rows, chunk_rows),
            p_send.at[chunk], p_recv.at[k], peer,
        )

    def send_polar(chunk):
        if chunk == 0:
            pl.semaphore_wait(turn.at[0], 1)
        for slot in range(2):
            for k in order:
                polar_copy(k, chunk, slot).start()

    def more_copy(target, slot):
        return remote(
            polar_more.at[slot],
            block_of(matrix.at[1], own_blocks[slot]),
            m_send.at[0], m_recv.at[0], target * classes,
        )

    def green_arrived(k, chunk):
        took(landed.at[from_of(k), :, span(chunk)], g_recv.at[k, chunk])

    @pl.when(diagonal == 0)
    def _():
        for chunk in range(CHUNKS):
            for k in order:
                green_arrived(k, chunk)

            def correlate(step, carry):
                rows = rows_of(step)
                mine = [landed[e, 0, rows, :].astype(jnp.float32) for e in range(volume)]
                theirs = [landed[e, 1, rows, :].astype(jnp.float32) for e in range(volume)]
                for e in range(volume):
                    if e % classes == 0:
                        place = (0, e // classes)
                    else:
                        place = (min(e, volume - e), e // classes)
                    polar_out[place[0], place[1], rows, :] = correlation(mine, theirs, e)
                return carry

            lax.fori_loop(chunk * steps, (chunk + 1) * steps, correlate, 0)
            send_polar(chunk)

    @pl.when(diagonal == 1)
    def _():
        def flip_both(e):
            for slot in range(2):
                mirror[e, slot] = flipped(landed[e, slot])

        flip_both(me)
        for k in order:
            for chunk in range(CHUNKS):
                green_arrived(k, chunk)
            flip_both(from_of(k))

        for slot in range(2):
            def correlate(step, carry, slot=slot):
                rows = rows_of(step)
                mine = [landed[e, slot, rows, :].astype(jnp.float32) for e in range(volume)]
                theirs = [mirror[e, slot, rows, :].astype(jnp.float32) for e in range(volume)]
                for e in range(classes):
                    polar_out[e, slot, rows, :] = correlation(mine, theirs, e)
                polar_more[slot, rows, :] = correlation(mine, theirs, classes)
                return carry

            lax.fori_loop(0, size // rows_at_once, correlate, 0)
        for chunk in range(CHUNKS):
            send_polar(chunk)
        for target in range(2):
            for slot in range(2):
                more_copy(target, slot).start()

    for slot in range(2):
        index, coords = where[slot]
        block_of(matrix.at[index], coords)[...] = polar_out[my_class, slot]

    @pl.when(diagonal == 0)
    def _():
        for e in range(volume):
            second_half[e] = flipped(landed[e, 1])

    @pl.when(diagonal == 1)
    def _():
        for e in range(volume):
            second_half[e] = landed[e, 1]

    @pl.when(second_core == 1)
    def _():
        for chunk in range(POLAR_AHEAD):
            took(landed.at[others, :, span(chunk)], p_send.at[chunk])
        pl.semaphore_signal(turn.at[0], inc=1, device_id=(me, slab - 1), device_id_type=MESH)

    swapped = 1 - lax.rem(my_class + classes - 1, classes) // (classes - 1)

    def complete(unit):
        coords = unit_blocks(unit, grid)
        off = 1 - unit // paired

        @pl.when(off == 1)
        def _():
            for index in range(2):
                source = swapped * (1 - index) + (1 - swapped) * index
                block_of(matrix.at[index], coords[1])[...] = flipped(
                    block_of(matrix.at[source], coords[0])[...]
                )

        @pl.when(jnp.logical_and(off == 0, my_class > 0))
        def _():
            for slot in range(2):
                block_of(matrix.at[1], coords[slot])[...] = flipped(
                    block_of(matrix.at[0], coords[slot])[...]
                )

    complete(me)
    for k in order:
        took(polar_out.at[0], p_recv.at[k])
        complete(from_of(k))

    @pl.when(my_class == 0)
    def _():
        took(polar_out.at[pl.ds(0, volume - paired)], m_recv.at[0])

    for index in range(2):
        inner[index] = plain_dot(coulomb[...], matrix[index]).astype(jnp.bfloat16)
    for index in range(2):
        product = plain_dot(inner[index], coulomb[...])
        second[index] = product
        matrix[index] = product.astype(jnp.bfloat16)
    for index in range(2):
        third = plain_dot(inner[index], matrix[index])
        screened[index] = (coulomb[...].astype(jnp.float32) + second[index] + third).astype(jnp.bfloat16)

    parts = [(half, sub) for half in range(2) for sub in range(SUBS)]
    sub_rows = size // SUBS
    for half, sub in parts:
        for t in range(1, classes):
            mate = first_mate + lax.rem(my_class + t, classes)
            rows, width = region(unit_blocks(mate, grid)[half], sub * sub_rows, sub_rows)
            remote(
                screened.at[:, rows, width],
                screen_in.at[my_class, half, :, pl.ds(sub * sub_rows, sub_rows)],
                w_send.at[0], w_recv.at[half, sub], mate,
            ).start()
    for half in range(2):
        rows, width = region(own_blocks[half])
        screen_in[my_class, half] = screened[:, rows, width]

    def sigma_copy(half, sub, target):
        return remote(
            sigma_out.at[target, half, pl.ds(sub * sub_rows, sub_rows)],
            block_of(sigma, own_blocks[half], sub * sub_rows, sub_rows),
            s_send.at[0], s_recv.at[0], target,
        )

    def for_others(act):
        for other in range(volume):
            pl.when(me != other)(functools.partial(act, other))

    for half, sub in parts:
        took(
            screen_in.at[pl.ds(0, classes - 1), half, :, pl.ds(sub * sub_rows, sub_rows)],
            w_recv.at[half, sub],
        )

        def convolve(step, carry, half=half):
            rows = rows_of(step)
            if half == 0:
                mine = [landed[e, 0, rows, :].astype(jnp.float32) for e in range(volume)]
            else:
                mine = [second_half[e, rows, :].astype(jnp.float32) for e in range(volume)]
            waves = [
                screen_in[min(e, volume - e) % classes, half, e // classes, rows, :].astype(jnp.float32)
                for e in range(volume)
            ]
            for e in range(volume):
                acc = mine[0] * waves[e]
                for e2 in range(1, volume):
                    acc += mine[e2] * waves[(e - e2) % volume]
                sigma_out[e, half, rows, :] = (acc * scale_sigma).astype(jnp.bfloat16)
            return carry

        lax.fori_loop(sub * sub_rows // rows_at_once, (sub + 1) * sub_rows // rows_at_once, convolve, 0)
        for_others(lambda target: sigma_copy(half, sub, target).start())
    for half in range(2):
        block_of(sigma, own_blocks[half])[...] = sigma_out[me, half]

    @pl.when(slab < slabs - 1)
    def _():
        corner_copy.wait_recv()
        near_next = plain_dot(coupling[...], next_corner[...]).astype(jnp.bfloat16)
        right_in[...] = plain_dot(near_next, turned[...]) * inv_root

    took(landed.at[others], s_recv.at[0])

    @pl.when(slab < slabs - 1)
    def _():
        sigma[last:, last:] = (sigma[last:, last:].astype(jnp.float32) + right_in[...]).astype(jnp.bfloat16)
        left_copy.wait_send()

    @pl.when(slab > 0)
    def _():
        left_copy.wait_recv()
        sigma[:size, :size] = (sigma[:size, :size].astype(jnp.float32) + left_in[...]).astype(jnp.bfloat16)
        corner_copy.wait_send()

    for chunk in range(CHUNKS):
        @pl.when(second_core + (chunk >= GREEN_AHEAD) > 0)
        def _():
            took(landed.at[others, :, span(chunk)], g_send.at[chunk])

        @pl.when(1 - second_core + (chunk >= POLAR_AHEAD) > 0)
        def _():
            took(landed.at[others, :, span(chunk)], p_send.at[chunk])

    took(screen_in.at[pl.ds(0, classes - 1)], w_send.at[0])
    took(landed.at[others], s_send.at[0])

    @pl.when(diagonal == 1)
    def _():
        took(polar_out.at[pl.ds(0, 2)], m_send.at[0])


def dress_kernel(inv_root, total, green, out):
    dressed = plain_dot(green[...], total[...]).astype(jnp.bfloat16)
    updated = green[...].astype(jnp.float32) + plain_dot(dressed, green[...]) * inv_root
    out[...] = updated.astype(jnp.bfloat16)


def fused_on_device(grid, green_blocks, coulomb, couple_cols, couple_vals):
    volume = lax.axis_size("energy")
    slabs = lax.axis_size("slab")
    orbitals = green_blocks.shape[-1]
    size = orbitals // grid
    half_type = jnp.bfloat16

    def pieces(*lead):
        return pltpu.VMEM((*lead, size, size), half_type)

    def wholes(*lead, kind=half_type):
        return pltpu.VMEM((*lead, orbitals, orbitals), kind)

    def pair(sends, recvs):
        return [pltpu.SemaphoreType.DMA(sends), pltpu.SemaphoreType.DMA(recvs)]

    wide = pltpu.VMEM((size, size), jnp.float32)
    classes = volume // 2
    inv_root = 1.0 / math.sqrt(orbitals)
    in_vmem = pl.BlockSpec(memory_space=pltpu.VMEM)
    total, green = pl.pallas_call(
        functools.partial(
            fused_kernel, volume, slabs, grid,
            0.5 / math.sqrt(orbitals * volume), 0.2 / math.sqrt(volume), inv_root,
        ),
        out_shape=[jax.ShapeDtypeStruct((orbitals, orbitals), half_type)] * 2,
        in_specs=[pl.BlockSpec(memory_space=pltpu.HBM)] * 4,
        out_specs=[in_vmem] * 2,
        scratch_shapes=[
            wholes(), pltpu.VMEM(couple_cols.shape[:0:-1], jnp.int32), pltpu.VMEM(couple_vals.shape[:0:-1], half_type),
            pieces(volume), pieces(volume, 2), pieces(volume, 2), pieces(volume), pieces(classes, 2), pieces(2),
            wholes(2), wholes(2), wholes(2, kind=jnp.float32), wholes(2),
            pieces(classes, 2, 2), pieces(volume, 2),
            pieces(), pieces(), pieces(), wide, wide, wide,
            *pair((CHUNKS,), (volume, CHUNKS)), *pair((CHUNKS,), (volume,)), *pair((1,), (1,)),
            *pair((1,), (2, SUBS)), *pair((1,), (1,)), *pair((2,), (2,)), pltpu.SemaphoreType.DMA((4,)),
            pltpu.SemaphoreType.REGULAR((2,)),
        ],
        compiler_params=pltpu.CompilerParams(
            collective_id=0, has_side_effects=True, vmem_limit_bytes=32 << 20
        ),
    )(*(
        pltpu.with_memory_space_constraint(array, pltpu.HBM)
        for array in (green_blocks[0, 0], coulomb[0], couple_cols[0].T, couple_vals[0].T)
    ))
    result = pl.pallas_call(
        functools.partial(dress_kernel, inv_root),
        out_shape=jax.ShapeDtypeStruct((orbitals, orbitals), half_type),
        in_specs=[in_vmem] * 2,
        out_specs=in_vmem,
        compiler_params=pltpu.CompilerParams(vmem_limit_bytes=16 << 20),
    )(total, green)
    return result[None, None]


def fused_grid(mesh):
    volume = mesh.shape["energy"]
    grid = math.isqrt(2 * volume)
    return grid if grid * grid == 2 * volume and grid % 2 == 0 else 0


def on_any(grid, green_blocks, coulomb, couple_cols, couple_vals):
    orbitals = green_blocks.shape[-1]
    fits = (
        grid > 2
        and green_blocks.shape[:2] == (1, 1)
        and orbitals % (128 * max(grid, 1)) == 0
        and couple_cols.shape[1] * grid == orbitals
        and lax.axis_size("slab") % 2 == 0
    )
    if fits:
        return fused_on_device(grid, green_blocks, coulomb, couple_cols, couple_vals)
    return on_device(green_blocks, coulomb, couple_cols, couple_vals)


def solution(mesh):
    return jax.shard_map(
        functools.partial(on_any, fused_grid(mesh)),
        mesh=mesh,
        in_specs=(
            P("energy", "slab", None, None),
            P("slab", None, None),
            P("slab", None, None),
            P("slab", None, None),
        ),
        out_specs=P("energy", "slab", None, None),
        check_vma=False,
    )
```

```python
import functools
import math

import jax
import jax.numpy as jnp
from jax import lax
from jax.experimental import pallas as pl
from jax.experimental.pallas import tpu as pltpu
from jax.sharding import PartitionSpec as P


def from_behind(x, axis, by):
    size = lax.axis_size(axis)
    pairs = [(i, i + by) for i in range(size) if 0 <= i + by < size]
    return lax.ppermute(x, axis, pairs)


def plain_dot(left, right):
    return jnp.dot(left, right, preferred_element_type=jnp.float32)


def split_parts(values):
    upper = values.astype(jnp.bfloat16)
    lower = (values - upper.astype(jnp.float32)).astype(jnp.bfloat16)
    return (upper, lower)


def coupling_matrix(column_ids, coupling_values):
    width = column_ids.shape[0]
    hits = column_ids[:, :, None] == jnp.arange(width, dtype=jnp.int32)[None, None, :]
    summed = jnp.sum(
        jnp.where(hits, coupling_values.astype(jnp.float32)[:, :, None], jnp.float32(0.0)), axis=1
    )
    return summed.astype(jnp.bfloat16)


def on_device(green_blocks, coulomb, couple_cols, couple_vals):
    own_green = green_blocks[:, 0]
    coulomb_block = coulomb[0]
    per_device = own_green.shape[0]
    orbitals = own_green.shape[1]
    volume = lax.axis_size("energy")
    energies = per_device * volume
    inv_root = 1.0 / math.sqrt(orbitals)
    flipped = jnp.swapaxes(own_green, 1, 2)
    received, flipped_recv = (
        lax.all_to_all(own_green, "energy", split_axis=1, concat_axis=0, tiled=True),
        lax.all_to_all(flipped, "energy", split_axis=1, concat_axis=0, tiled=True),
    )
    green_entries = received.reshape(energies, -1)
    flipped_entries = flipped_recv.reshape(energies, -1)
    entry_shape = received.shape
    halfway = energies // 2 + 1
    frequency = jnp.arange(halfway, dtype=jnp.int32)
    energy_index = jnp.arange(energies, dtype=jnp.int32)
    angles = (frequency[:, None] * energy_index[None, :] % energies).astype(jnp.float32) * (
        2.0 * math.pi / energies
    )
    cosine = jnp.cos(angles)
    sine = jnp.sin(angles)
    weights = (
        jnp.where((frequency == 0) | (2 * frequency == energies), 1.0, 2.0).astype(jnp.float32)
        / energies
    )
    forward_high, forward_low = split_parts(jnp.concatenate([cosine, -sine], axis=0))
    backward_table = jnp.concatenate(
        [cosine * weights[:, None], -sine * weights[:, None]], axis=0
    ).T
    backward_high, backward_low = split_parts(backward_table)

    def spectrum(entries):
        stacked = plain_dot(forward_high, entries) + plain_dot(forward_low, entries)
        return (stacked[:halfway], stacked[halfway:])

    def to_values(real_part, imag_part):
        data_high, data_low = split_parts(jnp.concatenate([real_part, imag_part], axis=0))
        return (
            plain_dot(backward_high, data_high)
            + plain_dot(backward_high, data_low)
            + plain_dot(backward_low, data_high)
        )

    green_real, green_imag = spectrum(green_entries)
    mirror_real, mirror_imag = spectrum(flipped_entries)
    polar_entries = to_values(
        green_real * mirror_real + green_imag * mirror_imag,
        green_imag * mirror_real - green_real * mirror_imag,
    )
    polar_entries = (polar_entries * (0.5 / math.sqrt(orbitals * energies))).astype(jnp.bfloat16)
    polar = lax.all_to_all(
        polar_entries.reshape(entry_shape), "energy", split_axis=0, concat_axis=1, tiled=True
    )
    inner = jnp.einsum(
        "ij,ejk->eik", coulomb_block, polar, preferred_element_type=jnp.float32
    ).astype(jnp.bfloat16)
    second = jnp.einsum("eij,jk->eik", inner, coulomb_block, preferred_element_type=jnp.float32)
    third = jnp.einsum(
        "eij,ejk->eik", inner, second.astype(jnp.bfloat16), preferred_element_type=jnp.float32
    )
    screened = (coulomb_block.astype(jnp.float32)[None] + second + third).astype(jnp.bfloat16)
    screened_entries = lax.all_to_all(
        screened, "energy", split_axis=1, concat_axis=0, tiled=True
    ).reshape(energies, -1)
    screen_real, screen_imag = spectrum(screened_entries)
    sigma_entries = to_values(
        green_real * screen_real - green_imag * screen_imag,
        green_real * screen_imag + green_imag * screen_real,
    )
    sigma_entries = (sigma_entries * (0.2 / math.sqrt(energies))).astype(jnp.bfloat16)
    sigma = lax.all_to_all(
        sigma_entries.reshape(entry_shape), "energy", split_axis=0, concat_axis=1, tiled=True
    )
    interface = couple_cols.shape[1]
    last = orbitals - interface
    coupling = coupling_matrix(couple_cols[0], couple_vals[0])
    prev_green, previous = from_behind((own_green, coupling), "slab", 1)
    next_green = from_behind(own_green, "slab", -1)
    prev_corner = prev_green[:, last:, last:]
    next_corner = next_green[:, :interface, :interface]
    near_next = jnp.einsum(
        "ij,ejk->eik", coupling, next_corner, preferred_element_type=jnp.float32
    ).astype(jnp.bfloat16)
    near_prev = jnp.einsum(
        "ji,ejk->eik", previous, prev_corner, preferred_element_type=jnp.float32
    ).astype(jnp.bfloat16)
    right_part = (
        jnp.einsum("eij,kj->eik", near_next, coupling, preferred_element_type=jnp.float32)
        * inv_root
    )
    left_part = (
        jnp.einsum("eij,jk->eik", near_prev, previous, preferred_element_type=jnp.float32)
        * inv_root
    )
    total = sigma.astype(jnp.float32)
    total = total.at[:, last:, last:].add(right_part)
    total = total.at[:, :interface, :interface].add(left_part)
    total_b = total.astype(jnp.bfloat16)
    dressed = jnp.einsum(
        "eij,ejk->eik", own_green, total_b, preferred_element_type=jnp.float32
    ).astype(jnp.bfloat16)
    updated = (
        own_green
        + jnp.einsum("eij,ejk->eik", dressed, own_green, preferred_element_type=jnp.float32)
        * inv_root
    )
    return updated.astype(jnp.bfloat16)[:, None]


MESH = pl.DeviceIdType.MESH


def unit_blocks(unit, grid):
    odd = grid - 1
    paired = grid * odd // 2
    slot = unit // odd
    turn = unit % odd
    diagonal = unit // paired
    first = (turn + slot) % odd
    second = (turn + odd - slot) % odd
    lone = 1 - (slot + odd - 1) // odd
    row = lone * odd + (1 - lone) * first
    col = lone * turn + (1 - lone) * second
    corner = 2 * (unit - paired)
    row0 = diagonal * corner + (1 - diagonal) * row
    col0 = diagonal * corner + (1 - diagonal) * col
    row1 = diagonal * (corner + 1) + (1 - diagonal) * col
    col1 = diagonal * (corner + 1) + (1 - diagonal) * row
    return ((row0, col0), (row1, col1))


CHUNKS = 1
GREEN_AHEAD = 1
POLAR_AHEAD = 1
SUBS = 2


def fused_kernel(
    volume, slabs, grid, scale_polar, scale_sigma, inv_root,
    green_hbm, coulomb_hbm, cols_hbm, vals_hbm, sigma, green,
    coulomb, cols, vals,
    stage, landed, mirror, second_half, polar_out, polar_more, matrix, inner, second, screened,
    screen_in, sigma_out,
    coupling, turned, next_corner, left_out, left_in, right_in,
    g_send, g_recv, p_send, p_recv, m_send, m_recv, w_send, w_recv, s_send, s_recv,
    slab_send, slab_recv, load_sem, turn, ready,
):
    loads = [
        pltpu.make_async_copy(source, target, load_sem.at[n])
        for n, (source, target) in enumerate(
            ((green_hbm, green), (coulomb_hbm, coulomb), (cols_hbm, cols), (vals_hbm, vals))
        )
    ]
    for load in loads:
        load.start()
    me = lax.axis_index("energy")
    slab = lax.axis_index("slab")
    size = green.shape[0] // grid
    last = green.shape[0] - size
    classes = volume // 2
    paired = grid * (grid - 1) // 2
    order = sorted(range(1, volume), key=lambda k: (-min(k, volume - k), k))
    has_prev = 1 - (slabs - 1 - slab + 0) // (slabs - 1)
    has_next = 1 - slab // (slabs - 1)
    planes = 4
    plane = volume // planes
    level = me // plane
    inner_level = level * (planes - 1 - level) // (planes - 2)

    def unit_of(device):
        return lax.rem(device + volume // 2, volume)

    my_unit = unit_of(me)
    diagonal = my_unit // paired
    my_class = lax.rem(me, classes)
    first_mate = me - my_class
    own_blocks = unit_blocks(my_unit, grid)
    chunk_rows = size // CHUNKS

    def peer_of(k):
        return lax.rem(me + k, volume)

    def from_of(k):
        return lax.rem(me + volume - k, volume)

    barrier = pltpu.get_barrier_semaphore()

    def apart(device):
        steps = device // plane - level
        return steps * steps

    for k in order:
        @pl.when(apart(peer_of(k)) <= 1)
        def _():
            pl.semaphore_signal(barrier, inc=1, device_id=(peer_of(k), slab), device_id_type=MESH)

    @pl.when(slab > 0)
    def _():
        pl.semaphore_signal(barrier, inc=1, device_id=(me, slab - 1), device_id_type=MESH)

    @pl.when(slab < slabs - 1)
    def _():
        pl.semaphore_signal(barrier, inc=1, device_id=(me, slab + 1), device_id_type=MESH)

    def flipped(block):
        return block.astype(jnp.float32).T.astype(jnp.bfloat16)

    def region(coords, start=0, rows=None):
        rows = size if rows is None else rows
        row = pl.multiple_of(coords[0] * size + start, rows)
        col = pl.multiple_of(coords[1] * size, size)
        return pl.ds(row, rows), pl.ds(col, size)

    def block_of(ref, coords, start=0, rows=None):
        return ref.at[region(coords, start, rows)]

    def remote(src, dst, sends, recvs, device):
        return pltpu.make_async_remote_copy(
            src_ref=src, dst_ref=dst, send_sem=sends, recv_sem=recvs,
            device_id=(device, slab), device_id_type=MESH,
        )

    loads[0].wait()
    for unit in range(volume):
        coords = unit_blocks(unit, grid)[1]
        block = green[coords[0] * size:(coords[0] + 1) * size, coords[1] * size:(coords[1] + 1) * size]
        stage[unit] = block if unit >= paired else flipped(block)

    pl.semaphore_wait(barrier, (2 + inner_level) * plane - 1 + has_prev + has_next)

    def tell(step, which):
        pl.semaphore_signal(ready.at[which], inc=1, device_id=(me + step * plane, slab), device_id_type=MESH)

    @pl.when(inner_level > 0)
    def _():
        tell(1, 0)
        tell(-1, 0)


    def took(shape, sem):
        pltpu.make_async_copy(shape, shape, sem).wait()

    others = pl.ds(0, volume - 1)

    def span(chunk):
        return pl.ds(chunk * chunk_rows, chunk_rows)

    def send_green(k):
        peer = peer_of(k)
        unit = unit_of(peer)
        for chunk in range(CHUNKS):
            for slot in range(2):
                if slot == 0:
                    source = block_of(green, unit_blocks(unit, grid)[0], chunk * chunk_rows, chunk_rows)
                else:
                    source = stage.at[unit, span(chunk)]
                remote(
                    source, landed.at[me, slot, span(chunk)], g_send.at[chunk], g_recv.at[k, chunk], peer
                ).start()

    def send_tier(low, high):
        for k in order:
            distance = apart(peer_of(k))
            pl.when(jnp.logical_and(distance >= low, distance <= high))(functools.partial(send_green, k))

    send_tier(0, 1)
    pl.semaphore_wait(ready.at[0], 1)

    @pl.when(level == 1)
    def _():
        tell(-1, 1)

    @pl.when(level == 2)
    def _():
        tell(1, 1)

    send_tier(4, 4)

    @pl.when(inner_level == 0)
    def _():
        pl.semaphore_wait(ready.at[1], 1)
        send_tier(9, 9)

    landed[me, 0] = block_of(green, own_blocks[0])[...]
    landed[me, 1] = stage[my_unit]

    corner_copy = pltpu.make_async_remote_copy(
        src_ref=green.at[pl.ds(0, size), pl.ds(0, size)], dst_ref=next_corner,
        send_sem=slab_send.at[0], recv_sem=slab_recv.at[0],
        device_id=(me, slab - has_prev), device_id_type=MESH,
    )
    left_copy = pltpu.make_async_remote_copy(
        src_ref=left_out, dst_ref=left_in,
        send_sem=slab_send.at[1], recv_sem=slab_recv.at[1],
        device_id=(me, slab + has_next), device_id_type=MESH,
    )

    @pl.when(slab > 0)
    def _():
        corner_copy.start()

    loads[2].wait()
    loads[3].wait()
    ids = cols[...]
    values = vals[...].astype(jnp.float32)
    columns = lax.broadcasted_iota(jnp.int32, (size, size), 0)
    summed = jnp.zeros((size, size), jnp.float32)
    for k in range(ids.shape[0]):
        summed += jnp.where(ids[k:k + 1, :] == columns, values[k:k + 1, :], jnp.float32(0.0))
    summed = summed.astype(jnp.bfloat16).astype(jnp.float32)
    turned[...] = summed.astype(jnp.bfloat16)
    coupling[...] = summed.T.astype(jnp.bfloat16)

    @pl.when(slab < slabs - 1)
    def _():
        near_prev = plain_dot(turned[...], green[last:, last:]).astype(jnp.bfloat16)
        left_out[...] = plain_dot(near_prev, coupling[...]) * inv_root
        left_copy.start()

    second_core = lax.rem(slab, 2)

    @pl.when(second_core == 0)
    def _():
        for chunk in range(GREEN_AHEAD):
            took(landed.at[others, :, span(chunk)], g_send.at[chunk])
        pl.semaphore_signal(turn.at[0], inc=1, device_id=(me, slab + 1), device_id_type=MESH)

    loads[1].wait()
    rows_at_once = 16
    steps = chunk_rows // rows_at_once

    def rows_of(step):
        return pl.ds(pl.multiple_of(step * rows_at_once, rows_at_once), rows_at_once)

    def correlation(mine, theirs, e):
        acc = mine[0] * theirs[(0 - e) % volume]
        for e2 in range(1, volume):
            acc += mine[e2] * theirs[(e2 - e) % volume]
        return (acc * scale_polar).astype(jnp.bfloat16)

    where = (
        (0, own_blocks[0]),
        (1 - diagonal, tuple(
            diagonal * d + (1 - diagonal) * o for d, o in zip(own_blocks[1], own_blocks[0])
        )),
    )

    def polar_copy(k, chunk, slot):
        peer = peer_of(k)
        index, coords = where[slot]
        return remote(
            polar_out.at[lax.rem(peer, classes), slot, span(chunk)],
            block_of(matrix.at[index], coords, chunk * chunk_rows, chunk_rows),
            p_send.at[chunk], p_recv.at[k], peer,
        )

    def send_polar(chunk):
        if chunk == 0:
            pl.semaphore_wait(turn.at[0], 1)
        for slot in range(2):
            for k in order:
                polar_copy(k, chunk, slot).start()

    def more_copy(target, slot):
        return remote(
            polar_more.at[slot],
            block_of(matrix.at[1], own_blocks[slot]),
            m_send.at[0], m_recv.at[0], target * classes,
        )

    def green_arrived(k, chunk):
        took(landed.at[from_of(k), :, span(chunk)], g_recv.at[k, chunk])

    @pl.when(diagonal == 0)
    def _():
        for chunk in range(CHUNKS):
            for k in order:
                green_arrived(k, chunk)

            def correlate(step, carry):
                rows = rows_of(step)
                mine = [landed[e, 0, rows, :].astype(jnp.float32) for e in range(volume)]
                theirs = [landed[e, 1, rows, :].astype(jnp.float32) for e in range(volume)]
                for e in range(volume):
                    if e % classes == 0:
                        place = (0, e // classes)
                    else:
                        place = (min(e, volume - e), e // classes)
                    polar_out[place[0], place[1], rows, :] = correlation(mine, theirs, e)
                return carry

            lax.fori_loop(chunk * steps, (chunk + 1) * steps, correlate, 0)
            send_polar(chunk)

    @pl.when(diagonal == 1)
    def _():
        def flip_both(e):
            for slot in range(2):
                mirror[e, slot] = flipped(landed[e, slot])

        flip_both(me)
        for k in order:
            for chunk in range(CHUNKS):
                green_arrived(k, chunk)
            flip_both(from_of(k))

        for slot in range(2):
            def correlate(step, carry, slot=slot):
                rows = rows_of(step)
                mine = [landed[e, slot, rows, :].astype(jnp.float32) for e in range(volume)]
                theirs = [mirror[e, slot, rows, :].astype(jnp.float32) for e in range(volume)]
                for e in range(classes):
                    polar_out[e, slot, rows, :] = correlation(mine, theirs, e)
                polar_more[slot, rows, :] = correlation(mine, theirs, classes)
                return carry

            lax.fori_loop(0, size // rows_at_once, correlate, 0)
        for chunk in range(CHUNKS):
            send_polar(chunk)
        for target in range(2):
            for slot in range(2):
                more_copy(target, slot).start()

    for slot in range(2):
        index, coords = where[slot]
        block_of(matrix.at[index], coords)[...] = polar_out[my_class, slot]

    @pl.when(diagonal == 0)
    def _():
        for e in range(volume):
            second_half[e] = flipped(landed[e, 1])

    @pl.when(diagonal == 1)
    def _():
        for e in range(volume):
            second_half[e] = landed[e, 1]

    @pl.when(second_core == 1)
    def _():
        for chunk in range(POLAR_AHEAD):
            took(landed.at[others, :, span(chunk)], p_send.at[chunk])
        pl.semaphore_signal(turn.at[0], inc=1, device_id=(me, slab - 1), device_id_type=MESH)

    swapped = 1 - lax.rem(my_class + classes - 1, classes) // (classes - 1)

    def complete(device):
        unit = unit_of(device)
        coords = unit_blocks(unit, grid)
        off = 1 - unit // paired

        @pl.when(off == 1)
        def _():
            for index in range(2):
                source = swapped * (1 - index) + (1 - swapped) * index
                block_of(matrix.at[index], coords[1])[...] = flipped(
                    block_of(matrix.at[source], coords[0])[...]
                )

        @pl.when(jnp.logical_and(off == 0, my_class > 0))
        def _():
            for slot in range(2):
                block_of(matrix.at[1], coords[slot])[...] = flipped(
                    block_of(matrix.at[0], coords[slot])[...]
                )

    complete(me)
    for k in order:
        took(polar_out.at[0], p_recv.at[k])
        complete(from_of(k))

    @pl.when(my_class == 0)
    def _():
        took(polar_out.at[pl.ds(0, volume - paired)], m_recv.at[0])

    for index in range(2):
        inner[index] = plain_dot(coulomb[...], matrix[index]).astype(jnp.bfloat16)
    for index in range(2):
        product = plain_dot(inner[index], coulomb[...])
        second[index] = product
        matrix[index] = product.astype(jnp.bfloat16)
    for index in range(2):
        third = plain_dot(inner[index], matrix[index])
        screened[index] = (coulomb[...].astype(jnp.float32) + second[index] + third).astype(jnp.bfloat16)

    parts = [(half, sub) for half in range(2) for sub in range(SUBS)]
    sub_rows = size // SUBS
    for half, sub in parts:
        for t in range(1, classes):
            mate = first_mate + lax.rem(my_class + t, classes)
            rows, width = region(unit_blocks(unit_of(mate), grid)[half], sub * sub_rows, sub_rows)
            remote(
                screened.at[:, rows, width],
                screen_in.at[my_class, half, :, pl.ds(sub * sub_rows, sub_rows)],
                w_send.at[0], w_recv.at[half, sub], mate,
            ).start()
    for half in range(2):
        rows, width = region(own_blocks[half])
        screen_in[my_class, half] = screened[:, rows, width]

    def sigma_copy(half, sub, target):
        return remote(
            sigma_out.at[target, half, pl.ds(sub * sub_rows, sub_rows)],
            block_of(sigma, own_blocks[half], sub * sub_rows, sub_rows),
            s_send.at[0], s_recv.at[0], target,
        )

    def for_others(act):
        for other in range(volume):
            pl.when(me != other)(functools.partial(act, other))

    for half, sub in parts:
        took(
            screen_in.at[pl.ds(0, classes - 1), half, :, pl.ds(sub * sub_rows, sub_rows)],
            w_recv.at[half, sub],
        )

        def convolve(step, carry, half=half):
            rows = rows_of(step)
            if half == 0:
                mine = [landed[e, 0, rows, :].astype(jnp.float32) for e in range(volume)]
            else:
                mine = [second_half[e, rows, :].astype(jnp.float32) for e in range(volume)]
            waves = [
                screen_in[min(e, volume - e) % classes, half, e // classes, rows, :].astype(jnp.float32)
                for e in range(volume)
            ]
            for e in range(volume):
                acc = mine[0] * waves[e]
                for e2 in range(1, volume):
                    acc += mine[e2] * waves[(e - e2) % volume]
                sigma_out[e, half, rows, :] = (acc * scale_sigma).astype(jnp.bfloat16)
            return carry

        lax.fori_loop(sub * sub_rows // rows_at_once, (sub + 1) * sub_rows // rows_at_once, convolve, 0)
        for_others(lambda target: sigma_copy(half, sub, target).start())
    for half in range(2):
        block_of(sigma, own_blocks[half])[...] = sigma_out[me, half]

    @pl.when(slab < slabs - 1)
    def _():
        corner_copy.wait_recv()
        near_next = plain_dot(coupling[...], next_corner[...]).astype(jnp.bfloat16)
        right_in[...] = plain_dot(near_next, turned[...]) * inv_root

    took(landed.at[others], s_recv.at[0])

    @pl.when(slab < slabs - 1)
    def _():
        sigma[last:, last:] = (sigma[last:, last:].astype(jnp.float32) + right_in[...]).astype(jnp.bfloat16)
        left_copy.wait_send()

    @pl.when(slab > 0)
    def _():
        left_copy.wait_recv()
        sigma[:size, :size] = (sigma[:size, :size].astype(jnp.float32) + left_in[...]).astype(jnp.bfloat16)
        corner_copy.wait_send()

    for chunk in range(CHUNKS):
        @pl.when(second_core + (chunk >= GREEN_AHEAD) > 0)
        def _():
            took(landed.at[others, :, span(chunk)], g_send.at[chunk])

        @pl.when(1 - second_core + (chunk >= POLAR_AHEAD) > 0)
        def _():
            took(landed.at[others, :, span(chunk)], p_send.at[chunk])

    took(screen_in.at[pl.ds(0, classes - 1)], w_send.at[0])
    took(landed.at[others], s_send.at[0])

    @pl.when(diagonal == 1)
    def _():
        took(polar_out.at[pl.ds(0, 2)], m_send.at[0])


def dress_kernel(inv_root, total, green, out):
    dressed = plain_dot(green[...], total[...]).astype(jnp.bfloat16)
    updated = green[...].astype(jnp.float32) + plain_dot(dressed, green[...]) * inv_root
    out[...] = updated.astype(jnp.bfloat16)


def fused_on_device(grid, green_blocks, coulomb, couple_cols, couple_vals):
    volume = lax.axis_size("energy")
    slabs = lax.axis_size("slab")
    orbitals = green_blocks.shape[-1]
    size = orbitals // grid
    half_type = jnp.bfloat16

    def pieces(*lead):
        return pltpu.VMEM((*lead, size, size), half_type)

    def wholes(*lead, kind=half_type):
        return pltpu.VMEM((*lead, orbitals, orbitals), kind)

    def pair(sends, recvs):
        return [pltpu.SemaphoreType.DMA(sends), pltpu.SemaphoreType.DMA(recvs)]

    wide = pltpu.VMEM((size, size), jnp.float32)
    classes = volume // 2
    inv_root = 1.0 / math.sqrt(orbitals)
    in_vmem = pl.BlockSpec(memory_space=pltpu.VMEM)
    total, green = pl.pallas_call(
        functools.partial(
            fused_kernel, volume, slabs, grid,
            0.5 / math.sqrt(orbitals * volume), 0.2 / math.sqrt(volume), inv_root,
        ),
        out_shape=[jax.ShapeDtypeStruct((orbitals, orbitals), half_type)] * 2,
        in_specs=[pl.BlockSpec(memory_space=pltpu.HBM)] * 4,
        out_specs=[in_vmem] * 2,
        scratch_shapes=[
            wholes(), pltpu.VMEM(couple_cols.shape[:0:-1], jnp.int32), pltpu.VMEM(couple_vals.shape[:0:-1], half_type),
            pieces(volume), pieces(volume, 2), pieces(volume, 2), pieces(volume), pieces(classes, 2), pieces(2),
            wholes(2), wholes(2), wholes(2, kind=jnp.float32), wholes(2),
            pieces(classes, 2, 2), pieces(volume, 2),
            pieces(), pieces(), pieces(), wide, wide, wide,
            *pair((CHUNKS,), (volume, CHUNKS)), *pair((CHUNKS,), (volume,)), *pair((1,), (1,)),
            *pair((1,), (2, SUBS)), *pair((1,), (1,)), *pair((2,), (2,)), pltpu.SemaphoreType.DMA((4,)),
            pltpu.SemaphoreType.REGULAR((1,)), pltpu.SemaphoreType.REGULAR((2,)),
        ],
        compiler_params=pltpu.CompilerParams(
            collective_id=0, has_side_effects=True, vmem_limit_bytes=32 << 20
        ),
    )(*(
        pltpu.with_memory_space_constraint(array, pltpu.HBM)
        for array in (green_blocks[0, 0], coulomb[0], couple_cols[0].T, couple_vals[0].T)
    ))
    result = pl.pallas_call(
        functools.partial(dress_kernel, inv_root),
        out_shape=jax.ShapeDtypeStruct((orbitals, orbitals), half_type),
        in_specs=[in_vmem] * 2,
        out_specs=in_vmem,
        compiler_params=pltpu.CompilerParams(vmem_limit_bytes=16 << 20),
    )(total, green)
    return result[None, None]


def fused_grid(mesh):
    volume = mesh.shape["energy"]
    grid = math.isqrt(2 * volume)
    return grid if grid * grid == 2 * volume and grid % 2 == 0 else 0


def on_any(grid, green_blocks, coulomb, couple_cols, couple_vals):
    orbitals = green_blocks.shape[-1]
    fits = (
        grid > 2
        and green_blocks.shape[:2] == (1, 1)
        and orbitals % (128 * max(grid, 1)) == 0
        and couple_cols.shape[1] * grid == orbitals
        and lax.axis_size("slab") % 2 == 0
    )
    if fits:
        return fused_on_device(grid, green_blocks, coulomb, couple_cols, couple_vals)
    return on_device(green_blocks, coulomb, couple_cols, couple_vals)


def solution(mesh):
    return jax.shard_map(
        functools.partial(on_any, fused_grid(mesh)),
        mesh=mesh,
        in_specs=(
            P("energy", "slab", None, None),
            P("slab", None, None),
            P("slab", None, None),
            P("slab", None, None),
        ),
        out_specs=P("energy", "slab", None, None),
        check_vma=False,
    )
```

```python
import functools
import math

import jax
import jax.numpy as jnp
from jax import lax
from jax.experimental import pallas as pl
from jax.experimental.pallas import tpu as pltpu
from jax.sharding import PartitionSpec as P


def from_behind(x, axis, by):
    size = lax.axis_size(axis)
    pairs = [(i, i + by) for i in range(size) if 0 <= i + by < size]
    return lax.ppermute(x, axis, pairs)


def plain_dot(left, right):
    return jnp.dot(left, right, preferred_element_type=jnp.float32)


def split_parts(values):
    upper = values.astype(jnp.bfloat16)
    lower = (values - upper.astype(jnp.float32)).astype(jnp.bfloat16)
    return (upper, lower)


def coupling_matrix(column_ids, coupling_values):
    width = column_ids.shape[0]
    hits = column_ids[:, :, None] == jnp.arange(width, dtype=jnp.int32)[None, None, :]
    summed = jnp.sum(
        jnp.where(hits, coupling_values.astype(jnp.float32)[:, :, None], jnp.float32(0.0)), axis=1
    )
    return summed.astype(jnp.bfloat16)


def on_device(green_blocks, coulomb, couple_cols, couple_vals):
    own_green = green_blocks[:, 0]
    coulomb_block = coulomb[0]
    per_device = own_green.shape[0]
    orbitals = own_green.shape[1]
    volume = lax.axis_size("energy")
    energies = per_device * volume
    inv_root = 1.0 / math.sqrt(orbitals)
    flipped = jnp.swapaxes(own_green, 1, 2)
    received, flipped_recv = (
        lax.all_to_all(own_green, "energy", split_axis=1, concat_axis=0, tiled=True),
        lax.all_to_all(flipped, "energy", split_axis=1, concat_axis=0, tiled=True),
    )
    green_entries = received.reshape(energies, -1)
    flipped_entries = flipped_recv.reshape(energies, -1)
    entry_shape = received.shape
    halfway = energies // 2 + 1
    frequency = jnp.arange(halfway, dtype=jnp.int32)
    energy_index = jnp.arange(energies, dtype=jnp.int32)
    angles = (frequency[:, None] * energy_index[None, :] % energies).astype(jnp.float32) * (
        2.0 * math.pi / energies
    )
    cosine = jnp.cos(angles)
    sine = jnp.sin(angles)
    weights = (
        jnp.where((frequency == 0) | (2 * frequency == energies), 1.0, 2.0).astype(jnp.float32)
        / energies
    )
    forward_high, forward_low = split_parts(jnp.concatenate([cosine, -sine], axis=0))
    backward_table = jnp.concatenate(
        [cosine * weights[:, None], -sine * weights[:, None]], axis=0
    ).T
    backward_high, backward_low = split_parts(backward_table)

    def spectrum(entries):
        stacked = plain_dot(forward_high, entries) + plain_dot(forward_low, entries)
        return (stacked[:halfway], stacked[halfway:])

    def to_values(real_part, imag_part):
        data_high, data_low = split_parts(jnp.concatenate([real_part, imag_part], axis=0))
        return (
            plain_dot(backward_high, data_high)
            + plain_dot(backward_high, data_low)
            + plain_dot(backward_low, data_high)
        )

    green_real, green_imag = spectrum(green_entries)
    mirror_real, mirror_imag = spectrum(flipped_entries)
    polar_entries = to_values(
        green_real * mirror_real + green_imag * mirror_imag,
        green_imag * mirror_real - green_real * mirror_imag,
    )
    polar_entries = (polar_entries * (0.5 / math.sqrt(orbitals * energies))).astype(jnp.bfloat16)
    polar = lax.all_to_all(
        polar_entries.reshape(entry_shape), "energy", split_axis=0, concat_axis=1, tiled=True
    )
    inner = jnp.einsum(
        "ij,ejk->eik", coulomb_block, polar, preferred_element_type=jnp.float32
    ).astype(jnp.bfloat16)
    second = jnp.einsum("eij,jk->eik", inner, coulomb_block, preferred_element_type=jnp.float32)
    third = jnp.einsum(
        "eij,ejk->eik", inner, second.astype(jnp.bfloat16), preferred_element_type=jnp.float32
    )
    screened = (coulomb_block.astype(jnp.float32)[None] + second + third).astype(jnp.bfloat16)
    screened_entries = lax.all_to_all(
        screened, "energy", split_axis=1, concat_axis=0, tiled=True
    ).reshape(energies, -1)
    screen_real, screen_imag = spectrum(screened_entries)
    sigma_entries = to_values(
        green_real * screen_real - green_imag * screen_imag,
        green_real * screen_imag + green_imag * screen_real,
    )
    sigma_entries = (sigma_entries * (0.2 / math.sqrt(energies))).astype(jnp.bfloat16)
    sigma = lax.all_to_all(
        sigma_entries.reshape(entry_shape), "energy", split_axis=0, concat_axis=1, tiled=True
    )
    interface = couple_cols.shape[1]
    last = orbitals - interface
    coupling = coupling_matrix(couple_cols[0], couple_vals[0])
    prev_green, previous = from_behind((own_green, coupling), "slab", 1)
    next_green = from_behind(own_green, "slab", -1)
    prev_corner = prev_green[:, last:, last:]
    next_corner = next_green[:, :interface, :interface]
    near_next = jnp.einsum(
        "ij,ejk->eik", coupling, next_corner, preferred_element_type=jnp.float32
    ).astype(jnp.bfloat16)
    near_prev = jnp.einsum(
        "ji,ejk->eik", previous, prev_corner, preferred_element_type=jnp.float32
    ).astype(jnp.bfloat16)
    right_part = (
        jnp.einsum("eij,kj->eik", near_next, coupling, preferred_element_type=jnp.float32)
        * inv_root
    )
    left_part = (
        jnp.einsum("eij,jk->eik", near_prev, previous, preferred_element_type=jnp.float32)
        * inv_root
    )
    total = sigma.astype(jnp.float32)
    total = total.at[:, last:, last:].add(right_part)
    total = total.at[:, :interface, :interface].add(left_part)
    total_b = total.astype(jnp.bfloat16)
    dressed = jnp.einsum(
        "eij,ejk->eik", own_green, total_b, preferred_element_type=jnp.float32
    ).astype(jnp.bfloat16)
    updated = (
        own_green
        + jnp.einsum("eij,ejk->eik", dressed, own_green, preferred_element_type=jnp.float32)
        * inv_root
    )
    return updated.astype(jnp.bfloat16)[:, None]


MESH = pl.DeviceIdType.MESH


def unit_blocks(unit, grid):
    odd = grid - 1
    paired = grid * odd // 2
    slot = unit // odd
    turn = unit % odd
    diagonal = unit // paired
    first = (turn + slot) % odd
    second = (turn + odd - slot) % odd
    lone = 1 - (slot + odd - 1) // odd
    row = lone * odd + (1 - lone) * first
    col = lone * turn + (1 - lone) * second
    corner = 2 * (unit - paired)
    row0 = diagonal * corner + (1 - diagonal) * row
    col0 = diagonal * corner + (1 - diagonal) * col
    row1 = diagonal * (corner + 1) + (1 - diagonal) * col
    col1 = diagonal * (corner + 1) + (1 - diagonal) * row
    return ((row0, col0), (row1, col1))


CHUNKS = 1
GREEN_AHEAD = 1
POLAR_AHEAD = 1
SUBS = 2
FIRST = 2
LATE = 2


def fused_kernel(
    volume, slabs, grid, scale_polar, scale_sigma, inv_root,
    green_hbm, coulomb_hbm, cols_hbm, vals_hbm, sigma, green,
    coulomb, cols, vals,
    stage, landed, mirror, second_half, polar_out, polar_more, matrix, inner, second, screened,
    screen_in, sigma_out,
    coupling, turned, next_corner, left_out, left_in, right_in,
    g_send, g_recv, p_send, p_recv, m_send, m_recv, w_send, w_recv, s_send, s_recv,
    slab_send, slab_recv, load_sem, turn, ready,
):
    loads = [
        pltpu.make_async_copy(source, target, load_sem.at[n])
        for n, (source, target) in enumerate(
            ((green_hbm, green), (coulomb_hbm, coulomb), (cols_hbm, cols), (vals_hbm, vals))
        )
    ]
    for load in loads:
        load.start()
    me = lax.axis_index("energy")
    slab = lax.axis_index("slab")
    size = green.shape[0] // grid
    last = green.shape[0] - size
    classes = volume // 2
    paired = grid * (grid - 1) // 2
    order = sorted(range(1, volume), key=lambda k: (-min(k, volume - k), k))
    has_prev = 1 - (slabs - 1 - slab + 0) // (slabs - 1)
    has_next = 1 - slab // (slabs - 1)
    planes = volume // 2
    plane = volume // planes
    level = me // plane
    inner_level = level * (planes - 1 - level) // (planes - 2)

    def unit_of(device):
        return lax.rem(device + volume // 2, volume)

    my_unit = unit_of(me)
    diagonal = my_unit // paired
    my_class = lax.rem(me, classes)
    first_mate = me - my_class
    own_blocks = unit_blocks(my_unit, grid)
    chunk_rows = size // CHUNKS

    def peer_of(k):
        return lax.rem(me + k, volume)

    def from_of(k):
        return lax.rem(me + volume - k, volume)

    barrier = pltpu.get_barrier_semaphore()

    def apart(device):
        steps = device // plane - level
        return steps * steps

    column = lax.rem(me, plane)

    def tier(device):
        aside = lax.rem(device, plane) - column
        return apart(device) * (apart(device) + 1) // 2 + aside * aside

    for k in order:
        @pl.when(tier(peer_of(k)) <= 1)
        def _():
            pl.semaphore_signal(barrier, inc=1, device_id=(peer_of(k), slab), device_id_type=MESH)

    @pl.when(slab > 0)
    def _():
        pl.semaphore_signal(barrier, inc=1, device_id=(me, slab - 1), device_id_type=MESH)

    @pl.when(slab < slabs - 1)
    def _():
        pl.semaphore_signal(barrier, inc=1, device_id=(me, slab + 1), device_id_type=MESH)

    def flipped(block):
        return block.astype(jnp.float32).T.astype(jnp.bfloat16)

    def region(coords, start=0, rows=None):
        rows = size if rows is None else rows
        row = pl.multiple_of(coords[0] * size + start, rows)
        col = pl.multiple_of(coords[1] * size, size)
        return pl.ds(row, rows), pl.ds(col, size)

    def block_of(ref, coords, start=0, rows=None):
        return ref.at[region(coords, start, rows)]

    def remote(src, dst, sends, recvs, device):
        return pltpu.make_async_remote_copy(
            src_ref=src, dst_ref=dst, send_sem=sends, recv_sem=recvs,
            device_id=(device, slab), device_id_type=MESH,
        )

    loads[0].wait()
    for unit in range(volume):
        coords = unit_blocks(unit, grid)[1]
        block = green[coords[0] * size:(coords[0] + 1) * size, coords[1] * size:(coords[1] + 1) * size]
        stage[unit] = block if unit >= paired else flipped(block)

    pl.semaphore_wait(barrier, inner_level + plane + has_prev + has_next)

    def tell(device, which):
        pl.semaphore_signal(ready.at[which], inc=1, device_id=(device, slab), device_id_type=MESH)

    for k in range(1, plane):
        tell(me - column + lax.rem(column + k, plane), 0)

    def took(shape, sem):
        pltpu.make_async_copy(shape, shape, sem).wait()

    others = pl.ds(0, volume - 1)

    def span(chunk):
        return pl.ds(chunk * chunk_rows, chunk_rows)

    def send_green(k):
        peer = peer_of(k)
        unit = unit_of(peer)
        for chunk in range(CHUNKS):
            for slot in range(2):
                if slot == 0:
                    source = block_of(green, unit_blocks(unit, grid)[0], chunk * chunk_rows, chunk_rows)
                else:
                    source = stage.at[unit, span(chunk)]
                remote(
                    source, landed.at[me, slot, span(chunk)], g_send.at[chunk], g_recv.at[k, chunk], peer
                ).start()

    def send_tier(low, high):
        for k in order[::-1]:
            distance = tier(peer_of(k))
            pl.when(jnp.logical_and(distance >= low, distance <= high))(functools.partial(send_green, k))

    send_tier(0, 1)
    pl.semaphore_wait(ready.at[0], plane - 1)

    @pl.when(inner_level > 0)
    def _():
        tell(me + plane, 1)
        tell(me - plane, 1)

    send_tier(2, 2)
    pl.semaphore_wait(ready.at[1], 1)

    @pl.when(level == 1)
    def _():
        tell(me - plane, 2)

    @pl.when(level == 2)
    def _():
        tell(me + plane, 2)

    send_tier(10, 11)

    @pl.when(inner_level == 0)
    def _():
        pl.semaphore_wait(ready.at[2], 1)
        send_tier(45, 46)

    landed[me, 0] = block_of(green, own_blocks[0])[...]
    landed[me, 1] = stage[my_unit]

    corner_copy = pltpu.make_async_remote_copy(
        src_ref=green.at[pl.ds(0, size), pl.ds(0, size)], dst_ref=next_corner,
        send_sem=slab_send.at[0], recv_sem=slab_recv.at[0],
        device_id=(me, slab - has_prev), device_id_type=MESH,
    )
    left_copy = pltpu.make_async_remote_copy(
        src_ref=left_out, dst_ref=left_in,
        send_sem=slab_send.at[1], recv_sem=slab_recv.at[1],
        device_id=(me, slab + has_next), device_id_type=MESH,
    )

    @pl.when(slab > 0)
    def _():
        corner_copy.start()

    loads[2].wait()
    loads[3].wait()
    ids = cols[...]
    values = vals[...].astype(jnp.float32)
    columns = lax.broadcasted_iota(jnp.int32, (size, size), 0)
    summed = jnp.zeros((size, size), jnp.float32)
    for k in range(ids.shape[0]):
        summed += jnp.where(ids[k:k + 1, :] == columns, values[k:k + 1, :], jnp.float32(0.0))
    summed = summed.astype(jnp.bfloat16).astype(jnp.float32)
    turned[...] = summed.astype(jnp.bfloat16)
    coupling[...] = summed.T.astype(jnp.bfloat16)

    @pl.when(slab < slabs - 1)
    def _():
        near_prev = plain_dot(turned[...], green[last:, last:]).astype(jnp.bfloat16)
        left_out[...] = plain_dot(near_prev, coupling[...]) * inv_root
        left_copy.start()

    second_core = lax.rem(slab, 2)

    @pl.when(second_core == 0)
    def _():
        for chunk in range(GREEN_AHEAD):
            took(landed.at[others, :, span(chunk)], g_send.at[chunk])
        pl.semaphore_signal(turn.at[0], inc=1, device_id=(me, slab + 1), device_id_type=MESH)

    loads[1].wait()
    rows_at_once = 16
    steps = chunk_rows // rows_at_once

    def rows_of(step):
        return pl.ds(pl.multiple_of(step * rows_at_once, rows_at_once), rows_at_once)

    def correlation(mine, theirs, e):
        acc = mine[0] * theirs[(0 - e) % volume]
        for e2 in range(1, volume):
            acc += mine[e2] * theirs[(e2 - e) % volume]
        return (acc * scale_polar).astype(jnp.bfloat16)

    where = (
        (0, own_blocks[0]),
        (1 - diagonal, tuple(
            diagonal * d + (1 - diagonal) * o for d, o in zip(own_blocks[1], own_blocks[0])
        )),
    )

    def polar_copy(k, chunk, slot):
        peer = peer_of(k)
        index, coords = where[slot]
        return remote(
            polar_out.at[lax.rem(peer, classes), slot, span(chunk)],
            block_of(matrix.at[index], coords, chunk * chunk_rows, chunk_rows),
            p_send.at[chunk], p_recv.at[k], peer,
        )

    def send_polar(chunk):
        if chunk == 0:
            pl.semaphore_wait(turn.at[0], 1)
        for slot in range(2):
            for k in order:
                polar_copy(k, chunk, slot).start()

    def more_copy(target, slot):
        return remote(
            polar_more.at[slot],
            block_of(matrix.at[1], own_blocks[slot]),
            m_send.at[0], m_recv.at[0], target * classes,
        )

    def green_arrived(k, chunk):
        took(landed.at[from_of(k), :, span(chunk)], g_recv.at[k, chunk])

    @pl.when(diagonal == 0)
    def _():
        for chunk in range(CHUNKS):
            for k in order:
                green_arrived(k, chunk)

            def correlate(step, carry):
                rows = rows_of(step)
                mine = [landed[e, 0, rows, :].astype(jnp.float32) for e in range(volume)]
                theirs = [landed[e, 1, rows, :].astype(jnp.float32) for e in range(volume)]
                for e in range(volume):
                    if e % classes == 0:
                        place = (0, e // classes)
                    else:
                        place = (min(e, volume - e), e // classes)
                    polar_out[place[0], place[1], rows, :] = correlation(mine, theirs, e)
                return carry

            lax.fori_loop(chunk * steps, (chunk + 1) * steps, correlate, 0)
            send_polar(chunk)

    @pl.when(diagonal == 1)
    def _():
        def flip_both(e):
            for slot in range(2):
                mirror[e, slot] = flipped(landed[e, slot])

        flip_both(me)
        for k in order:
            for chunk in range(CHUNKS):
                green_arrived(k, chunk)
            flip_both(from_of(k))

        for slot in range(2):
            def correlate(step, carry, slot=slot):
                rows = rows_of(step)
                mine = [landed[e, slot, rows, :].astype(jnp.float32) for e in range(volume)]
                theirs = [mirror[e, slot, rows, :].astype(jnp.float32) for e in range(volume)]
                for e in range(classes):
                    polar_out[e, slot, rows, :] = correlation(mine, theirs, e)
                polar_more[slot, rows, :] = correlation(mine, theirs, classes)
                return carry

            lax.fori_loop(0, size // rows_at_once, correlate, 0)
        for chunk in range(CHUNKS):
            send_polar(chunk)
        for target in range(2):
            for slot in range(2):
                more_copy(target, slot).start()

    for slot in range(2):
        index, coords = where[slot]
        block_of(matrix.at[index], coords)[...] = polar_out[my_class, slot]

    @pl.when(diagonal == 0)
    def _():
        for e in range(volume):
            second_half[e] = flipped(landed[e, 1])

    @pl.when(diagonal == 1)
    def _():
        for e in range(volume):
            second_half[e] = landed[e, 1]

    @pl.when(second_core == 1)
    def _():
        for chunk in range(POLAR_AHEAD):
            took(landed.at[others, :, span(chunk)], p_send.at[chunk])
        pl.semaphore_signal(turn.at[0], inc=1, device_id=(me, slab - 1), device_id_type=MESH)

    swapped = 1 - lax.rem(my_class + classes - 1, classes) // (classes - 1)

    def complete(device):
        unit = unit_of(device)
        coords = unit_blocks(unit, grid)
        off = 1 - unit // paired

        @pl.when(off == 1)
        def _():
            for index in range(2):
                source = swapped * (1 - index) + (1 - swapped) * index
                block_of(matrix.at[index], coords[1])[...] = flipped(
                    block_of(matrix.at[source], coords[0])[...]
                )

        @pl.when(jnp.logical_and(off == 0, my_class > 0))
        def _():
            for slot in range(2):
                block_of(matrix.at[1], coords[slot])[...] = flipped(
                    block_of(matrix.at[0], coords[slot])[...]
                )

    complete(me)
    for k in order:
        took(polar_out.at[0], p_recv.at[k])
        complete(from_of(k))

    @pl.when(my_class == 0)
    def _():
        took(polar_out.at[pl.ds(0, volume - paired)], m_recv.at[0])

    for index in range(2):
        inner[index] = plain_dot(coulomb[...], matrix[index]).astype(jnp.bfloat16)
    for index in range(2):
        product = plain_dot(inner[index], coulomb[...])
        second[index] = product
        matrix[index] = product.astype(jnp.bfloat16)
    parts = [(half, sub) for half in range(2) for sub in range(SUBS)]
    sub_rows = size // SUBS

    def wave(index, coords):
        rows, width = region(coords)
        third = plain_dot(inner[index, rows, :], matrix[index, :, width])
        whole = coulomb[rows, width].astype(jnp.float32) + second[index, rows, width] + third
        return whole.astype(jnp.bfloat16)

    for half in range(2):
        for t in range(1, classes):
            coords = unit_blocks(unit_of(first_mate + lax.rem(my_class + t, classes)), grid)[half]
            for index in range(2):
                screened[t, half, index] = wave(index, coords)
        for sub in range(SUBS):
            for t in range(1, classes):
                span_now = pl.ds(sub * sub_rows, sub_rows)
                remote(
                    screened.at[t, half, :, span_now], screen_in.at[my_class, half, :, span_now],
                    w_send.at[0], w_recv.at[half, sub], first_mate + lax.rem(my_class + t, classes),
                ).start()
    for half in range(2):
        for index in range(2):
            screen_in[my_class, half, index] = wave(index, own_blocks[half])

    def sigma_copy(half, sub, target):
        return remote(
            sigma_out.at[target, half, pl.ds(sub * sub_rows, sub_rows)],
            block_of(sigma, own_blocks[half], sub * sub_rows, sub_rows),
            s_send.at[0], s_recv.at[0], target,
        )

    def for_others(act):
        for other in range(volume):
            pl.when(me != other)(functools.partial(act, other))

    def send_sigma(n, targets):
        for target in targets:
            pl.when(me != target)(lambda: sigma_copy(*parts[n], target).start())

    for n, (half, sub) in enumerate(parts):
        took(
            screen_in.at[pl.ds(0, classes - 1), half, :, pl.ds(sub * sub_rows, sub_rows)],
            w_recv.at[half, sub],
        )

        def convolve(step, carry, half=half):
            rows = rows_of(step)
            if half == 0:
                mine = [landed[e, 0, rows, :].astype(jnp.float32) for e in range(volume)]
            else:
                mine = [second_half[e, rows, :].astype(jnp.float32) for e in range(volume)]
            waves = [
                screen_in[min(e, volume - e) % classes, half, e // classes, rows, :].astype(jnp.float32)
                for e in range(volume)
            ]
            for e in range(volume):
                acc = mine[0] * waves[e]
                for e2 in range(1, volume):
                    acc += mine[e2] * waves[(e - e2) % volume]
                sigma_out[e, half, rows, :] = (acc * scale_sigma).astype(jnp.bfloat16)
            return carry

        lax.fori_loop(sub * sub_rows // rows_at_once, (sub + 1) * sub_rows // rows_at_once, convolve, 0)
        send_sigma(n, range(FIRST))
        if n >= LATE:
            send_sigma(n - LATE, range(FIRST, volume))
    for n in range(len(parts) - LATE, len(parts)):
        send_sigma(n, range(FIRST, volume))
    for half in range(2):
        block_of(sigma, own_blocks[half])[...] = sigma_out[me, half]

    @pl.when(slab < slabs - 1)
    def _():
        corner_copy.wait_recv()
        near_next = plain_dot(coupling[...], next_corner[...]).astype(jnp.bfloat16)
        right_in[...] = plain_dot(near_next, turned[...]) * inv_root

    took(landed.at[others], s_recv.at[0])

    @pl.when(slab < slabs - 1)
    def _():
        sigma[last:, last:] = (sigma[last:, last:].astype(jnp.float32) + right_in[...]).astype(jnp.bfloat16)
        left_copy.wait_send()

    @pl.when(slab > 0)
    def _():
        left_copy.wait_recv()
        sigma[:size, :size] = (sigma[:size, :size].astype(jnp.float32) + left_in[...]).astype(jnp.bfloat16)
        corner_copy.wait_send()

    for chunk in range(CHUNKS):
        @pl.when(second_core + (chunk >= GREEN_AHEAD) > 0)
        def _():
            took(landed.at[others, :, span(chunk)], g_send.at[chunk])

        @pl.when(1 - second_core + (chunk >= POLAR_AHEAD) > 0)
        def _():
            took(landed.at[others, :, span(chunk)], p_send.at[chunk])

    took(screen_in.at[pl.ds(0, classes - 1)], w_send.at[0])
    took(landed.at[others], s_send.at[0])

    @pl.when(diagonal == 1)
    def _():
        took(polar_out.at[pl.ds(0, 2)], m_send.at[0])


def dress_kernel(inv_root, total, green, out):
    dressed = plain_dot(green[...], total[...]).astype(jnp.bfloat16)
    updated = green[...].astype(jnp.float32) + plain_dot(dressed, green[...]) * inv_root
    out[...] = updated.astype(jnp.bfloat16)


def fused_on_device(grid, green_blocks, coulomb, couple_cols, couple_vals):
    volume = lax.axis_size("energy")
    slabs = lax.axis_size("slab")
    orbitals = green_blocks.shape[-1]
    size = orbitals // grid
    half_type = jnp.bfloat16

    def pieces(*lead):
        return pltpu.VMEM((*lead, size, size), half_type)

    def wholes(*lead, kind=half_type):
        return pltpu.VMEM((*lead, orbitals, orbitals), kind)

    def pair(sends, recvs):
        return [pltpu.SemaphoreType.DMA(sends), pltpu.SemaphoreType.DMA(recvs)]

    wide = pltpu.VMEM((size, size), jnp.float32)
    classes = volume // 2
    inv_root = 1.0 / math.sqrt(orbitals)
    in_vmem = pl.BlockSpec(memory_space=pltpu.VMEM)
    total, green = pl.pallas_call(
        functools.partial(
            fused_kernel, volume, slabs, grid,
            0.5 / math.sqrt(orbitals * volume), 0.2 / math.sqrt(volume), inv_root,
        ),
        out_shape=[jax.ShapeDtypeStruct((orbitals, orbitals), half_type)] * 2,
        in_specs=[pl.BlockSpec(memory_space=pltpu.HBM)] * 4,
        out_specs=[in_vmem] * 2,
        scratch_shapes=[
            wholes(), pltpu.VMEM(couple_cols.shape[:0:-1], jnp.int32), pltpu.VMEM(couple_vals.shape[:0:-1], half_type),
            pieces(volume), pieces(volume, 2), pieces(volume, 2), pieces(volume), pieces(classes, 2), pieces(2),
            wholes(2), wholes(2), wholes(2, kind=jnp.float32), pieces(classes, 2, 2),
            pieces(classes, 2, 2), pieces(volume, 2),
            pieces(), pieces(), pieces(), wide, wide, wide,
            *pair((CHUNKS,), (volume, CHUNKS)), *pair((CHUNKS,), (volume,)), *pair((1,), (1,)),
            *pair((1,), (2, SUBS)), *pair((1,), (1,)), *pair((2,), (2,)), pltpu.SemaphoreType.DMA((4,)),
            pltpu.SemaphoreType.REGULAR((1,)), pltpu.SemaphoreType.REGULAR((3,)),
        ],
        compiler_params=pltpu.CompilerParams(
            collective_id=0, has_side_effects=True, vmem_limit_bytes=32 << 20
        ),
    )(*(
        pltpu.with_memory_space_constraint(array, pltpu.HBM)
        for array in (green_blocks[0, 0], coulomb[0], couple_cols[0].T, couple_vals[0].T)
    ))
    result = pl.pallas_call(
        functools.partial(dress_kernel, inv_root),
        out_shape=jax.ShapeDtypeStruct((orbitals, orbitals), half_type),
        in_specs=[in_vmem] * 2,
        out_specs=in_vmem,
        compiler_params=pltpu.CompilerParams(vmem_limit_bytes=16 << 20),
    )(total, green)
    return result[None, None]


def fused_grid(mesh):
    volume = mesh.shape["energy"]
    grid = math.isqrt(2 * volume)
    return grid if grid * grid == 2 * volume and grid % 2 == 0 else 0


def on_any(grid, green_blocks, coulomb, couple_cols, couple_vals):
    orbitals = green_blocks.shape[-1]
    fits = (
        grid > 2
        and grid * 2 == lax.axis_size("energy")
        and green_blocks.shape[:2] == (1, 1)
        and orbitals % (128 * max(grid, 1)) == 0
        and couple_cols.shape[1] * grid == orbitals
        and lax.axis_size("slab") % 2 == 0
    )
    if fits:
        return fused_on_device(grid, green_blocks, coulomb, couple_cols, couple_vals)
    return on_device(green_blocks, coulomb, couple_cols, couple_vals)


def solution(mesh):
    return jax.shard_map(
        functools.partial(on_any, fused_grid(mesh)),
        mesh=mesh,
        in_specs=(
            P("energy", "slab", None, None),
            P("slab", None, None),
            P("slab", None, None),
            P("slab", None, None),
        ),
        out_specs=P("energy", "slab", None, None),
        check_vma=False,
    )
```

```python
import functools
import math

import jax
import jax.numpy as jnp
from jax import lax
from jax.experimental import pallas as pl
from jax.experimental.pallas import tpu as pltpu
from jax.sharding import PartitionSpec as P


def from_behind(x, axis, by):
    size = lax.axis_size(axis)
    pairs = [(i, i + by) for i in range(size) if 0 <= i + by < size]
    return lax.ppermute(x, axis, pairs)


def plain_dot(left, right):
    return jnp.dot(left, right, preferred_element_type=jnp.float32)


def split_parts(values):
    upper = values.astype(jnp.bfloat16)
    lower = (values - upper.astype(jnp.float32)).astype(jnp.bfloat16)
    return (upper, lower)


def coupling_matrix(column_ids, coupling_values):
    width = column_ids.shape[0]
    hits = column_ids[:, :, None] == jnp.arange(width, dtype=jnp.int32)[None, None, :]
    summed = jnp.sum(
        jnp.where(hits, coupling_values.astype(jnp.float32)[:, :, None], jnp.float32(0.0)), axis=1
    )
    return summed.astype(jnp.bfloat16)


def on_device(green_blocks, coulomb, couple_cols, couple_vals):
    own_green = green_blocks[:, 0]
    coulomb_block = coulomb[0]
    per_device = own_green.shape[0]
    orbitals = own_green.shape[1]
    volume = lax.axis_size("energy")
    energies = per_device * volume
    inv_root = 1.0 / math.sqrt(orbitals)
    flipped = jnp.swapaxes(own_green, 1, 2)
    received, flipped_recv = (
        lax.all_to_all(own_green, "energy", split_axis=1, concat_axis=0, tiled=True),
        lax.all_to_all(flipped, "energy", split_axis=1, concat_axis=0, tiled=True),
    )
    green_entries = received.reshape(energies, -1)
    flipped_entries = flipped_recv.reshape(energies, -1)
    entry_shape = received.shape
    halfway = energies // 2 + 1
    frequency = jnp.arange(halfway, dtype=jnp.int32)
    energy_index = jnp.arange(energies, dtype=jnp.int32)
    angles = (frequency[:, None] * energy_index[None, :] % energies).astype(jnp.float32) * (
        2.0 * math.pi / energies
    )
    cosine = jnp.cos(angles)
    sine = jnp.sin(angles)
    weights = (
        jnp.where((frequency == 0) | (2 * frequency == energies), 1.0, 2.0).astype(jnp.float32)
        / energies
    )
    forward_high, forward_low = split_parts(jnp.concatenate([cosine, -sine], axis=0))
    backward_table = jnp.concatenate(
        [cosine * weights[:, None], -sine * weights[:, None]], axis=0
    ).T
    backward_high, backward_low = split_parts(backward_table)

    def spectrum(entries):
        stacked = plain_dot(forward_high, entries) + plain_dot(forward_low, entries)
        return (stacked[:halfway], stacked[halfway:])

    def to_values(real_part, imag_part):
        data_high, data_low = split_parts(jnp.concatenate([real_part, imag_part], axis=0))
        return (
            plain_dot(backward_high, data_high)
            + plain_dot(backward_high, data_low)
            + plain_dot(backward_low, data_high)
        )

    green_real, green_imag = spectrum(green_entries)
    mirror_real, mirror_imag = spectrum(flipped_entries)
    polar_entries = to_values(
        green_real * mirror_real + green_imag * mirror_imag,
        green_imag * mirror_real - green_real * mirror_imag,
    )
    polar_entries = (polar_entries * (0.5 / math.sqrt(orbitals * energies))).astype(jnp.bfloat16)
    polar = lax.all_to_all(
        polar_entries.reshape(entry_shape), "energy", split_axis=0, concat_axis=1, tiled=True
    )
    inner = jnp.einsum(
        "ij,ejk->eik", coulomb_block, polar, preferred_element_type=jnp.float32
    ).astype(jnp.bfloat16)
    second = jnp.einsum("eij,jk->eik", inner, coulomb_block, preferred_element_type=jnp.float32)
    third = jnp.einsum(
        "eij,ejk->eik", inner, second.astype(jnp.bfloat16), preferred_element_type=jnp.float32
    )
    screened = (coulomb_block.astype(jnp.float32)[None] + second + third).astype(jnp.bfloat16)
    screened_entries = lax.all_to_all(
        screened, "energy", split_axis=1, concat_axis=0, tiled=True
    ).reshape(energies, -1)
    screen_real, screen_imag = spectrum(screened_entries)
    sigma_entries = to_values(
        green_real * screen_real - green_imag * screen_imag,
        green_real * screen_imag + green_imag * screen_real,
    )
    sigma_entries = (sigma_entries * (0.2 / math.sqrt(energies))).astype(jnp.bfloat16)
    sigma = lax.all_to_all(
        sigma_entries.reshape(entry_shape), "energy", split_axis=0, concat_axis=1, tiled=True
    )
    interface = couple_cols.shape[1]
    last = orbitals - interface
    coupling = coupling_matrix(couple_cols[0], couple_vals[0])
    prev_green, previous = from_behind((own_green, coupling), "slab", 1)
    next_green = from_behind(own_green, "slab", -1)
    prev_corner = prev_green[:, last:, last:]
    next_corner = next_green[:, :interface, :interface]
    near_next = jnp.einsum(
        "ij,ejk->eik", coupling, next_corner, preferred_element_type=jnp.float32
    ).astype(jnp.bfloat16)
    near_prev = jnp.einsum(
        "ji,ejk->eik", previous, prev_corner, preferred_element_type=jnp.float32
    ).astype(jnp.bfloat16)
    right_part = (
        jnp.einsum("eij,kj->eik", near_next, coupling, preferred_element_type=jnp.float32)
        * inv_root
    )
    left_part = (
        jnp.einsum("eij,jk->eik", near_prev, previous, preferred_element_type=jnp.float32)
        * inv_root
    )
    total = sigma.astype(jnp.float32)
    total = total.at[:, last:, last:].add(right_part)
    total = total.at[:, :interface, :interface].add(left_part)
    total_b = total.astype(jnp.bfloat16)
    dressed = jnp.einsum(
        "eij,ejk->eik", own_green, total_b, preferred_element_type=jnp.float32
    ).astype(jnp.bfloat16)
    updated = (
        own_green
        + jnp.einsum("eij,ejk->eik", dressed, own_green, preferred_element_type=jnp.float32)
        * inv_root
    )
    return updated.astype(jnp.bfloat16)[:, None]


MESH = pl.DeviceIdType.MESH


def unit_blocks(unit, grid):
    odd = grid - 1
    paired = grid * odd // 2
    slot = unit // odd
    turn = unit % odd
    diagonal = unit // paired
    first = (turn + slot) % odd
    second = (turn + odd - slot) % odd
    lone = 1 - (slot + odd - 1) // odd
    row = lone * odd + (1 - lone) * first
    col = lone * turn + (1 - lone) * second
    corner = 2 * (unit - paired)
    row0 = diagonal * corner + (1 - diagonal) * row
    col0 = diagonal * corner + (1 - diagonal) * col
    row1 = diagonal * (corner + 1) + (1 - diagonal) * col
    col1 = diagonal * (corner + 1) + (1 - diagonal) * row
    return ((row0, col0), (row1, col1))


CHUNKS = 1
SUBS = 2


def fused_kernel(
    volume, slabs, grid, scale_polar, scale_sigma, inv_root,
    green_hbm, coulomb_hbm, cols_hbm, vals_hbm, sigma, green,
    coulomb, cols, vals,
    stage, landed, mirror, second_half, polar_out, polar_more, matrix, inner, second, screened,
    screen_in, sigma_out,
    coupling, turned, next_corner, left_out, left_in, right_in,
    g_send, g_recv, p_send, p_recv, m_send, m_recv, w_send, w_recv, s_send, s_recv,
    slab_send, slab_recv, load_sem, turn, ready,
):
    loads = [
        pltpu.make_async_copy(source, target, load_sem.at[n])
        for n, (source, target) in enumerate(
            ((green_hbm, green), (coulomb_hbm, coulomb), (cols_hbm, cols), (vals_hbm, vals))
        )
    ]
    for load in loads:
        load.start()
    me = lax.axis_index("energy")
    slab = lax.axis_index("slab")
    size = green.shape[0] // grid
    last = green.shape[0] - size
    classes = volume // 2
    paired = grid * (grid - 1) // 2
    order = sorted(range(1, volume), key=lambda k: (-min(k, volume - k), k))
    has_prev = 1 - (slabs - 1 - slab + 0) // (slabs - 1)
    has_next = 1 - slab // (slabs - 1)
    planes = volume // 2
    plane = volume // planes
    level = me // plane
    inner_level = level * (planes - 1 - level) // (planes - 2)

    def unit_of(device):
        return lax.rem(device + volume // 2, volume)

    my_unit = unit_of(me)
    diagonal = my_unit // paired
    my_class = lax.rem(me, classes)
    first_mate = me - my_class
    own_blocks = unit_blocks(my_unit, grid)
    chunk_rows = size // CHUNKS

    def peer_of(k):
        return lax.rem(me + k, volume)

    def from_of(k):
        return lax.rem(me + volume - k, volume)

    barrier = pltpu.get_barrier_semaphore()

    def apart(device):
        steps = device // plane - level
        return steps * steps

    column = lax.rem(me, plane)

    def tier(device):
        aside = lax.rem(device, plane) - column
        return apart(device) * (apart(device) + 1) // 2 + aside * aside

    for k in order:
        @pl.when(tier(peer_of(k)) <= 1)
        def _():
            pl.semaphore_signal(barrier, inc=1, device_id=(peer_of(k), slab), device_id_type=MESH)

    @pl.when(slab > 0)
    def _():
        pl.semaphore_signal(barrier, inc=1, device_id=(me, slab - 1), device_id_type=MESH)

    @pl.when(slab < slabs - 1)
    def _():
        pl.semaphore_signal(barrier, inc=1, device_id=(me, slab + 1), device_id_type=MESH)

    def flipped(block):
        return block.astype(jnp.float32).T.astype(jnp.bfloat16)

    def region(coords, start=0, rows=None):
        rows = size if rows is None else rows
        row = pl.multiple_of(coords[0] * size + start, rows)
        col = pl.multiple_of(coords[1] * size, size)
        return pl.ds(row, rows), pl.ds(col, size)

    def block_of(ref, coords, start=0, rows=None):
        return ref.at[region(coords, start, rows)]

    def remote(src, dst, sends, recvs, device):
        return pltpu.make_async_remote_copy(
            src_ref=src, dst_ref=dst, send_sem=sends, recv_sem=recvs,
            device_id=(device, slab), device_id_type=MESH,
        )

    loads[0].wait()
    for unit in range(volume):
        coords = unit_blocks(unit, grid)[1]
        block = green[coords[0] * size:(coords[0] + 1) * size, coords[1] * size:(coords[1] + 1) * size]
        stage[unit] = block if unit >= paired else flipped(block)

    pl.semaphore_wait(barrier, inner_level + plane + has_prev + has_next)

    def tell(device, which):
        pl.semaphore_signal(ready.at[which], inc=1, device_id=(device, slab), device_id_type=MESH)

    for k in range(1, plane):
        tell(me - column + lax.rem(column + k, plane), 0)

    def took(shape, sem):
        pltpu.make_async_copy(shape, shape, sem).wait()

    others = pl.ds(0, volume - 1)

    def span(chunk):
        return pl.ds(chunk * chunk_rows, chunk_rows)

    def send_green(k):
        peer = peer_of(k)
        unit = unit_of(peer)
        for chunk in range(CHUNKS):
            for slot in range(2):
                if slot == 0:
                    source = block_of(green, unit_blocks(unit, grid)[0], chunk * chunk_rows, chunk_rows)
                else:
                    source = stage.at[unit, span(chunk)]
                remote(
                    source, landed.at[me, slot, span(chunk)], g_send.at[chunk], g_recv.at[k, chunk], peer
                ).start()

    def send_tier(low, high):
        for k in order[::-1]:
            distance = tier(peer_of(k))
            pl.when(jnp.logical_and(distance >= low, distance <= high))(functools.partial(send_green, k))

    send_tier(0, 1)
    pl.semaphore_wait(ready.at[0], plane - 1)

    @pl.when(inner_level > 0)
    def _():
        tell(me + plane, 1)
        tell(me - plane, 1)

    send_tier(2, 2)
    pl.semaphore_wait(ready.at[1], 1)

    @pl.when(level == 1)
    def _():
        tell(me - plane, 2)

    @pl.when(level == 2)
    def _():
        tell(me + plane, 2)

    send_tier(10, 11)

    @pl.when(inner_level == 0)
    def _():
        pl.semaphore_wait(ready.at[2], 1)
        send_tier(45, 46)

    landed[me, 0] = block_of(green, own_blocks[0])[...]
    landed[me, 1] = stage[my_unit]

    corner_copy = pltpu.make_async_remote_copy(
        src_ref=green.at[pl.ds(0, size), pl.ds(0, size)], dst_ref=next_corner,
        send_sem=slab_send.at[0], recv_sem=slab_recv.at[0],
        device_id=(me, slab - has_prev), device_id_type=MESH,
    )
    left_copy = pltpu.make_async_remote_copy(
        src_ref=left_out, dst_ref=left_in,
        send_sem=slab_send.at[1], recv_sem=slab_recv.at[1],
        device_id=(me, slab + has_next), device_id_type=MESH,
    )

    @pl.when(slab > 0)
    def _():
        corner_copy.start()

    loads[2].wait()
    loads[3].wait()
    ids = cols[...]
    values = vals[...].astype(jnp.float32)
    columns = lax.broadcasted_iota(jnp.int32, (size, size), 0)
    summed = jnp.zeros((size, size), jnp.float32)
    for k in range(ids.shape[0]):
        summed += jnp.where(ids[k:k + 1, :] == columns, values[k:k + 1, :], jnp.float32(0.0))
    summed = summed.astype(jnp.bfloat16).astype(jnp.float32)
    turned[...] = summed.astype(jnp.bfloat16)
    coupling[...] = summed.T.astype(jnp.bfloat16)

    @pl.when(slab < slabs - 1)
    def _():
        near_prev = plain_dot(turned[...], green[last:, last:]).astype(jnp.bfloat16)
        left_out[...] = plain_dot(near_prev, coupling[...]) * inv_root
        left_copy.start()

    second_core = 1 - lax.rem(slab, 2)
    partner = slab - 1 + 2 * second_core

    @pl.when(second_core == 0)
    def _():
        for chunk in range(CHUNKS):
            took(landed.at[others, :, span(chunk)], g_send.at[chunk])
        pl.semaphore_signal(turn.at[0], inc=1, device_id=(me, partner), device_id_type=MESH)

    loads[1].wait()
    rows_at_once = 16
    steps = chunk_rows // rows_at_once

    def rows_of(step):
        return pl.ds(pl.multiple_of(step * rows_at_once, rows_at_once), rows_at_once)

    def correlation(mine, theirs, e):
        acc = mine[0] * theirs[(0 - e) % volume]
        for e2 in range(1, volume):
            acc += mine[e2] * theirs[(e2 - e) % volume]
        return (acc * scale_polar).astype(jnp.bfloat16)

    where = (
        (0, own_blocks[0]),
        (1 - diagonal, tuple(
            diagonal * d + (1 - diagonal) * o for d, o in zip(own_blocks[1], own_blocks[0])
        )),
    )

    def polar_copy(k, chunk, slot):
        peer = peer_of(k)
        index, coords = where[slot]
        return remote(
            polar_out.at[lax.rem(peer, classes), slot, span(chunk)],
            block_of(matrix.at[index], coords, chunk * chunk_rows, chunk_rows),
            p_send.at[chunk], p_recv.at[k], peer,
        )

    def send_polar(chunk):
        if chunk == 0:
            pl.semaphore_wait(turn.at[0], 1)
        for slot in range(2):
            for k in order:
                polar_copy(k, chunk, slot).start()

    def more_copy(target, slot):
        return remote(
            polar_more.at[slot],
            block_of(matrix.at[1], own_blocks[slot]),
            m_send.at[0], m_recv.at[0], target * classes,
        )

    def green_arrived(k, chunk):
        took(landed.at[from_of(k), :, span(chunk)], g_recv.at[k, chunk])

    @pl.when(diagonal == 0)
    def _():
        for chunk in range(CHUNKS):
            for k in order:
                green_arrived(k, chunk)

            def correlate(step, carry):
                rows = rows_of(step)
                mine = [landed[e, 0, rows, :].astype(jnp.float32) for e in range(volume)]
                theirs = [landed[e, 1, rows, :].astype(jnp.float32) for e in range(volume)]
                for e in range(volume):
                    if e % classes == 0:
                        place = (0, e // classes)
                    else:
                        place = (min(e, volume - e), e // classes)
                    polar_out[place[0], place[1], rows, :] = correlation(mine, theirs, e)
                return carry

            lax.fori_loop(chunk * steps, (chunk + 1) * steps, correlate, 0)
            send_polar(chunk)

    @pl.when(diagonal == 1)
    def _():
        def flip_both(e):
            for slot in range(2):
                mirror[e, slot] = flipped(landed[e, slot])

        flip_both(me)
        for k in order:
            for chunk in range(CHUNKS):
                green_arrived(k, chunk)
            flip_both(from_of(k))

        for slot in range(2):
            def correlate(step, carry, slot=slot):
                rows = rows_of(step)
                mine = [landed[e, slot, rows, :].astype(jnp.float32) for e in range(volume)]
                theirs = [mirror[e, slot, rows, :].astype(jnp.float32) for e in range(volume)]
                for e in range(classes):
                    polar_out[e, slot, rows, :] = correlation(mine, theirs, e)
                polar_more[slot, rows, :] = correlation(mine, theirs, classes)
                return carry

            lax.fori_loop(0, size // rows_at_once, correlate, 0)
        for chunk in range(CHUNKS):
            send_polar(chunk)
        for target in range(2):
            for slot in range(2):
                more_copy(target, slot).start()

    for slot in range(2):
        index, coords = where[slot]
        block_of(matrix.at[index], coords)[...] = polar_out[my_class, slot]

    @pl.when(diagonal == 0)
    def _():
        for e in range(volume):
            second_half[e] = flipped(landed[e, 1])

    @pl.when(diagonal == 1)
    def _():
        for e in range(volume):
            second_half[e] = landed[e, 1]

    @pl.when(second_core == 1)
    def _():
        for chunk in range(CHUNKS):
            took(landed.at[others, :, span(chunk)], p_send.at[chunk])
        pl.semaphore_signal(turn.at[0], inc=1, device_id=(me, partner), device_id_type=MESH)

    swapped = 1 - lax.rem(my_class + classes - 1, classes) // (classes - 1)

    def complete(device):
        unit = unit_of(device)
        coords = unit_blocks(unit, grid)
        off = 1 - unit // paired

        @pl.when(off == 1)
        def _():
            for index in range(2):
                source = swapped * (1 - index) + (1 - swapped) * index
                block_of(matrix.at[index], coords[1])[...] = flipped(
                    block_of(matrix.at[source], coords[0])[...]
                )

        @pl.when(jnp.logical_and(off == 0, my_class > 0))
        def _():
            for slot in range(2):
                block_of(matrix.at[1], coords[slot])[...] = flipped(
                    block_of(matrix.at[0], coords[slot])[...]
                )

    complete(me)
    for k in order:
        took(polar_out.at[0], p_recv.at[k])
        complete(from_of(k))

    @pl.when(my_class == 0)
    def _():
        took(polar_out.at[pl.ds(0, volume - paired)], m_recv.at[0])

    for index in range(2):
        inner[index] = plain_dot(coulomb[...], matrix[index]).astype(jnp.bfloat16)
    for index in range(2):
        product = plain_dot(inner[index], coulomb[...])
        second[index] = product
        matrix[index] = product.astype(jnp.bfloat16)
    parts = [(half, sub) for half in range(2) for sub in range(SUBS)]
    sub_rows = size // SUBS

    def wave(index, coords):
        rows, width = region(coords)
        third = plain_dot(inner[index, rows, :], matrix[index, :, width])
        whole = coulomb[rows, width].astype(jnp.float32) + second[index, rows, width] + third
        return whole.astype(jnp.bfloat16)

    for half in range(2):
        for t in range(1, classes):
            coords = unit_blocks(unit_of(first_mate + lax.rem(my_class + t, classes)), grid)[half]
            for index in range(2):
                screened[t, half, index] = wave(index, coords)
        for sub in range(SUBS):
            for t in range(1, classes):
                span_now = pl.ds(sub * sub_rows, sub_rows)
                remote(
                    screened.at[t, half, :, span_now], screen_in.at[my_class, half, :, span_now],
                    w_send.at[0], w_recv.at[half, sub], first_mate + lax.rem(my_class + t, classes),
                ).start()
    for half in range(2):
        for index in range(2):
            screen_in[my_class, half, index] = wave(index, own_blocks[half])

    def sigma_copy(half, sub, target):
        return remote(
            sigma_out.at[target, half, pl.ds(sub * sub_rows, sub_rows)],
            block_of(sigma, own_blocks[half], sub * sub_rows, sub_rows),
            s_send.at[0], s_recv.at[0], target,
        )

    def for_others(act):
        for other in range(volume):
            pl.when(me != other)(functools.partial(act, other))

    def send_sigma(n, targets):
        for target in range(volume):
            crosses = target // classes != me // classes
            chosen = crosses if targets else jnp.logical_and(me != target, jnp.logical_not(crosses))
            pl.when(chosen)(lambda: sigma_copy(*parts[n], target).start())

    for n, (half, sub) in enumerate(parts):
        took(
            screen_in.at[pl.ds(0, classes - 1), half, :, pl.ds(sub * sub_rows, sub_rows)],
            w_recv.at[half, sub],
        )

        def convolve(step, carry, half=half):
            rows = rows_of(step)
            if half == 0:
                mine = [landed[e, 0, rows, :].astype(jnp.float32) for e in range(volume)]
            else:
                mine = [second_half[e, rows, :].astype(jnp.float32) for e in range(volume)]
            waves = [
                screen_in[min(e, volume - e) % classes, half, e // classes, rows, :].astype(jnp.float32)
                for e in range(volume)
            ]
            for e in range(volume):
                acc = mine[0] * waves[e]
                for e2 in range(1, volume):
                    acc += mine[e2] * waves[(e - e2) % volume]
                sigma_out[e, half, rows, :] = (acc * scale_sigma).astype(jnp.bfloat16)
            return carry

        lax.fori_loop(sub * sub_rows // rows_at_once, (sub + 1) * sub_rows // rows_at_once, convolve, 0)
        send_sigma(n, True)
        send_sigma(n, False)
    for half in range(2):
        block_of(sigma, own_blocks[half])[...] = sigma_out[me, half]

    @pl.when(slab < slabs - 1)
    def _():
        corner_copy.wait_recv()
        near_next = plain_dot(coupling[...], next_corner[...]).astype(jnp.bfloat16)
        right_in[...] = plain_dot(near_next, turned[...]) * inv_root

    took(landed.at[others], s_recv.at[0])

    @pl.when(slab < slabs - 1)
    def _():
        sigma[last:, last:] = (sigma[last:, last:].astype(jnp.float32) + right_in[...]).astype(jnp.bfloat16)
        left_copy.wait_send()

    @pl.when(slab > 0)
    def _():
        left_copy.wait_recv()
        sigma[:size, :size] = (sigma[:size, :size].astype(jnp.float32) + left_in[...]).astype(jnp.bfloat16)
        corner_copy.wait_send()

    for chunk in range(CHUNKS):
        @pl.when(second_core > 0)
        def _():
            took(landed.at[others, :, span(chunk)], g_send.at[chunk])

        @pl.when(second_core == 0)
        def _():
            took(landed.at[others, :, span(chunk)], p_send.at[chunk])

    took(screen_in.at[pl.ds(0, classes - 1)], w_send.at[0])
    took(landed.at[others], s_send.at[0])

    @pl.when(diagonal == 1)
    def _():
        took(polar_out.at[pl.ds(0, 2)], m_send.at[0])


def dress_kernel(inv_root, total, green, out):
    dressed = plain_dot(green[...], total[...]).astype(jnp.bfloat16)
    updated = green[...].astype(jnp.float32) + plain_dot(dressed, green[...]) * inv_root
    out[...] = updated.astype(jnp.bfloat16)


def fused_on_device(grid, green_blocks, coulomb, couple_cols, couple_vals):
    volume = lax.axis_size("energy")
    slabs = lax.axis_size("slab")
    orbitals = green_blocks.shape[-1]
    size = orbitals // grid
    half_type = jnp.bfloat16

    def pieces(*lead):
        return pltpu.VMEM((*lead, size, size), half_type)

    def wholes(*lead, kind=half_type):
        return pltpu.VMEM((*lead, orbitals, orbitals), kind)

    def pair(sends, recvs):
        return [pltpu.SemaphoreType.DMA(sends), pltpu.SemaphoreType.DMA(recvs)]

    wide = pltpu.VMEM((size, size), jnp.float32)
    classes = volume // 2
    inv_root = 1.0 / math.sqrt(orbitals)
    in_vmem = pl.BlockSpec(memory_space=pltpu.VMEM)
    total, green = pl.pallas_call(
        functools.partial(
            fused_kernel, volume, slabs, grid,
            0.5 / math.sqrt(orbitals * volume), 0.2 / math.sqrt(volume), inv_root,
        ),
        out_shape=[jax.ShapeDtypeStruct((orbitals, orbitals), half_type)] * 2,
        in_specs=[pl.BlockSpec(memory_space=pltpu.HBM)] * 4,
        out_specs=[in_vmem] * 2,
        scratch_shapes=[
            wholes(), pltpu.VMEM(couple_cols.shape[:0:-1], jnp.int32), pltpu.VMEM(couple_vals.shape[:0:-1], half_type),
            pieces(volume), pieces(volume, 2), pieces(volume, 2), pieces(volume), pieces(classes, 2), pieces(2),
            wholes(2), wholes(2), wholes(2, kind=jnp.float32), pieces(classes, 2, 2),
            pieces(classes, 2, 2), pieces(volume, 2),
            pieces(), pieces(), pieces(), wide, wide, wide,
            *pair((CHUNKS,), (volume, CHUNKS)), *pair((CHUNKS,), (volume,)), *pair((1,), (1,)),
            *pair((1,), (2, SUBS)), *pair((1,), (1,)), *pair((2,), (2,)), pltpu.SemaphoreType.DMA((4,)),
            pltpu.SemaphoreType.REGULAR((1,)), pltpu.SemaphoreType.REGULAR((3,)),
        ],
        compiler_params=pltpu.CompilerParams(
            collective_id=0, has_side_effects=True, vmem_limit_bytes=32 << 20
        ),
    )(*(
        pltpu.with_memory_space_constraint(array, pltpu.HBM)
        for array in (green_blocks[0, 0], coulomb[0], couple_cols[0].T, couple_vals[0].T)
    ))
    result = pl.pallas_call(
        functools.partial(dress_kernel, inv_root),
        out_shape=jax.ShapeDtypeStruct((orbitals, orbitals), half_type),
        in_specs=[in_vmem] * 2,
        out_specs=in_vmem,
        compiler_params=pltpu.CompilerParams(vmem_limit_bytes=16 << 20),
    )(total, green)
    return result[None, None]


def fused_grid(mesh):
    volume = mesh.shape["energy"]
    grid = math.isqrt(2 * volume)
    return grid if grid * grid == 2 * volume and grid % 2 == 0 else 0


def on_any(grid, green_blocks, coulomb, couple_cols, couple_vals):
    orbitals = green_blocks.shape[-1]
    fits = (
        grid > 2
        and grid * 2 == lax.axis_size("energy")
        and green_blocks.shape[:2] == (1, 1)
        and orbitals % (128 * max(grid, 1)) == 0
        and couple_cols.shape[1] * grid == orbitals
        and lax.axis_size("slab") % 2 == 0
    )
    if fits:
        return fused_on_device(grid, green_blocks, coulomb, couple_cols, couple_vals)
    return on_device(green_blocks, coulomb, couple_cols, couple_vals)


def solution(mesh):
    return jax.shard_map(
        functools.partial(on_any, fused_grid(mesh)),
        mesh=mesh,
        in_specs=(
            P("energy", "slab", None, None),
            P("slab", None, None),
            P("slab", None, None),
            P("slab", None, None),
        ),
        out_specs=P("energy", "slab", None, None),
        check_vma=False,
    )
```

```python
import functools
import math

import jax
import jax.numpy as jnp
from jax import lax
from jax.experimental import pallas as pl
from jax.experimental.pallas import tpu as pltpu
from jax.sharding import PartitionSpec as P


def from_behind(x, axis, by):
    size = lax.axis_size(axis)
    pairs = [(i, i + by) for i in range(size) if 0 <= i + by < size]
    return lax.ppermute(x, axis, pairs)


def plain_dot(left, right):
    return jnp.dot(left, right, preferred_element_type=jnp.float32)


def split_parts(values):
    upper = values.astype(jnp.bfloat16)
    lower = (values - upper.astype(jnp.float32)).astype(jnp.bfloat16)
    return (upper, lower)


def coupling_matrix(column_ids, coupling_values):
    width = column_ids.shape[0]
    hits = column_ids[:, :, None] == jnp.arange(width, dtype=jnp.int32)[None, None, :]
    summed = jnp.sum(
        jnp.where(hits, coupling_values.astype(jnp.float32)[:, :, None], jnp.float32(0.0)), axis=1
    )
    return summed.astype(jnp.bfloat16)


def on_device(green_blocks, coulomb, couple_cols, couple_vals):
    own_green = green_blocks[:, 0]
    coulomb_block = coulomb[0]
    per_device = own_green.shape[0]
    orbitals = own_green.shape[1]
    volume = lax.axis_size("energy")
    energies = per_device * volume
    inv_root = 1.0 / math.sqrt(orbitals)
    flipped = jnp.swapaxes(own_green, 1, 2)
    received, flipped_recv = (
        lax.all_to_all(own_green, "energy", split_axis=1, concat_axis=0, tiled=True),
        lax.all_to_all(flipped, "energy", split_axis=1, concat_axis=0, tiled=True),
    )
    green_entries = received.reshape(energies, -1)
    flipped_entries = flipped_recv.reshape(energies, -1)
    entry_shape = received.shape
    halfway = energies // 2 + 1
    frequency = jnp.arange(halfway, dtype=jnp.int32)
    energy_index = jnp.arange(energies, dtype=jnp.int32)
    angles = (frequency[:, None] * energy_index[None, :] % energies).astype(jnp.float32) * (
        2.0 * math.pi / energies
    )
    cosine = jnp.cos(angles)
    sine = jnp.sin(angles)
    weights = (
        jnp.where((frequency == 0) | (2 * frequency == energies), 1.0, 2.0).astype(jnp.float32)
        / energies
    )
    forward_high, forward_low = split_parts(jnp.concatenate([cosine, -sine], axis=0))
    backward_table = jnp.concatenate(
        [cosine * weights[:, None], -sine * weights[:, None]], axis=0
    ).T
    backward_high, backward_low = split_parts(backward_table)

    def spectrum(entries):
        stacked = plain_dot(forward_high, entries) + plain_dot(forward_low, entries)
        return (stacked[:halfway], stacked[halfway:])

    def to_values(real_part, imag_part):
        data_high, data_low = split_parts(jnp.concatenate([real_part, imag_part], axis=0))
        return (
            plain_dot(backward_high, data_high)
            + plain_dot(backward_high, data_low)
            + plain_dot(backward_low, data_high)
        )

    green_real, green_imag = spectrum(green_entries)
    mirror_real, mirror_imag = spectrum(flipped_entries)
    polar_entries = to_values(
        green_real * mirror_real + green_imag * mirror_imag,
        green_imag * mirror_real - green_real * mirror_imag,
    )
    polar_entries = (polar_entries * (0.5 / math.sqrt(orbitals * energies))).astype(jnp.bfloat16)
    polar = lax.all_to_all(
        polar_entries.reshape(entry_shape), "energy", split_axis=0, concat_axis=1, tiled=True
    )
    inner = jnp.einsum(
        "ij,ejk->eik", coulomb_block, polar, preferred_element_type=jnp.float32
    ).astype(jnp.bfloat16)
    second = jnp.einsum("eij,jk->eik", inner, coulomb_block, preferred_element_type=jnp.float32)
    third = jnp.einsum(
        "eij,ejk->eik", inner, second.astype(jnp.bfloat16), preferred_element_type=jnp.float32
    )
    screened = (coulomb_block.astype(jnp.float32)[None] + second + third).astype(jnp.bfloat16)
    screened_entries = lax.all_to_all(
        screened, "energy", split_axis=1, concat_axis=0, tiled=True
    ).reshape(energies, -1)
    screen_real, screen_imag = spectrum(screened_entries)
    sigma_entries = to_values(
        green_real * screen_real - green_imag * screen_imag,
        green_real * screen_imag + green_imag * screen_real,
    )
    sigma_entries = (sigma_entries * (0.2 / math.sqrt(energies))).astype(jnp.bfloat16)
    sigma = lax.all_to_all(
        sigma_entries.reshape(entry_shape), "energy", split_axis=0, concat_axis=1, tiled=True
    )
    interface = couple_cols.shape[1]
    last = orbitals - interface
    coupling = coupling_matrix(couple_cols[0], couple_vals[0])
    prev_green, previous = from_behind((own_green, coupling), "slab", 1)
    next_green = from_behind(own_green, "slab", -1)
    prev_corner = prev_green[:, last:, last:]
    next_corner = next_green[:, :interface, :interface]
    near_next = jnp.einsum(
        "ij,ejk->eik", coupling, next_corner, preferred_element_type=jnp.float32
    ).astype(jnp.bfloat16)
    near_prev = jnp.einsum(
        "ji,ejk->eik", previous, prev_corner, preferred_element_type=jnp.float32
    ).astype(jnp.bfloat16)
    right_part = (
        jnp.einsum("eij,kj->eik", near_next, coupling, preferred_element_type=jnp.float32)
        * inv_root
    )
    left_part = (
        jnp.einsum("eij,jk->eik", near_prev, previous, preferred_element_type=jnp.float32)
        * inv_root
    )
    total = sigma.astype(jnp.float32)
    total = total.at[:, last:, last:].add(right_part)
    total = total.at[:, :interface, :interface].add(left_part)
    total_b = total.astype(jnp.bfloat16)
    dressed = jnp.einsum(
        "eij,ejk->eik", own_green, total_b, preferred_element_type=jnp.float32
    ).astype(jnp.bfloat16)
    updated = (
        own_green
        + jnp.einsum("eij,ejk->eik", dressed, own_green, preferred_element_type=jnp.float32)
        * inv_root
    )
    return updated.astype(jnp.bfloat16)[:, None]


MESH = pl.DeviceIdType.MESH


def unit_blocks(unit, grid):
    odd = grid - 1
    paired = grid * odd // 2
    slot = unit // odd
    turn = unit % odd
    diagonal = unit // paired
    first = (turn + slot) % odd
    second = (turn + odd - slot) % odd
    lone = 1 - (slot + odd - 1) // odd
    row = lone * odd + (1 - lone) * first
    col = lone * turn + (1 - lone) * second
    corner = 2 * (unit - paired)
    row0 = diagonal * corner + (1 - diagonal) * row
    col0 = diagonal * corner + (1 - diagonal) * col
    row1 = diagonal * (corner + 1) + (1 - diagonal) * col
    col1 = diagonal * (corner + 1) + (1 - diagonal) * row
    return ((row0, col0), (row1, col1))


CHUNKS = 1
SUBS = 2


def fused_kernel(
    volume, slabs, grid, scale_polar, scale_sigma, inv_root,
    green_hbm, coulomb_hbm, cols_hbm, vals_hbm, sigma, green,
    coulomb, cols, vals,
    stage, landed, mirror, second_half, polar_out, polar_more, matrix, inner, second, screened,
    screen_in, sigma_out,
    coupling, turned, next_corner, left_out, left_in, right_in,
    g_send, g_recv, p_send, p_recv, m_send, m_recv, w_send, w_recv, s_send, s_recv,
    slab_send, slab_recv, load_sem, turn, ready,
):
    loads = [
        pltpu.make_async_copy(source, target, load_sem.at[n])
        for n, (source, target) in enumerate(
            ((green_hbm, green), (coulomb_hbm, coulomb), (cols_hbm, cols), (vals_hbm, vals))
        )
    ]
    for load in loads:
        load.start()
    me = lax.axis_index("energy")
    slab = lax.axis_index("slab")
    size = green.shape[0] // grid
    last = green.shape[0] - size
    classes = volume // 2
    paired = grid * (grid - 1) // 2
    order = sorted(range(1, volume), key=lambda k: (-min(k, volume - k), k))
    has_prev = 1 - (slabs - 1 - slab + 0) // (slabs - 1)
    has_next = 1 - slab // (slabs - 1)
    planes = volume // 2
    plane = volume // planes
    level = me // plane
    inner_level = level * (planes - 1 - level) // (planes - 2)

    def unit_of(device):
        return lax.rem(device + volume // 2, volume)

    my_unit = unit_of(me)
    diagonal = my_unit // paired
    my_class = lax.rem(me, classes)
    first_mate = me - my_class
    own_blocks = unit_blocks(my_unit, grid)
    chunk_rows = size // CHUNKS

    def peer_of(k):
        return lax.rem(me + k, volume)

    def from_of(k):
        return lax.rem(me + volume - k, volume)

    barrier = pltpu.get_barrier_semaphore()

    def apart(device):
        steps = device // plane - level
        return steps * steps

    column = lax.rem(me, plane)

    def tier(device):
        aside = lax.rem(device, plane) - column
        return apart(device) * (apart(device) + 1) // 2 + aside * aside

    for k in order:
        @pl.when(tier(peer_of(k)) <= 1)
        def _():
            pl.semaphore_signal(barrier, inc=1, device_id=(peer_of(k), slab), device_id_type=MESH)

    @pl.when(slab > 0)
    def _():
        pl.semaphore_signal(barrier, inc=1, device_id=(me, slab - 1), device_id_type=MESH)

    @pl.when(slab < slabs - 1)
    def _():
        pl.semaphore_signal(barrier, inc=1, device_id=(me, slab + 1), device_id_type=MESH)

    def flipped(block):
        return block.T

    def region(coords, start=0, rows=None):
        rows = size if rows is None else rows
        row = pl.multiple_of(coords[0] * size + start, rows)
        col = pl.multiple_of(coords[1] * size, size)
        return pl.ds(row, rows), pl.ds(col, size)

    def block_of(ref, coords, start=0, rows=None):
        return ref.at[region(coords, start, rows)]

    def remote(src, dst, sends, recvs, device):
        return pltpu.make_async_remote_copy(
            src_ref=src, dst_ref=dst, send_sem=sends, recv_sem=recvs,
            device_id=(device, slab), device_id_type=MESH,
        )

    loads[0].wait()
    for unit in range(volume):
        coords = unit_blocks(unit, grid)[1]
        block = green[coords[0] * size:(coords[0] + 1) * size, coords[1] * size:(coords[1] + 1) * size]
        stage[unit] = block if unit >= paired else flipped(block)

    pl.semaphore_wait(barrier, inner_level + plane + has_prev + has_next)

    def tell(device, which):
        pl.semaphore_signal(ready.at[which], inc=1, device_id=(device, slab), device_id_type=MESH)

    for k in range(1, plane):
        tell(me - column + lax.rem(column + k, plane), 0)

    def took(shape, sem):
        pltpu.make_async_copy(shape, shape, sem).wait()

    others = pl.ds(0, volume - 1)

    def span(chunk):
        return pl.ds(chunk * chunk_rows, chunk_rows)

    def send_green(k):
        peer = peer_of(k)
        unit = unit_of(peer)
        for chunk in range(CHUNKS):
            for slot in range(2):
                if slot == 0:
                    source = block_of(green, unit_blocks(unit, grid)[0], chunk * chunk_rows, chunk_rows)
                else:
                    source = stage.at[unit, span(chunk)]
                remote(
                    source, landed.at[me, slot, span(chunk)], g_send.at[chunk], g_recv.at[k, chunk], peer
                ).start()

    def send_tier(low, high):
        for k in order[::-1]:
            distance = tier(peer_of(k))
            pl.when(jnp.logical_and(distance >= low, distance <= high))(functools.partial(send_green, k))

    send_tier(0, 1)
    pl.semaphore_wait(ready.at[0], plane - 1)

    @pl.when(inner_level > 0)
    def _():
        tell(me + plane, 1)
        tell(me - plane, 1)

    send_tier(2, 2)
    pl.semaphore_wait(ready.at[1], 1)

    @pl.when(level == 1)
    def _():
        tell(me - plane, 2)

    @pl.when(level == 2)
    def _():
        tell(me + plane, 2)

    send_tier(10, 11)

    @pl.when(inner_level == 0)
    def _():
        pl.semaphore_wait(ready.at[2], 1)
        send_tier(45, 46)

    landed[me, 0] = block_of(green, own_blocks[0])[...]
    landed[me, 1] = stage[my_unit]

    corner_copy = pltpu.make_async_remote_copy(
        src_ref=green.at[pl.ds(0, size), pl.ds(0, size)], dst_ref=next_corner,
        send_sem=slab_send.at[0], recv_sem=slab_recv.at[0],
        device_id=(me, slab - has_prev), device_id_type=MESH,
    )
    left_copy = pltpu.make_async_remote_copy(
        src_ref=left_out, dst_ref=left_in,
        send_sem=slab_send.at[1], recv_sem=slab_recv.at[1],
        device_id=(me, slab + has_next), device_id_type=MESH,
    )

    @pl.when(slab > 0)
    def _():
        corner_copy.start()

    loads[2].wait()
    loads[3].wait()
    ids = cols[...]
    values = vals[...].astype(jnp.float32)
    columns = lax.broadcasted_iota(jnp.int32, (size, size), 0)
    summed = jnp.zeros((size, size), jnp.float32)
    for k in range(ids.shape[0]):
        summed += jnp.where(ids[k:k + 1, :] == columns, values[k:k + 1, :], jnp.float32(0.0))
    summed = summed.astype(jnp.bfloat16).astype(jnp.float32)
    turned[...] = summed.astype(jnp.bfloat16)
    coupling[...] = summed.T.astype(jnp.bfloat16)

    @pl.when(slab < slabs - 1)
    def _():
        near_prev = plain_dot(turned[...], green[last:, last:]).astype(jnp.bfloat16)
        left_out[...] = plain_dot(near_prev, coupling[...]) * inv_root
        left_copy.start()

    second_core = 1 - lax.rem(slab, 2)
    partner = slab - 1 + 2 * second_core

    @pl.when(second_core == 0)
    def _():
        for chunk in range(CHUNKS):
            took(landed.at[others, :, span(chunk)], g_send.at[chunk])
        pl.semaphore_signal(turn.at[0], inc=1, device_id=(me, partner), device_id_type=MESH)

    loads[1].wait()
    rows_at_once = 16
    steps = chunk_rows // rows_at_once

    def rows_of(step):
        return pl.ds(pl.multiple_of(step * rows_at_once, rows_at_once), rows_at_once)

    def correlation(mine, theirs, e):
        acc = mine[0] * theirs[(0 - e) % volume]
        for e2 in range(1, volume):
            acc += mine[e2] * theirs[(e2 - e) % volume]
        return (acc * scale_polar).astype(jnp.bfloat16)

    where = (
        (0, own_blocks[0]),
        (1 - diagonal, tuple(
            diagonal * d + (1 - diagonal) * o for d, o in zip(own_blocks[1], own_blocks[0])
        )),
    )

    def polar_copy(k, chunk, slot):
        peer = peer_of(k)
        index, coords = where[slot]
        return remote(
            polar_out.at[lax.rem(peer, classes), slot, span(chunk)],
            block_of(matrix.at[index], coords, chunk * chunk_rows, chunk_rows),
            p_send.at[chunk], p_recv.at[k], peer,
        )

    def send_polar(chunk):
        if chunk == 0:
            pl.semaphore_wait(turn.at[0], 1)
        for slot in range(2):
            for k in order:
                polar_copy(k, chunk, slot).start()

    def more_copy(target, slot):
        return remote(
            polar_more.at[slot],
            block_of(matrix.at[1], own_blocks[slot]),
            m_send.at[0], m_recv.at[0], target * classes,
        )

    def green_arrived(k, chunk):
        took(landed.at[from_of(k), :, span(chunk)], g_recv.at[k, chunk])

    @pl.when(diagonal == 0)
    def _():
        for chunk in range(CHUNKS):
            for k in order:
                green_arrived(k, chunk)

            def correlate(step, carry):
                rows = rows_of(step)
                mine = [landed[e, 0, rows, :].astype(jnp.float32) for e in range(volume)]
                theirs = [landed[e, 1, rows, :].astype(jnp.float32) for e in range(volume)]
                for e in range(volume):
                    if e % classes == 0:
                        place = (0, e // classes)
                    else:
                        place = (min(e, volume - e), e // classes)
                    polar_out[place[0], place[1], rows, :] = correlation(mine, theirs, e)
                return carry

            lax.fori_loop(chunk * steps, (chunk + 1) * steps, correlate, 0)
            send_polar(chunk)

    @pl.when(diagonal == 1)
    def _():
        def flip_both(e):
            for slot in range(2):
                mirror[e, slot] = flipped(landed[e, slot])

        flip_both(me)
        for k in order:
            for chunk in range(CHUNKS):
                green_arrived(k, chunk)
            flip_both(from_of(k))

        for slot in range(2):
            def correlate(step, carry, slot=slot):
                rows = rows_of(step)
                mine = [landed[e, slot, rows, :].astype(jnp.float32) for e in range(volume)]
                theirs = [mirror[e, slot, rows, :].astype(jnp.float32) for e in range(volume)]
                for e in range(classes):
                    polar_out[e, slot, rows, :] = correlation(mine, theirs, e)
                polar_more[slot, rows, :] = correlation(mine, theirs, classes)
                return carry

            lax.fori_loop(0, size // rows_at_once, correlate, 0)
        for chunk in range(CHUNKS):
            send_polar(chunk)
        for target in range(2):
            for slot in range(2):
                more_copy(target, slot).start()

    for slot in range(2):
        index, coords = where[slot]
        block_of(matrix.at[index], coords)[...] = polar_out[my_class, slot]

    @pl.when(diagonal == 0)
    def _():
        for e in range(volume):
            second_half[e] = flipped(landed[e, 1])

    @pl.when(diagonal == 1)
    def _():
        for e in range(volume):
            second_half[e] = landed[e, 1]

    @pl.when(second_core == 1)
    def _():
        for chunk in range(CHUNKS):
            took(landed.at[others, :, span(chunk)], p_send.at[chunk])
        pl.semaphore_signal(turn.at[0], inc=1, device_id=(me, partner), device_id_type=MESH)

    swapped = 1 - lax.rem(my_class + classes - 1, classes) // (classes - 1)

    def complete(device):
        unit = unit_of(device)
        coords = unit_blocks(unit, grid)
        off = 1 - unit // paired

        @pl.when(off == 1)
        def _():
            for index in range(2):
                source = swapped * (1 - index) + (1 - swapped) * index
                block_of(matrix.at[index], coords[1])[...] = flipped(
                    block_of(matrix.at[source], coords[0])[...]
                )

        @pl.when(jnp.logical_and(off == 0, my_class > 0))
        def _():
            for slot in range(2):
                block_of(matrix.at[1], coords[slot])[...] = flipped(
                    block_of(matrix.at[0], coords[slot])[...]
                )

    complete(me)
    for k in order:
        took(polar_out.at[0], p_recv.at[k])
        complete(from_of(k))

    @pl.when(my_class == 0)
    def _():
        took(polar_out.at[pl.ds(0, volume - paired)], m_recv.at[0])

    for index in range(2):
        inner[index] = plain_dot(coulomb[...], matrix[index]).astype(jnp.bfloat16)
    for index in range(2):
        product = plain_dot(inner[index], coulomb[...])
        second[index] = product
        matrix[index] = product.astype(jnp.bfloat16)
    parts = [(half, sub) for half in range(2) for sub in range(SUBS)]
    sub_rows = size // SUBS

    def wave(index, coords):
        rows, width = region(coords)
        third = plain_dot(inner[index, rows, :], matrix[index, :, width])
        whole = coulomb[rows, width].astype(jnp.float32) + second[index, rows, width] + third
        return whole.astype(jnp.bfloat16)

    for half in range(2):
        for t in range(1, classes):
            coords = unit_blocks(unit_of(first_mate + lax.rem(my_class + t, classes)), grid)[half]
            for index in range(2):
                screened[t, half, index] = wave(index, coords)
        for sub in range(SUBS):
            for t in range(1, classes):
                span_now = pl.ds(sub * sub_rows, sub_rows)
                remote(
                    screened.at[t, half, :, span_now], screen_in.at[my_class, half, :, span_now],
                    w_send.at[0], w_recv.at[half, sub], first_mate + lax.rem(my_class + t, classes),
                ).start()
    for half in range(2):
        for index in range(2):
            screen_in[my_class, half, index] = wave(index, own_blocks[half])

    def sigma_copy(half, sub, target):
        return remote(
            sigma_out.at[target, half, pl.ds(sub * sub_rows, sub_rows)],
            block_of(sigma, own_blocks[half], sub * sub_rows, sub_rows),
            s_send.at[0], s_recv.at[0], target,
        )

    def for_others(act):
        for other in range(volume):
            pl.when(me != other)(functools.partial(act, other))

    def send_sigma(n, targets):
        for target in range(volume):
            crosses = target // classes != me // classes
            chosen = crosses if targets else jnp.logical_and(me != target, jnp.logical_not(crosses))
            pl.when(chosen)(lambda: sigma_copy(*parts[n], target).start())

    for n, (half, sub) in enumerate(parts):
        took(
            screen_in.at[pl.ds(0, classes - 1), half, :, pl.ds(sub * sub_rows, sub_rows)],
            w_recv.at[half, sub],
        )

        def convolve(step, carry, half=half):
            rows = rows_of(step)
            if half == 0:
                mine = [landed[e, 0, rows, :].astype(jnp.float32) for e in range(volume)]
            else:
                mine = [second_half[e, rows, :].astype(jnp.float32) for e in range(volume)]
            waves = [
                screen_in[min(e, volume - e) % classes, half, e // classes, rows, :].astype(jnp.float32)
                for e in range(volume)
            ]
            for e in range(volume):
                acc = mine[0] * waves[e]
                for e2 in range(1, volume):
                    acc += mine[e2] * waves[(e - e2) % volume]
                sigma_out[e, half, rows, :] = (acc * scale_sigma).astype(jnp.bfloat16)
            return carry

        lax.fori_loop(sub * sub_rows // rows_at_once, (sub + 1) * sub_rows // rows_at_once, convolve, 0)
        send_sigma(n, True)
        send_sigma(n, False)
    for half in range(2):
        block_of(sigma, own_blocks[half])[...] = sigma_out[me, half]

    @pl.when(slab < slabs - 1)
    def _():
        corner_copy.wait_recv()
        near_next = plain_dot(coupling[...], next_corner[...]).astype(jnp.bfloat16)
        right_in[...] = plain_dot(near_next, turned[...]) * inv_root

    took(landed.at[others], s_recv.at[0])

    @pl.when(slab < slabs - 1)
    def _():
        sigma[last:, last:] = (sigma[last:, last:].astype(jnp.float32) + right_in[...]).astype(jnp.bfloat16)
        left_copy.wait_send()

    @pl.when(slab > 0)
    def _():
        left_copy.wait_recv()
        sigma[:size, :size] = (sigma[:size, :size].astype(jnp.float32) + left_in[...]).astype(jnp.bfloat16)
        corner_copy.wait_send()

    for chunk in range(CHUNKS):
        @pl.when(second_core > 0)
        def _():
            took(landed.at[others, :, span(chunk)], g_send.at[chunk])

        @pl.when(second_core == 0)
        def _():
            took(landed.at[others, :, span(chunk)], p_send.at[chunk])

    took(screen_in.at[pl.ds(0, classes - 1)], w_send.at[0])
    took(landed.at[others], s_send.at[0])

    @pl.when(diagonal == 1)
    def _():
        took(polar_out.at[pl.ds(0, 2)], m_send.at[0])


def dress_kernel(inv_root, total, green, out):
    dressed = plain_dot(green[...], total[...]).astype(jnp.bfloat16)
    updated = green[...].astype(jnp.float32) + plain_dot(dressed, green[...]) * inv_root
    out[...] = updated.astype(jnp.bfloat16)


def fused_on_device(grid, green_blocks, coulomb, couple_cols, couple_vals):
    volume = lax.axis_size("energy")
    slabs = lax.axis_size("slab")
    orbitals = green_blocks.shape[-1]
    size = orbitals // grid
    half_type = jnp.bfloat16

    def pieces(*lead):
        return pltpu.VMEM((*lead, size, size), half_type)

    def wholes(*lead, kind=half_type):
        return pltpu.VMEM((*lead, orbitals, orbitals), kind)

    def pair(sends, recvs):
        return [pltpu.SemaphoreType.DMA(sends), pltpu.SemaphoreType.DMA(recvs)]

    wide = pltpu.VMEM((size, size), jnp.float32)
    classes = volume // 2
    inv_root = 1.0 / math.sqrt(orbitals)
    in_vmem = pl.BlockSpec(memory_space=pltpu.VMEM)
    total, green = pl.pallas_call(
        functools.partial(
            fused_kernel, volume, slabs, grid,
            0.5 / math.sqrt(orbitals * volume), 0.2 / math.sqrt(volume), inv_root,
        ),
        out_shape=[jax.ShapeDtypeStruct((orbitals, orbitals), half_type)] * 2,
        in_specs=[pl.BlockSpec(memory_space=pltpu.HBM)] * 4,
        out_specs=[in_vmem] * 2,
        scratch_shapes=[
            wholes(), pltpu.VMEM(couple_cols.shape[:0:-1], jnp.int32), pltpu.VMEM(couple_vals.shape[:0:-1], half_type),
            pieces(volume), pieces(volume, 2), pieces(volume, 2), pieces(volume), pieces(classes, 2), pieces(2),
            wholes(2), wholes(2), wholes(2, kind=jnp.float32), pieces(classes, 2, 2),
            pieces(classes, 2, 2), pieces(volume, 2),
            pieces(), pieces(), pieces(), wide, wide, wide,
            *pair((CHUNKS,), (volume, CHUNKS)), *pair((CHUNKS,), (volume,)), *pair((1,), (1,)),
            *pair((1,), (2, SUBS)), *pair((1,), (1,)), *pair((2,), (2,)), pltpu.SemaphoreType.DMA((4,)),
            pltpu.SemaphoreType.REGULAR((1,)), pltpu.SemaphoreType.REGULAR((3,)),
        ],
        compiler_params=pltpu.CompilerParams(
            collective_id=0, has_side_effects=True, vmem_limit_bytes=32 << 20
        ),
    )(*(
        pltpu.with_memory_space_constraint(array, pltpu.HBM)
        for array in (green_blocks[0, 0], coulomb[0], couple_cols[0].T, couple_vals[0].T)
    ))
    result = pl.pallas_call(
        functools.partial(dress_kernel, inv_root),
        out_shape=jax.ShapeDtypeStruct((orbitals, orbitals), half_type),
        in_specs=[in_vmem] * 2,
        out_specs=in_vmem,
        compiler_params=pltpu.CompilerParams(vmem_limit_bytes=16 << 20),
    )(total, green)
    return result[None, None]


def fused_grid(mesh):
    volume = mesh.shape["energy"]
    grid = math.isqrt(2 * volume)
    return grid if grid * grid == 2 * volume and grid % 2 == 0 else 0


def on_any(grid, green_blocks, coulomb, couple_cols, couple_vals):
    orbitals = green_blocks.shape[-1]
    fits = (
        grid > 2
        and grid * 2 == lax.axis_size("energy")
        and green_blocks.shape[:2] == (1, 1)
        and orbitals % (128 * max(grid, 1)) == 0
        and couple_cols.shape[1] * grid == orbitals
        and lax.axis_size("slab") % 2 == 0
    )
    if fits:
        return fused_on_device(grid, green_blocks, coulomb, couple_cols, couple_vals)
    return on_device(green_blocks, coulomb, couple_cols, couple_vals)


def solution(mesh):
    return jax.shard_map(
        functools.partial(on_any, fused_grid(mesh)),
        mesh=mesh,
        in_specs=(
            P("energy", "slab", None, None),
            P("slab", None, None),
            P("slab", None, None),
            P("slab", None, None),
        ),
        out_specs=P("energy", "slab", None, None),
        check_vma=False,
    )
```

```python
import functools
import math

import jax
import jax.numpy as jnp
from jax import lax
from jax.experimental import pallas as pl
from jax.experimental.pallas import tpu as pltpu
from jax.sharding import PartitionSpec as P


def from_behind(x, axis, by):
    size = lax.axis_size(axis)
    pairs = [(i, i + by) for i in range(size) if 0 <= i + by < size]
    return lax.ppermute(x, axis, pairs)


def plain_dot(left, right):
    return jnp.dot(left, right, preferred_element_type=jnp.float32)


def split_parts(values):
    upper = values.astype(jnp.bfloat16)
    lower = (values - upper.astype(jnp.float32)).astype(jnp.bfloat16)
    return (upper, lower)


def coupling_matrix(column_ids, coupling_values):
    width = column_ids.shape[0]
    hits = column_ids[:, :, None] == jnp.arange(width, dtype=jnp.int32)[None, None, :]
    summed = jnp.sum(
        jnp.where(hits, coupling_values.astype(jnp.float32)[:, :, None], jnp.float32(0.0)), axis=1
    )
    return summed.astype(jnp.bfloat16)


def on_device(green_blocks, coulomb, couple_cols, couple_vals):
    own_green = green_blocks[:, 0]
    coulomb_block = coulomb[0]
    per_device = own_green.shape[0]
    orbitals = own_green.shape[1]
    volume = lax.axis_size("energy")
    energies = per_device * volume
    inv_root = 1.0 / math.sqrt(orbitals)
    flipped = jnp.swapaxes(own_green, 1, 2)
    received, flipped_recv = (
        lax.all_to_all(own_green, "energy", split_axis=1, concat_axis=0, tiled=True),
        lax.all_to_all(flipped, "energy", split_axis=1, concat_axis=0, tiled=True),
    )
    green_entries = received.reshape(energies, -1)
    flipped_entries = flipped_recv.reshape(energies, -1)
    entry_shape = received.shape
    halfway = energies // 2 + 1
    frequency = jnp.arange(halfway, dtype=jnp.int32)
    energy_index = jnp.arange(energies, dtype=jnp.int32)
    angles = (frequency[:, None] * energy_index[None, :] % energies).astype(jnp.float32) * (
        2.0 * math.pi / energies
    )
    cosine = jnp.cos(angles)
    sine = jnp.sin(angles)
    weights = (
        jnp.where((frequency == 0) | (2 * frequency == energies), 1.0, 2.0).astype(jnp.float32)
        / energies
    )
    forward_high, forward_low = split_parts(jnp.concatenate([cosine, -sine], axis=0))
    backward_table = jnp.concatenate(
        [cosine * weights[:, None], -sine * weights[:, None]], axis=0
    ).T
    backward_high, backward_low = split_parts(backward_table)

    def spectrum(entries):
        stacked = plain_dot(forward_high, entries) + plain_dot(forward_low, entries)
        return (stacked[:halfway], stacked[halfway:])

    def to_values(real_part, imag_part):
        data_high, data_low = split_parts(jnp.concatenate([real_part, imag_part], axis=0))
        return (
            plain_dot(backward_high, data_high)
            + plain_dot(backward_high, data_low)
            + plain_dot(backward_low, data_high)
        )

    green_real, green_imag = spectrum(green_entries)
    mirror_real, mirror_imag = spectrum(flipped_entries)
    polar_entries = to_values(
        green_real * mirror_real + green_imag * mirror_imag,
        green_imag * mirror_real - green_real * mirror_imag,
    )
    polar_entries = (polar_entries * (0.5 / math.sqrt(orbitals * energies))).astype(jnp.bfloat16)
    polar = lax.all_to_all(
        polar_entries.reshape(entry_shape), "energy", split_axis=0, concat_axis=1, tiled=True
    )
    inner = jnp.einsum(
        "ij,ejk->eik", coulomb_block, polar, preferred_element_type=jnp.float32
    ).astype(jnp.bfloat16)
    second = jnp.einsum("eij,jk->eik", inner, coulomb_block, preferred_element_type=jnp.float32)
    third = jnp.einsum(
        "eij,ejk->eik", inner, second.astype(jnp.bfloat16), preferred_element_type=jnp.float32
    )
    screened = (coulomb_block.astype(jnp.float32)[None] + second + third).astype(jnp.bfloat16)
    screened_entries = lax.all_to_all(
        screened, "energy", split_axis=1, concat_axis=0, tiled=True
    ).reshape(energies, -1)
    screen_real, screen_imag = spectrum(screened_entries)
    sigma_entries = to_values(
        green_real * screen_real - green_imag * screen_imag,
        green_real * screen_imag + green_imag * screen_real,
    )
    sigma_entries = (sigma_entries * (0.2 / math.sqrt(energies))).astype(jnp.bfloat16)
    sigma = lax.all_to_all(
        sigma_entries.reshape(entry_shape), "energy", split_axis=0, concat_axis=1, tiled=True
    )
    interface = couple_cols.shape[1]
    last = orbitals - interface
    coupling = coupling_matrix(couple_cols[0], couple_vals[0])
    prev_green, previous = from_behind((own_green, coupling), "slab", 1)
    next_green = from_behind(own_green, "slab", -1)
    prev_corner = prev_green[:, last:, last:]
    next_corner = next_green[:, :interface, :interface]
    near_next = jnp.einsum(
        "ij,ejk->eik", coupling, next_corner, preferred_element_type=jnp.float32
    ).astype(jnp.bfloat16)
    near_prev = jnp.einsum(
        "ji,ejk->eik", previous, prev_corner, preferred_element_type=jnp.float32
    ).astype(jnp.bfloat16)
    right_part = (
        jnp.einsum("eij,kj->eik", near_next, coupling, preferred_element_type=jnp.float32)
        * inv_root
    )
    left_part = (
        jnp.einsum("eij,jk->eik", near_prev, previous, preferred_element_type=jnp.float32)
        * inv_root
    )
    total = sigma.astype(jnp.float32)
    total = total.at[:, last:, last:].add(right_part)
    total = total.at[:, :interface, :interface].add(left_part)
    total_b = total.astype(jnp.bfloat16)
    dressed = jnp.einsum(
        "eij,ejk->eik", own_green, total_b, preferred_element_type=jnp.float32
    ).astype(jnp.bfloat16)
    updated = (
        own_green
        + jnp.einsum("eij,ejk->eik", dressed, own_green, preferred_element_type=jnp.float32)
        * inv_root
    )
    return updated.astype(jnp.bfloat16)[:, None]


MESH = pl.DeviceIdType.MESH


def unit_blocks(unit, grid):
    odd = grid - 1
    paired = grid * odd // 2
    slot = unit // odd
    turn = unit % odd
    diagonal = unit // paired
    first = (turn + slot) % odd
    second = (turn + odd - slot) % odd
    lone = 1 - (slot + odd - 1) // odd
    row = lone * odd + (1 - lone) * first
    col = lone * turn + (1 - lone) * second
    corner = 2 * (unit - paired)
    row0 = diagonal * corner + (1 - diagonal) * row
    col0 = diagonal * corner + (1 - diagonal) * col
    row1 = diagonal * (corner + 1) + (1 - diagonal) * col
    col1 = diagonal * (corner + 1) + (1 - diagonal) * row
    return ((row0, col0), (row1, col1))


CHUNKS = 1
SUBS = 2


def fused_kernel(
    volume, slabs, grid, scale_polar, scale_sigma, inv_root,
    green_hbm, coulomb_hbm, cols_hbm, vals_hbm, sigma, green,
    coulomb, cols, vals,
    stage, landed, mirror, second_half, polar_out, polar_more, matrix, inner, second, screened,
    screen_in, sigma_out,
    coupling, turned, next_corner, left_out, left_in, right_in,
    g_send, g_recv, p_send, p_recv, m_send, m_recv, w_send, w_recv, s_send, s_recv,
    slab_send, slab_recv, load_sem, turn, ready,
):
    loads = [
        pltpu.make_async_copy(source, target, load_sem.at[n])
        for n, (source, target) in enumerate(
            ((green_hbm, green), (coulomb_hbm, coulomb), (cols_hbm, cols), (vals_hbm, vals))
        )
    ]
    for load in loads:
        load.start()
    me = lax.axis_index("energy")
    slab = lax.axis_index("slab")
    size = green.shape[0] // grid
    last = green.shape[0] - size
    classes = volume // 2
    paired = grid * (grid - 1) // 2
    order = sorted(range(1, volume), key=lambda k: (-min(k, volume - k), k))
    has_prev = 1 - (slabs - 1 - slab + 0) // (slabs - 1)
    has_next = 1 - slab // (slabs - 1)
    planes = volume // 2
    plane = volume // planes
    level = me // plane
    inner_level = level * (planes - 1 - level) // (planes - 2)

    def unit_of(device):
        return lax.rem(device + volume // 2, volume)

    my_unit = unit_of(me)
    diagonal = my_unit // paired
    my_class = lax.rem(me, classes)
    first_mate = me - my_class
    own_blocks = unit_blocks(my_unit, grid)
    chunk_rows = size // CHUNKS

    def peer_of(k):
        return lax.rem(me + k, volume)

    def from_of(k):
        return lax.rem(me + volume - k, volume)

    barrier = pltpu.get_barrier_semaphore()

    def apart(device):
        steps = device // plane - level
        return steps * steps

    column = lax.rem(me, plane)

    def tier(device):
        aside = lax.rem(device, plane) - column
        return apart(device) * (apart(device) + 1) // 2 + aside * aside

    for k in order:
        @pl.when(tier(peer_of(k)) <= 1)
        def _():
            pl.semaphore_signal(barrier, inc=1, device_id=(peer_of(k), slab), device_id_type=MESH)

    @pl.when(slab > 0)
    def _():
        pl.semaphore_signal(barrier, inc=1, device_id=(me, slab - 1), device_id_type=MESH)

    @pl.when(slab < slabs - 1)
    def _():
        pl.semaphore_signal(barrier, inc=1, device_id=(me, slab + 1), device_id_type=MESH)

    def flipped(block):
        return block.T

    def region(coords, start=0, rows=None):
        rows = size if rows is None else rows
        row = pl.multiple_of(coords[0] * size + start, rows)
        col = pl.multiple_of(coords[1] * size, size)
        return pl.ds(row, rows), pl.ds(col, size)

    def block_of(ref, coords, start=0, rows=None):
        return ref.at[region(coords, start, rows)]

    def remote(src, dst, sends, recvs, device):
        return pltpu.make_async_remote_copy(
            src_ref=src, dst_ref=dst, send_sem=sends, recv_sem=recvs,
            device_id=(device, slab), device_id_type=MESH,
        )

    loads[0].wait()
    pl.semaphore_wait(barrier, inner_level + plane + has_prev + has_next)

    def tell(device, which):
        pl.semaphore_signal(ready.at[which], inc=1, device_id=(device, slab), device_id_type=MESH)

    for k in range(1, plane):
        tell(me - column + lax.rem(column + k, plane), 0)

    def took(shape, sem):
        pltpu.make_async_copy(shape, shape, sem).wait()

    others = pl.ds(0, volume - 1)

    def span(chunk):
        return pl.ds(chunk * chunk_rows, chunk_rows)

    def send_green(slots, k):
        peer = peer_of(k)
        unit = unit_of(peer)
        for chunk in range(CHUNKS):
            for slot in slots:
                if slot == 0:
                    source = block_of(green, unit_blocks(unit, grid)[0], chunk * chunk_rows, chunk_rows)
                else:
                    source = stage.at[unit, span(chunk)]
                remote(
                    source, landed.at[me, slot, span(chunk)], g_send.at[chunk], g_recv.at[k, chunk], peer
                ).start()

    def send_tier(low, high, slots=(0, 1)):
        for k in order[::-1]:
            distance = tier(peer_of(k))
            pl.when(jnp.logical_and(distance >= low, distance <= high))(functools.partial(send_green, slots, k))

    send_tier(0, 1, (0,))
    for unit in range(volume):
        coords = unit_blocks(unit, grid)[1]
        block = green[coords[0] * size:(coords[0] + 1) * size, coords[1] * size:(coords[1] + 1) * size]
        stage[unit] = block if unit >= paired else flipped(block)

    send_tier(0, 1, (1,))
    pl.semaphore_wait(ready.at[0], plane - 1)

    @pl.when(inner_level > 0)
    def _():
        tell(me + plane, 1)
        tell(me - plane, 1)

    send_tier(2, 2)
    pl.semaphore_wait(ready.at[1], 1)

    @pl.when(level == 1)
    def _():
        tell(me - plane, 2)

    @pl.when(level == 2)
    def _():
        tell(me + plane, 2)

    send_tier(10, 11)

    @pl.when(inner_level == 0)
    def _():
        pl.semaphore_wait(ready.at[2], 1)
        send_tier(45, 46)

    landed[me, 0] = block_of(green, own_blocks[0])[...]
    landed[me, 1] = stage[my_unit]

    corner_copy = pltpu.make_async_remote_copy(
        src_ref=green.at[pl.ds(0, size), pl.ds(0, size)], dst_ref=next_corner,
        send_sem=slab_send.at[0], recv_sem=slab_recv.at[0],
        device_id=(me, slab - has_prev), device_id_type=MESH,
    )
    left_copy = pltpu.make_async_remote_copy(
        src_ref=left_out, dst_ref=left_in,
        send_sem=slab_send.at[1], recv_sem=slab_recv.at[1],
        device_id=(me, slab + has_next), device_id_type=MESH,
    )

    @pl.when(slab > 0)
    def _():
        corner_copy.start()

    loads[2].wait()
    loads[3].wait()
    ids = cols[...]
    values = vals[...].astype(jnp.float32)
    columns = lax.broadcasted_iota(jnp.int32, (size, size), 0)
    summed = jnp.zeros((size, size), jnp.float32)
    for k in range(ids.shape[0]):
        summed += jnp.where(ids[k:k + 1, :] == columns, values[k:k + 1, :], jnp.float32(0.0))
    summed = summed.astype(jnp.bfloat16).astype(jnp.float32)
    turned[...] = summed.astype(jnp.bfloat16)
    coupling[...] = summed.T.astype(jnp.bfloat16)

    @pl.when(slab < slabs - 1)
    def _():
        near_prev = plain_dot(turned[...], green[last:, last:]).astype(jnp.bfloat16)
        left_out[...] = plain_dot(near_prev, coupling[...]) * inv_root
        left_copy.start()

    second_core = 1 - lax.rem(slab, 2)
    partner = slab - 1 + 2 * second_core

    @pl.when(second_core == 0)
    def _():
        for chunk in range(CHUNKS):
            took(landed.at[others, :, span(chunk)], g_send.at[chunk])
        pl.semaphore_signal(turn.at[0], inc=1, device_id=(me, partner), device_id_type=MESH)

    loads[1].wait()
    rows_at_once = 16
    steps = chunk_rows // rows_at_once

    def rows_of(step):
        return pl.ds(pl.multiple_of(step * rows_at_once, rows_at_once), rows_at_once)

    def correlation(mine, theirs, e):
        acc = mine[0] * theirs[(0 - e) % volume]
        for e2 in range(1, volume):
            acc += mine[e2] * theirs[(e2 - e) % volume]
        return (acc * scale_polar).astype(jnp.bfloat16)

    where = (
        (0, own_blocks[0]),
        (1 - diagonal, tuple(
            diagonal * d + (1 - diagonal) * o for d, o in zip(own_blocks[1], own_blocks[0])
        )),
    )

    def polar_copy(k, chunk, slot):
        peer = peer_of(k)
        index, coords = where[slot]
        return remote(
            polar_out.at[lax.rem(peer, classes), slot, span(chunk)],
            block_of(matrix.at[index], coords, chunk * chunk_rows, chunk_rows),
            p_send.at[chunk], p_recv.at[k], peer,
        )

    def send_polar(chunk):
        if chunk == 0:
            pl.semaphore_wait(turn.at[0], 1)
        for slot in range(2):
            for k in order:
                polar_copy(k, chunk, slot).start()

    def more_copy(target, slot):
        return remote(
            polar_more.at[slot],
            block_of(matrix.at[1], own_blocks[slot]),
            m_send.at[0], m_recv.at[0], target * classes,
        )

    def green_arrived(k, chunk):
        took(landed.at[from_of(k), :, span(chunk)], g_recv.at[k, chunk])

    @pl.when(diagonal == 0)
    def _():
        for chunk in range(CHUNKS):
            for k in order:
                green_arrived(k, chunk)

            def correlate(step, carry):
                rows = rows_of(step)
                mine = [landed[e, 0, rows, :].astype(jnp.float32) for e in range(volume)]
                theirs = [landed[e, 1, rows, :].astype(jnp.float32) for e in range(volume)]
                for e in range(volume):
                    if e % classes == 0:
                        place = (0, e // classes)
                    else:
                        place = (min(e, volume - e), e // classes)
                    polar_out[place[0], place[1], rows, :] = correlation(mine, theirs, e)
                return carry

            lax.fori_loop(chunk * steps, (chunk + 1) * steps, correlate, 0)
            send_polar(chunk)

    @pl.when(diagonal == 1)
    def _():
        def flip_both(e):
            for slot in range(2):
                mirror[e, slot] = flipped(landed[e, slot])

        flip_both(me)
        for k in order:
            for chunk in range(CHUNKS):
                green_arrived(k, chunk)
            flip_both(from_of(k))

        for slot in range(2):
            def correlate(step, carry, slot=slot):
                rows = rows_of(step)
                mine = [landed[e, slot, rows, :].astype(jnp.float32) for e in range(volume)]
                theirs = [mirror[e, slot, rows, :].astype(jnp.float32) for e in range(volume)]
                for e in range(classes):
                    polar_out[e, slot, rows, :] = correlation(mine, theirs, e)
                polar_more[slot, rows, :] = correlation(mine, theirs, classes)
                return carry

            lax.fori_loop(0, size // rows_at_once, correlate, 0)
        for chunk in range(CHUNKS):
            send_polar(chunk)
        for target in range(2):
            for slot in range(2):
                more_copy(target, slot).start()

    for slot in range(2):
        index, coords = where[slot]
        block_of(matrix.at[index], coords)[...] = polar_out[my_class, slot]

    @pl.when(diagonal == 0)
    def _():
        for e in range(volume):
            second_half[e] = flipped(landed[e, 1])

    @pl.when(diagonal == 1)
    def _():
        for e in range(volume):
            second_half[e] = landed[e, 1]

    @pl.when(second_core == 1)
    def _():
        for chunk in range(CHUNKS):
            took(landed.at[others, :, span(chunk)], p_send.at[chunk])
        pl.semaphore_signal(turn.at[0], inc=1, device_id=(me, partner), device_id_type=MESH)

    swapped = 1 - lax.rem(my_class + classes - 1, classes) // (classes - 1)

    def complete(device):
        unit = unit_of(device)
        coords = unit_blocks(unit, grid)
        off = 1 - unit // paired

        @pl.when(off == 1)
        def _():
            for index in range(2):
                source = swapped * (1 - index) + (1 - swapped) * index
                block_of(matrix.at[index], coords[1])[...] = flipped(
                    block_of(matrix.at[source], coords[0])[...]
                )

        @pl.when(jnp.logical_and(off == 0, my_class > 0))
        def _():
            for slot in range(2):
                block_of(matrix.at[1], coords[slot])[...] = flipped(
                    block_of(matrix.at[0], coords[slot])[...]
                )

    complete(me)
    for k in order:
        took(polar_out.at[0], p_recv.at[k])
        complete(from_of(k))

    @pl.when(my_class == 0)
    def _():
        took(polar_out.at[pl.ds(0, volume - paired)], m_recv.at[0])

    for index in range(2):
        inner[index] = plain_dot(coulomb[...], matrix[index]).astype(jnp.bfloat16)
    for index in range(2):
        product = plain_dot(inner[index], coulomb[...])
        second[index] = product
        matrix[index] = product.astype(jnp.bfloat16)
    parts = [(half, sub) for half in range(2) for sub in range(SUBS)]
    sub_rows = size // SUBS

    def wave(index, coords):
        rows, width = region(coords)
        third = plain_dot(inner[index, rows, :], matrix[index, :, width])
        whole = coulomb[rows, width].astype(jnp.float32) + second[index, rows, width] + third
        return whole.astype(jnp.bfloat16)

    for half in range(2):
        for t in range(1, classes):
            coords = unit_blocks(unit_of(first_mate + lax.rem(my_class + t, classes)), grid)[half]
            for index in range(2):
                screened[t, half, index] = wave(index, coords)
        for sub in range(SUBS):
            for t in range(1, classes):
                span_now = pl.ds(sub * sub_rows, sub_rows)
                remote(
                    screened.at[t, half, :, span_now], screen_in.at[my_class, half, :, span_now],
                    w_send.at[0], w_recv.at[half, sub], first_mate + lax.rem(my_class + t, classes),
                ).start()
    for half in range(2):
        for index in range(2):
            screen_in[my_class, half, index] = wave(index, own_blocks[half])

    def sigma_copy(half, sub, target):
        return remote(
            sigma_out.at[target, half, pl.ds(sub * sub_rows, sub_rows)],
            block_of(sigma, own_blocks[half], sub * sub_rows, sub_rows),
            s_send.at[0], s_recv.at[0], target,
        )

    def for_others(act):
        for other in range(volume):
            pl.when(me != other)(functools.partial(act, other))

    def send_sigma(n, targets):
        for target in range(volume):
            crosses = target // classes != me // classes
            chosen = crosses if targets else jnp.logical_and(me != target, jnp.logical_not(crosses))
            pl.when(chosen)(lambda: sigma_copy(*parts[n], target).start())

    for n, (half, sub) in enumerate(parts):
        took(
            screen_in.at[pl.ds(0, classes - 1), half, :, pl.ds(sub * sub_rows, sub_rows)],
            w_recv.at[half, sub],
        )

        def convolve(step, carry, half=half):
            rows = rows_of(step)
            if half == 0:
                mine = [landed[e, 0, rows, :].astype(jnp.float32) for e in range(volume)]
            else:
                mine = [second_half[e, rows, :].astype(jnp.float32) for e in range(volume)]
            waves = [
                screen_in[min(e, volume - e) % classes, half, e // classes, rows, :].astype(jnp.float32)
                for e in range(volume)
            ]
            for e in range(volume):
                acc = mine[0] * waves[e]
                for e2 in range(1, volume):
                    acc += mine[e2] * waves[(e - e2) % volume]
                sigma_out[e, half, rows, :] = (acc * scale_sigma).astype(jnp.bfloat16)
            return carry

        lax.fori_loop(sub * sub_rows // rows_at_once, (sub + 1) * sub_rows // rows_at_once, convolve, 0)
        send_sigma(n, True)
        send_sigma(n, False)
    for half in range(2):
        block_of(sigma, own_blocks[half])[...] = sigma_out[me, half]

    @pl.when(slab < slabs - 1)
    def _():
        corner_copy.wait_recv()
        near_next = plain_dot(coupling[...], next_corner[...]).astype(jnp.bfloat16)
        right_in[...] = plain_dot(near_next, turned[...]) * inv_root

    took(landed.at[others], s_recv.at[0])

    @pl.when(slab < slabs - 1)
    def _():
        sigma[last:, last:] = (sigma[last:, last:].astype(jnp.float32) + right_in[...]).astype(jnp.bfloat16)
        left_copy.wait_send()

    @pl.when(slab > 0)
    def _():
        left_copy.wait_recv()
        sigma[:size, :size] = (sigma[:size, :size].astype(jnp.float32) + left_in[...]).astype(jnp.bfloat16)
        corner_copy.wait_send()

    for chunk in range(CHUNKS):
        @pl.when(second_core > 0)
        def _():
            took(landed.at[others, :, span(chunk)], g_send.at[chunk])

        @pl.when(second_core == 0)
        def _():
            took(landed.at[others, :, span(chunk)], p_send.at[chunk])

    took(screen_in.at[pl.ds(0, classes - 1)], w_send.at[0])
    took(landed.at[others], s_send.at[0])

    @pl.when(diagonal == 1)
    def _():
        took(polar_out.at[pl.ds(0, 2)], m_send.at[0])


def dress_kernel(inv_root, total, green, out):
    dressed = plain_dot(green[...], total[...]).astype(jnp.bfloat16)
    updated = green[...].astype(jnp.float32) + plain_dot(dressed, green[...]) * inv_root
    out[...] = updated.astype(jnp.bfloat16)


def fused_on_device(grid, green_blocks, coulomb, couple_cols, couple_vals):
    volume = lax.axis_size("energy")
    slabs = lax.axis_size("slab")
    orbitals = green_blocks.shape[-1]
    size = orbitals // grid
    half_type = jnp.bfloat16

    def pieces(*lead):
        return pltpu.VMEM((*lead, size, size), half_type)

    def wholes(*lead, kind=half_type):
        return pltpu.VMEM((*lead, orbitals, orbitals), kind)

    def pair(sends, recvs):
        return [pltpu.SemaphoreType.DMA(sends), pltpu.SemaphoreType.DMA(recvs)]

    wide = pltpu.VMEM((size, size), jnp.float32)
    classes = volume // 2
    inv_root = 1.0 / math.sqrt(orbitals)
    in_vmem = pl.BlockSpec(memory_space=pltpu.VMEM)
    total, green = pl.pallas_call(
        functools.partial(
            fused_kernel, volume, slabs, grid,
            0.5 / math.sqrt(orbitals * volume), 0.2 / math.sqrt(volume), inv_root,
        ),
        out_shape=[jax.ShapeDtypeStruct((orbitals, orbitals), half_type)] * 2,
        in_specs=[pl.BlockSpec(memory_space=pltpu.HBM)] * 4,
        out_specs=[in_vmem] * 2,
        scratch_shapes=[
            wholes(), pltpu.VMEM(couple_cols.shape[:0:-1], jnp.int32), pltpu.VMEM(couple_vals.shape[:0:-1], half_type),
            pieces(volume), pieces(volume, 2), pieces(volume, 2), pieces(volume), pieces(classes, 2), pieces(2),
            wholes(2), wholes(2), wholes(2, kind=jnp.float32), pieces(classes, 2, 2),
            pieces(classes, 2, 2), pieces(volume, 2),
            pieces(), pieces(), pieces(), wide, wide, wide,
            *pair((CHUNKS,), (volume, CHUNKS)), *pair((CHUNKS,), (volume,)), *pair((1,), (1,)),
            *pair((1,), (2, SUBS)), *pair((1,), (1,)), *pair((2,), (2,)), pltpu.SemaphoreType.DMA((4,)),
            pltpu.SemaphoreType.REGULAR((1,)), pltpu.SemaphoreType.REGULAR((3,)),
        ],
        compiler_params=pltpu.CompilerParams(
            collective_id=0, has_side_effects=True, vmem_limit_bytes=32 << 20
        ),
    )(*(
        pltpu.with_memory_space_constraint(array, pltpu.HBM)
        for array in (green_blocks[0, 0], coulomb[0], couple_cols[0].T, couple_vals[0].T)
    ))
    result = pl.pallas_call(
        functools.partial(dress_kernel, inv_root),
        out_shape=jax.ShapeDtypeStruct((orbitals, orbitals), half_type),
        in_specs=[in_vmem] * 2,
        out_specs=in_vmem,
        compiler_params=pltpu.CompilerParams(vmem_limit_bytes=16 << 20),
    )(total, green)
    return result[None, None]


def fused_grid(mesh):
    volume = mesh.shape["energy"]
    grid = math.isqrt(2 * volume)
    return grid if grid * grid == 2 * volume and grid % 2 == 0 else 0


def on_any(grid, green_blocks, coulomb, couple_cols, couple_vals):
    orbitals = green_blocks.shape[-1]
    fits = (
        grid > 2
        and grid * 2 == lax.axis_size("energy")
        and green_blocks.shape[:2] == (1, 1)
        and orbitals % (128 * max(grid, 1)) == 0
        and couple_cols.shape[1] * grid == orbitals
        and lax.axis_size("slab") % 2 == 0
    )
    if fits:
        return fused_on_device(grid, green_blocks, coulomb, couple_cols, couple_vals)
    return on_device(green_blocks, coulomb, couple_cols, couple_vals)


def solution(mesh):
    return jax.shard_map(
        functools.partial(on_any, fused_grid(mesh)),
        mesh=mesh,
        in_specs=(
            P("energy", "slab", None, None),
            P("slab", None, None),
            P("slab", None, None),
            P("slab", None, None),
        ),
        out_specs=P("energy", "slab", None, None),
        check_vma=False,
    )
```
